32 devices in a mesh: ent: 2 (over x), blk: 4 (over y, core), rel: 4 (over z).
Axes of the slice: x: 2, y: 2, z: 4, core: 2. Of those that a mesh axis runs over, the one named last changes fastest.
Arguments:
- factors: bfloat16 [8192, 256], P(('ent', 'blk')), may hold values from -12 to 12
- heads: int32 [8, 4, 1, 8192], P(None, 'rel', None, ('ent', 'blk')), may hold values from 0 to 1023, as said below
- tails: int32 [8, 4, 1, 8192], P(None, 'rel', None, ('ent', 'blk')), may hold values from 0 to 1023, as said below
- values: float32 [8, 4, 1, 8192], P(None, 'rel', None, ('ent', 'blk')), may hold values from 0.3 to 9
Outputs:
- relation_fit: float32 [32, 256, 256], P(('ent', 'blk', 'rel'))
- residual: float32 [32, 256, 256], P(('ent', 'blk', 'rel'))
The draws below stay inside these ranges and needn't reach their ends.
Inputs may be any that keep to these rules, and one draw needn't show every extreme that they name: In every aligned tile of 128 triple columns (columns 128 t to 128 t + 127 of one relation) all heads lie in one aligned block of 128 positions (128 b to 128 b + 127). In every aligned tile of 128 triple columns all tails lie in one aligned block of 128 positions.
All inputs are finite; a program needn't handle non-finite values.
Results may differ from the reference program's by a relative error of at most 0.0029.
Values sent between devices are 32-bit elements; how exact they have to be, the bound alone decides.
A program may use at most 128 MiB of HBM per device.

```python
import math
import jax
import jax.numpy as jnp
from jax import lax

RANK = 256
ENT_DEV = 1024
TRIP = 1024
REL_DEV = 1
ITERS = 8
SHARDS = 8
ENTS = 8192
RELS = 32
N_REL = 4


def draw_factors(key, part):
    keys = jax.random.split(jax.random.fold_in(key, 11), 3)
    entries = jnp.clip(jax.random.normal(keys[0], (ENTS, RANK), jnp.float32), -6.0, 6.0)
    columns = jnp.exp(jax.random.uniform(keys[1], (RANK,), jnp.float32, math.log(0.1), 0.0))
    row_scale = jnp.exp(jax.random.uniform(keys[2], (ENTS, 1), jnp.float32, math.log(0.5), math.log(2.0)))
    return (entries * columns[None, :] * row_scale).astype(jnp.bfloat16)


def tiled_positions(key, salt):
    keys = jax.random.split(jax.random.fold_in(key, salt), 2)
    tile_count = SHARDS * TRIP // 128
    block_ids = jax.random.randint(keys[0], (SHARDS, N_REL, REL_DEV, tile_count, 1), 0, ENT_DEV // 128, jnp.int32)
    inside = jax.random.randint(keys[1], (SHARDS, N_REL, REL_DEV, tile_count, 128), 0, 128, jnp.int32)
    return (block_ids * 128 + inside).reshape(SHARDS, N_REL, REL_DEV, SHARDS * TRIP).astype(jnp.int32)


def draw_heads(key, part):
    return tiled_positions(key, 31)


def draw_tails(key, part):
    return tiled_positions(key, 47)


def draw_values(key, part):
    shape_all = (SHARDS, N_REL, REL_DEV, SHARDS * TRIP)
    sub_key = jax.random.fold_in(key, 23)
    base_values = jnp.exp(jax.random.uniform(sub_key, shape_all, jnp.float32, math.log(0.5), math.log(2.0)))
    first_index = jnp.arange(SHARDS, dtype=jnp.int32)[:, None, None, None]
    second_index = jnp.arange(N_REL, dtype=jnp.int32)[None, :, None, None]
    third_index = jnp.arange(REL_DEV, dtype=jnp.int32)[None, None, :, None]
    relation_index = ((first_index * N_REL + second_index) * REL_DEV + third_index).astype(jnp.float32)
    rising = 1.0 + 2.0 * relation_index / max(RELS - 1, 1)
    return (base_values * rising).astype(jnp.float32)


def setup_inputs(seed: int = 0) -> dict:
    streams_of = jax.random.split(jax.random.key(seed), 5)
    factors = draw_factors(jax.random.fold_in(streams_of[4], 71), 0)
    heads = draw_heads(jax.random.fold_in(streams_of[4], 71), 0)
    tails = draw_tails(jax.random.fold_in(streams_of[4], 71), 0)
    values = draw_values(jax.random.fold_in(streams_of[4], 71), 0)
    return dict(factors=factors, heads=heads, tails=tails, values=values)


ridge_weight = 0.01

def apply_normal(gram_matrix, stacked):
    left_side = jnp.einsum('ab,kbc->kac', gram_matrix, stacked, precision=lax.Precision.HIGHEST)
    return jnp.einsum('kac,cd->kad', left_side, gram_matrix, precision=lax.Precision.HIGHEST) + ridge_weight * stacked

def reference(factors, heads, tails, values):
    gram_matrix = jnp.dot(factors.T, factors, preferred_element_type=jnp.float32) / ENTS
    column_ids = jnp.arange(SHARDS * TRIP, dtype=jnp.int32)
    offsets = (column_ids // TRIP * ENT_DEV).astype(jnp.int32)
    head_ids = (heads.reshape(RELS, SHARDS * TRIP) + offsets).astype(jnp.int32)
    tail_ids = (tails.reshape(RELS, SHARDS * TRIP) + offsets).astype(jnp.int32)
    weights = values.reshape(RELS, SHARDS * TRIP)
    norm_scale = 1.0 / math.sqrt(SHARDS * TRIP)

    def single(operands):
        head_row, tail_row, weight_row = operands
        weighted = (weight_row[:, None] * jnp.take(factors, head_row, axis=0).astype(jnp.float32)).astype(jnp.bfloat16)
        tail_rows = jnp.take(factors, tail_row, axis=0)
        return jnp.dot(weighted.T, tail_rows, preferred_element_type=jnp.float32) * norm_scale
    target = lax.map(single, (head_ids, tail_ids, weights))
    fitted = jnp.zeros_like(target)
    residual = target
    direction = target
    norm_now = jnp.sum(residual * residual)
    for step_index in range(ITERS):
        image_map = apply_normal(gram_matrix, direction)
        step_size = norm_now / jnp.sum(direction * image_map)
        fitted = fitted + step_size * direction
        residual = residual - step_size * image_map
        norm_next = jnp.sum(residual * residual)
        direction = residual + norm_next / norm_now * direction
        norm_now = norm_next
    return (fitted, residual)
```

```python
import functools
import math

import jax
import jax.numpy as jnp
from jax import lax
from jax.experimental import pallas as pl
from jax.experimental.pallas import tpu as pltpu
from jax.sharding import PartitionSpec as P

ITERS = 8


ridge_weight = 0.01
tile_width = 128


def apply_normal(gram_matrix, stacked):
    left_side = jnp.einsum("ab,kbc->kac", gram_matrix, stacked, precision=lax.Precision.HIGHEST)
    return (
        jnp.einsum("kac,cd->kad", left_side, gram_matrix, precision=lax.Precision.HIGHEST)
        + ridge_weight * stacked
    )


def two_products(residual, image_map):
    return lax.psum(
        (jnp.sum(residual * residual), jnp.sum(residual * image_map)), ("ent", "blk", "rel")
    )


def select_rows(entity_ids, block_table):
    group_size, width = entity_ids.shape
    tile_count = width // tile_width
    block_count = block_table.shape[0]
    tiled_ids = entity_ids.reshape(group_size, tile_count, tile_width)
    block_of = tiled_ids[:, :, 0] // tile_width
    block_pick = (
        block_of[:, :, None] == jnp.arange(block_count, dtype=jnp.int32)[None, None, :]
    ).astype(jnp.bfloat16)
    chosen = jnp.einsum(
        "gtb,bcr->gtcr", block_pick, block_table, preferred_element_type=jnp.float32
    ).astype(jnp.bfloat16)
    inside = tiled_ids % tile_width
    slot_pick = (
        inside[:, :, :, None] == jnp.arange(tile_width, dtype=jnp.int32)[None, None, None, :]
    ).astype(jnp.bfloat16)
    return jnp.einsum("gtoc,gtcr->gtor", slot_pick, chosen, preferred_element_type=jnp.float32)


def body(factors, heads, tails, values):
    shards = lax.axis_size(("ent", "blk"))
    ent_dev = factors.shape[0]
    rank_width = factors.shape[1]
    triple_count = heads.shape[3]
    relation_rows = heads.shape[0] * heads.shape[2]
    norm_scale = 1.0 / math.sqrt(shards * triple_count)
    gram_total = lax.psum(
        jnp.dot(factors.T, factors, preferred_element_type=jnp.float32), ("ent", "blk")
    )
    gram_matrix = gram_total / (ent_dev * shards)
    block_table = factors.reshape(ent_dev // tile_width, tile_width, rank_width)
    head_ids = heads.reshape(relation_rows, triple_count)
    tail_ids = tails.reshape(relation_rows, triple_count)
    weights = values.reshape(relation_rows, triple_count)

    def grouped(operands):
        head_group, tail_group, weight_group = operands
        group_size = head_group.shape[0]
        tile_count = triple_count // tile_width
        head_rows = select_rows(head_group, block_table)
        weighted = (
            weight_group.reshape(group_size, tile_count, tile_width)[:, :, :, None] * head_rows
        ).astype(jnp.bfloat16)
        tail_rows = select_rows(tail_group, block_table).astype(jnp.bfloat16)
        product = jnp.einsum(
            "gtci,gtcj->gij", weighted, tail_rows, preferred_element_type=jnp.float32
        )
        return product * norm_scale

    own_rows = relation_rows // shards
    group_size = math.gcd(own_rows * lax.axis_size(("ent", "blk")), 4)
    group_total = own_rows * lax.axis_size(("ent", "blk")) // group_size
    shaped = (
        head_ids.reshape(group_total, group_size, triple_count),
        tail_ids.reshape(group_total, group_size, triple_count),
        weights.reshape(group_total, group_size, triple_count),
    )
    results = lax.map(grouped, shaped)
    target = lax.psum_scatter(
        results.reshape(own_rows * lax.axis_size(("ent", "blk")), rank_width, rank_width),
        ("ent", "blk"),
        scatter_dimension=0,
        tiled=True,
    )
    fitted = jnp.zeros_like(target)
    residual = target
    image_map = apply_normal(gram_matrix, residual)
    norm_now, product = two_products(residual, image_map)
    step_size = norm_now / product
    direction = residual
    along = image_map
    for step_index in range(ITERS):
        fitted = fitted + step_size * direction
        residual = residual - step_size * along
        if step_index + 1 < ITERS:
            image_map = apply_normal(gram_matrix, residual)
            norm_next, product = two_products(residual, image_map)
            ratio_next = norm_next / norm_now
            step_size = norm_next / (product - ratio_next * norm_next / step_size)
            direction = residual + ratio_next * direction
            along = image_map + ratio_next * along
            norm_now = norm_next
    return (fitted, residual)


MESH = pl.DeviceIdType.MESH
COPIES = 24


def fused_kernel(
    z_count, scale_gram, scale_target,
    factors_hbm, heads_hbm, tails_hbm, values_hbm,
    fit_ref, res_ref,
    factors_ref, heads_ref, tails_ref, values_ref, head_ids, tail_ids,
    first_heads, first_tails, load_sem, ready,
    turned, left_rows, right_rows,
    gram_part, gram_in, gram_half, gram_xy, gram_line, gram_full, gram_pair,
    pair_out, pair_in, own_sum, first_a, first_b, second_a, second_b,
    basis, early, late, send_sem, recv_sem,
):
    f32, bf16 = jnp.float32, jnp.bfloat16
    width = factors_ref.shape[1]
    half = width // 2
    share = half // z_count
    part = share // 2
    triples = heads_ref.shape[3]
    e = lax.axis_index("ent")
    b = lax.axis_index("blk")
    z = lax.axis_index("rel")
    y = b // 2
    c = b % 2
    pair_peer = (e, y * 2 + 1 - c, z)
    x_peer = (1 - e, b, z)
    y_peer = (e, (1 - y) * 2 + c, z)

    def group_peer(mask):
        me, my, mc = mask // 4, (mask // 2) % 2, mask % 2
        return (
            (1 - e) if me else e,
            ((1 - y) if my else y) * 2 + ((1 - c) if mc else c),
            z,
        )

    def z_peer(hop):
        return (e, b, lax.rem(z + hop, z_count))

    near = [group_peer(m) for m in (1, 2, 4)]
    inner = ((z > 0, -1), (z < z_count - 1, 1))

    def tell(semaphore):
        for present, hop in inner:
            @pl.when(present)
            def _():
                pl.semaphore_signal(
                    semaphore, inc=1, device_id=(e, b, z + hop), device_id_type=MESH
                )

    line_count = jnp.where(z > 0, 1, 0) + jnp.where(z < z_count - 1, 1, 0)
    barrier = pltpu.get_barrier_semaphore()
    for peer in near:
        pl.semaphore_signal(barrier, inc=1, device_id=peer, device_id_type=MESH)
    tell(barrier)
    first_q = (1 - e) * 4 + (1 - y) * 2 + 1 - c
    loads = []
    for slot, (source, dest) in enumerate(
        (
            (factors_hbm, factors_ref),
            (heads_hbm.at[pl.ds(first_q, 1)], first_heads),
            (tails_hbm.at[pl.ds(first_q, 1)], first_tails),
            (heads_hbm, heads_ref),
            (values_hbm, values_ref),
            (tails_hbm, tails_ref),
            (heads_hbm, head_ids),
            (tails_hbm, tail_ids),
        )
    ):
        loads.append(pltpu.make_async_copy(source, dest, load_sem.at[slot]))
        loads[-1].start()

    counter = [0]

    def spare():
        slot = counter[0]
        counter[0] += 1
        return send_sem.at[slot], recv_sem.at[slot]

    def copy_to(source, dest, peer, pair):
        return pltpu.make_async_remote_copy(
            src_ref=source, dst_ref=dest, send_sem=pair[0], recv_sem=pair[1],
            device_id=peer, device_id_type=MESH,
        )

    def send(source, dest, peer):
        copy = copy_to(source, dest, peer, spare())
        copy.start()
        return copy

    far_peers = [
        (m, hop) for hop in range(z_count - 1, -1, -1) for m in (7, 6, 5, 3, 4, 2, 1, 0) if m or hop
    ]

    def spread(table):
        pair = spare()
        for m, hop in far_peers:
            peer = group_peer(m)[:2] + (lax.rem(z + hop, z_count),)
            place = m * z_count + (z_count - hop) % z_count
            copy_to(table.at[0], table.at[place], peer, pair).start()
        others = table.at[pl.ds(1, 8 * z_count - 1)]
        return copy_to(others, others, pair_peer, pair)

    loads[0].wait()
    flipped = factors_ref[...].T
    for block in range(turned.shape[0]):
        turned[block] = flipped[:, block * tile_width : (block + 1) * tile_width]
    own_rows = pl.ds(pl.multiple_of(c * half, half), half)
    other_rows = pl.ds(pl.multiple_of((1 - c) * half, half), half)
    own_share = pl.ds(pl.multiple_of(c * half + z * share, share), share)
    other_share = pl.ds(pl.multiple_of((1 - c) * half + z * share, share), share)

    row_number = lax.broadcasted_iota(jnp.int32, (tile_width, tile_width), 0)
    blank = jnp.zeros((tile_width, tile_width), bf16)

    def gathered(ids_ref, scalar_ref, q, place, first):
        picks, blocks = [], []
        for tile in (first, first + 1):
            start = tile * tile_width
            inside = lax.rem(ids_ref[q, 0, :, start : start + tile_width], tile_width)
            picks.append(jnp.where(row_number == inside, 1.0, 0.0).astype(bf16))
            blocks.append(turned[lax.div(scalar_ref[place, 0, 0, start], tile_width)])
        mixed = jnp.concatenate(
            [
                jnp.concatenate([picks[0], blank], axis=1),
                jnp.concatenate([blank, picks[1]], axis=1),
            ],
            axis=0,
        )
        return jnp.dot(jnp.concatenate(blocks, axis=1), mixed, preferred_element_type=f32)

    def partial(pe, py, pc, head_blocks=head_ids, tail_blocks=tail_ids, place=None):
        q = pe * 4 + py * 2 + pc
        place = q if place is None else place
        for first in range(0, triples // tile_width, 2):
            cols = slice(first * tile_width, (first + 2) * tile_width)
            rows = gathered(heads_ref, head_blocks, q, place, first)
            left_rows[:, cols] = (values_ref[q, 0, :, cols] * rows).astype(bf16)
            right_rows[:, cols] = gathered(tails_ref, tail_blocks, q, place, first).astype(bf16)
        return lax.dot_general(
            left_rows[...], right_rows[...], (((1,), (1,)), ((), ())), preferred_element_type=f32
        )

    targets = ((1 - e, 1 - y), (1 - e, y), (e, 1 - y), (e, y))
    pair_copies = []

    def give(index):
        pe, py = targets[index]
        pair_out[index] = partial(pe, py, 1 - c)
        pair_copies.append(send(pair_out.at[index], pair_in.at[index], pair_peer))

    def keep(index):
        pe, py = targets[index]
        own_sum[index] = partial(pe, py, c)

    def join(index):
        pair_copies[index].wait()
        own_sum[index] = own_sum[index] + pair_in[index]

    top, low = pl.ds(0, half), pl.ds(half, half)
    for load in loads[1:6]:
        load.wait()
    pair_out[0] = partial(1 - e, 1 - y, 1 - c, first_heads, first_tails, 0)
    pl.semaphore_wait(barrier, len(near) + line_count)
    pair_copies.append(send(pair_out.at[0], pair_in.at[0], pair_peer))
    if z_count > 2:
        tell(ready.at[0])
    gram_part[...] = lax.dot_general(
        flipped, flipped, (((1,), (1,)), ((), ())), preferred_element_type=f32
    )
    g_pair = send(gram_part.at[other_share], gram_in, pair_peer)
    for load in loads[6:]:
        load.wait()
    keep(0)
    g_pair.wait()
    gram_half[0] = gram_part[own_share, :] + gram_in[...]
    upper, lower = pl.ds(0, part), pl.ds(part, part)
    g_a1 = send(gram_half.at[0, upper], gram_xy.at[0, upper], x_peer)
    g_b1 = send(gram_half.at[0, lower], gram_xy.at[0, lower], y_peer)
    join(0)
    a_diag = send(own_sum.at[0, top], first_a.at[0], x_peer)
    b_diag = send(own_sum.at[0, low], first_b.at[0], y_peer)
    give(1)
    give(2)
    for step in range(1, z_count - 2):
        pl.semaphore_wait(ready.at[step - 1], line_count)
        tell(ready.at[step])
    keep(1)
    g_a1.wait()
    g_b1.wait()
    gram_half[1] = gram_half[0] + gram_xy[0]
    g_a2 = send(gram_half.at[1, upper], gram_xy.at[1, upper], y_peer)
    g_b2 = send(gram_half.at[1, lower], gram_xy.at[1, lower], x_peer)
    join(1)
    a_side = send(own_sum.at[1, top], first_a.at[1], x_peer)
    keep(2)
    join(2)
    b_side = send(own_sum.at[2, low], first_b.at[1], y_peer)
    give(3)
    keep(3)
    a_diag.wait()
    second_a[0] = own_sum[2, :half, :] + first_a[0]
    a_last = send(second_a.at[0], second_a.at[1], y_peer)
    b_diag.wait()
    second_b[0] = own_sum[1, half:, :] + first_b[0]
    b_last = send(second_b.at[0], second_b.at[1], x_peer)
    g_a2.wait()
    g_b2.wait()
    gram_line[0] = gram_half[1] + gram_xy[1]
    if z_count > 2:
        pl.semaphore_wait(ready.at[z_count - 3], line_count)
    line_copies = [
        send(gram_line.at[0], gram_line.at[z_count - hop], z_peer(hop))
        for hop in range(1, z_count)
    ]
    join(3)
    for copy in line_copies:
        copy.wait()
    for hop in range(z_count):
        place = lax.rem(z + hop, z_count)
        gram_pair[0, pl.ds(pl.multiple_of(place * share, share), share), :] = gram_line[hop]
    g_full = send(gram_pair.at[0], gram_pair.at[1], pair_peer)
    g_full.wait()
    gram_full[own_rows, :] = gram_pair[0] * scale_gram
    gram_full[other_rows, :] = gram_pair[1] * scale_gram

    def split(value):
        high = value.astype(bf16)
        return high, (value - high.astype(f32)).astype(bf16)

    def total(value):
        return jnp.sum(jnp.sum(value, axis=0, keepdims=True), axis=1, keepdims=True)

    def two_sided(matrix):
        matrix_high, matrix_low = split(matrix)
        matrix_both = jnp.concatenate([matrix_high, matrix_low], axis=0)

        def apply(value):
            high, low_part = split(value)
            both = jnp.dot(matrix_both, high, preferred_element_type=f32)
            inner = both[:width] + (
                both[width:] + jnp.dot(matrix_high, low_part, preferred_element_type=f32)
            )
            high, low_part = split(inner)
            both = jnp.dot(
                jnp.concatenate([high, low_part], axis=0),
                matrix_high,
                preferred_element_type=f32,
            )
            return both[:width] + (
                both[width:] + jnp.dot(high, matrix_low, preferred_element_type=f32)
            )

        return apply

    gram = gram_full[...]
    gram_high, gram_low = split(gram)
    gram_twice = jnp.dot(gram_high, gram_high, preferred_element_type=f32) + (
        jnp.dot(gram_high, gram_low, preferred_element_type=f32)
        + jnp.dot(gram_low, gram_high, preferred_element_type=f32)
    )
    once, twice = two_sided(gram), two_sided(gram_twice)
    a_side.wait()
    b_side.wait()
    a_last.wait()
    b_last.wait()
    basis[0, :half, :] = ((own_sum[3, :half, :] + first_a[1]) + second_a[1]) * scale_target
    basis[0, half:, :] = ((own_sum[3, half:, :] + first_b[1]) + second_b[1]) * scale_target

    lane = lax.broadcasted_iota(jnp.int32, (1, 128), 1)
    record = jnp.zeros((1, 128), f32)

    def noted(record, place, value):
        return jnp.where(lane == place, value, record)

    def sized(vector):
        square = total(vector * vector)
        inverse = jnp.where(square > 0.0, lax.rsqrt(square), 0.0)
        return inverse, square * inverse

    inverses = []
    for index in range(0, ITERS, 2):
        vector = basis[index]
        image = once(vector)
        image_twice = twice(vector)
        inverse, length = sized(vector)
        record = noted(record, ITERS + index, length)
        if index + 2 == ITERS:
            early[0] = record
            early_copy = spread(early)
        diagonal = (total(vector * image) * inverse) * inverse
        record = noted(record, index, diagonal + ridge_weight)
        following = (image - diagonal * vector) * inverse
        beyond = (image_twice - diagonal * image) * inverse
        if index > 0:
            ratio = length * inverses[-1]
            following = following - ratio * basis[index - 1]
            beyond = beyond - ratio * mapped
        mapped = beyond
        inverses.append(inverse)
        basis[index + 1] = following
        inverse, length = sized(following)
        diagonal = (total(following * beyond) * inverse) * inverse
        record = noted(record, index + 1, diagonal + ridge_weight)
        record = noted(record, ITERS + index + 1, length)
        if index + 2 == ITERS:
            late[0] = record
            late_copy = spread(late)
        basis[index + 2] = (beyond - diagonal * following) * inverse - (
            length * inverses[-1]
        ) * vector
        inverses.append(inverse)

    def lanes_of(table):
        lines = table[...].reshape(8 * z_count, 128)
        blank_lines = jnp.zeros((128 - 8 * z_count, 128), f32)
        return jnp.concatenate([lines, blank_lines], axis=0).T

    early_copy.wait()
    filled = lanes_of(early)
    alpha = [filled[j : j + 1, :] for j in range(ITERS - 2)]
    beta = [filled[ITERS + j : ITERS + j + 1, :] for j in range(ITERS - 1)]

    def reduced(rows):
        added = rows[0]
        for row in rows[1:]:
            added = added + row
        return jnp.sum(added, axis=1, keepdims=True)

    def small_map(rows):
        count = len(rows)
        made = []
        for j in range(count + 1):
            entry = None
            if j < count:
                entry = alpha[j] * rows[j]
            if j > 0:
                term = beta[j] * rows[j - 1]
                entry = term if entry is None else entry + term
            if j + 1 < count:
                entry = entry + beta[j + 1] * rows[j + 1]
            made.append(entry)
        return made

    def mixed_sum(first, ratio, second):
        return [
            one + ratio * second[j] if j < len(second) else one for j, one in enumerate(first)
        ]

    residual = [beta[0]]
    image = small_map(residual)
    norm_now = reduced([row * row for row in residual])
    product = reduced([row * image[j] for j, row in enumerate(residual)])
    step_size = norm_now / product
    direction, along = residual, image
    fitted = []
    for index in range(ITERS):
        fitted = [
            fitted[j] + step_size * row if j < len(fitted) else step_size * row
            for j, row in enumerate(direction)
        ]
        residual = [
            residual[j] - step_size * row if j < len(residual) else -(step_size * row)
            for j, row in enumerate(along)
        ]
        if index + 1 < ITERS:
            norm_next = reduced([row * row for row in residual])
            if index + 3 == ITERS:
                late_copy.wait()
                filled = lanes_of(late)
                alpha += [filled[j : j + 1, :] for j in range(ITERS - 2, ITERS)]
                beta += [filled[2 * ITERS - 1 : 2 * ITERS, :], jnp.ones((1, 128), f32)]
            image = small_map(residual)
            product = reduced([row * image[j] for j, row in enumerate(residual)])
            ratio = norm_next / norm_now
            step_size = norm_next / (product - ratio * norm_next / step_size)
            direction = mixed_sum(residual, ratio, direction)
            along = mixed_sum(image, ratio, along)
            norm_now = norm_next
    inverses.append(jnp.ones((1, 1), f32))
    fit_weights = [row[:, 0:1] * inverses[j] for j, row in enumerate(fitted)]
    res_weights = [row[:, 0:1] * inverses[j] for j, row in enumerate(residual)]
    fit = fit_weights[0] * basis[0]
    res = res_weights[0] * basis[0]
    for j in range(1, ITERS):
        fit = fit + fit_weights[j] * basis[j]
        res = res + res_weights[j] * basis[j]
    fit_ref[0] = fit
    res_ref[0] = res + res_weights[ITERS] * basis[ITERS]


def fused_body(factors, heads, tails, values):
    shards = lax.axis_size(("ent", "blk"))
    z_count = lax.axis_size("rel")
    ent_dev, width = factors.shape
    triples = heads.shape[3]
    half = width // 2
    f32, bf16 = jnp.float32, jnp.bfloat16
    vmem = pl.BlockSpec(memory_space=pltpu.VMEM)
    out = pltpu.VMEM((1, width, width), f32)
    share = half // z_count
    return pl.pallas_call(
        functools.partial(
            fused_kernel, z_count, 1.0 / (ent_dev * shards), 1.0 / math.sqrt(shards * triples)
        ),
        out_shape=(out, out),
        in_specs=[pl.BlockSpec(memory_space=pl.ANY)] * 4,
        out_specs=(vmem, vmem),
        scratch_shapes=[
            pltpu.VMEM(factors.shape, bf16),
            pltpu.VMEM(heads.shape, jnp.int32),
            pltpu.VMEM(tails.shape, jnp.int32),
            pltpu.VMEM(values.shape, f32),
            pltpu.SMEM(heads.shape, jnp.int32),
            pltpu.SMEM(tails.shape, jnp.int32),
            pltpu.SMEM((1,) + heads.shape[1:], jnp.int32),
            pltpu.SMEM((1,) + heads.shape[1:], jnp.int32),
            pltpu.SemaphoreType.DMA((8,)),
            pltpu.SemaphoreType.REGULAR((max(z_count - 2, 1),)),
            pltpu.VMEM((ent_dev // tile_width, width, tile_width), bf16),
            pltpu.VMEM((width, triples), bf16),
            pltpu.VMEM((width, triples), bf16),
            pltpu.VMEM((width, width), f32),
            pltpu.VMEM((share, width), f32),
            pltpu.VMEM((2, share, width), f32),
            pltpu.VMEM((2, share, width), f32),
            pltpu.VMEM((z_count, share, width), f32),
            pltpu.VMEM((width, width), f32),
            pltpu.VMEM((2, half, width), f32),
            pltpu.VMEM((4, width, width), f32),
            pltpu.VMEM((4, width, width), f32),
            pltpu.VMEM((4, width, width), f32),
            pltpu.VMEM((2, half, width), f32),
            pltpu.VMEM((2, half, width), f32),
            pltpu.VMEM((2, half, width), f32),
            pltpu.VMEM((2, half, width), f32),
            pltpu.VMEM((ITERS + 1, width, width), f32),
            pltpu.VMEM((8 * z_count, 1, 128), f32),
            pltpu.VMEM((8 * z_count, 1, 128), f32),
            pltpu.SemaphoreType.DMA((COPIES,)),
            pltpu.SemaphoreType.DMA((COPIES,)),
        ],
        compiler_params=pltpu.CompilerParams(collective_id=0, has_side_effects=True),
    )(factors, heads, tails, values)


def solution(mesh):
    placed = (
        P(("ent", "blk"), None),
        P(None, "rel", None, ("ent", "blk")),
        P(None, "rel", None, ("ent", "blk")),
        P(None, "rel", None, ("ent", "blk")),
    )
    sizes = dict(mesh.shape)
    fused = sizes["ent"] == 2 and sizes["blk"] == 4 and sizes["rel"] in (2, 4, 8)
    return jax.shard_map(
        fused_body if fused else body,
        mesh=mesh,
        in_specs=placed,
        out_specs=(P(("ent", "blk", "rel"), None, None), P(("ent", "blk", "rel"), None, None)),
        check_vma=False,
    )
```

```python
import functools
import math

import jax
import jax.numpy as jnp
from jax import lax
from jax.experimental import pallas as pl
from jax.experimental.pallas import tpu as pltpu
from jax.sharding import PartitionSpec as P

ITERS = 8


ridge_weight = 0.01
tile_width = 128


def apply_normal(gram_matrix, stacked):
    left_side = jnp.einsum("ab,kbc->kac", gram_matrix, stacked, precision=lax.Precision.HIGHEST)
    return (
        jnp.einsum("kac,cd->kad", left_side, gram_matrix, precision=lax.Precision.HIGHEST)
        + ridge_weight * stacked
    )


def two_products(residual, image_map):
    return lax.psum(
        (jnp.sum(residual * residual), jnp.sum(residual * image_map)), ("ent", "blk", "rel")
    )


def select_rows(entity_ids, block_table):
    group_size, width = entity_ids.shape
    tile_count = width // tile_width
    block_count = block_table.shape[0]
    tiled_ids = entity_ids.reshape(group_size, tile_count, tile_width)
    block_of = tiled_ids[:, :, 0] // tile_width
    block_pick = (
        block_of[:, :, None] == jnp.arange(block_count, dtype=jnp.int32)[None, None, :]
    ).astype(jnp.bfloat16)
    chosen = jnp.einsum(
        "gtb,bcr->gtcr", block_pick, block_table, preferred_element_type=jnp.float32
    ).astype(jnp.bfloat16)
    inside = tiled_ids % tile_width
    slot_pick = (
        inside[:, :, :, None] == jnp.arange(tile_width, dtype=jnp.int32)[None, None, None, :]
    ).astype(jnp.bfloat16)
    return jnp.einsum("gtoc,gtcr->gtor", slot_pick, chosen, preferred_element_type=jnp.float32)


def body(factors, heads, tails, values):
    shards = lax.axis_size(("ent", "blk"))
    ent_dev = factors.shape[0]
    rank_width = factors.shape[1]
    triple_count = heads.shape[3]
    relation_rows = heads.shape[0] * heads.shape[2]
    norm_scale = 1.0 / math.sqrt(shards * triple_count)
    gram_total = lax.psum(
        jnp.dot(factors.T, factors, preferred_element_type=jnp.float32), ("ent", "blk")
    )
    gram_matrix = gram_total / (ent_dev * shards)
    block_table = factors.reshape(ent_dev // tile_width, tile_width, rank_width)
    head_ids = heads.reshape(relation_rows, triple_count)
    tail_ids = tails.reshape(relation_rows, triple_count)
    weights = values.reshape(relation_rows, triple_count)

    def grouped(operands):
        head_group, tail_group, weight_group = operands
        group_size = head_group.shape[0]
        tile_count = triple_count // tile_width
        head_rows = select_rows(head_group, block_table)
        weighted = (
            weight_group.reshape(group_size, tile_count, tile_width)[:, :, :, None] * head_rows
        ).astype(jnp.bfloat16)
        tail_rows = select_rows(tail_group, block_table).astype(jnp.bfloat16)
        product = jnp.einsum(
            "gtci,gtcj->gij", weighted, tail_rows, preferred_element_type=jnp.float32
        )
        return product * norm_scale

    own_rows = relation_rows // shards
    group_size = math.gcd(own_rows * lax.axis_size(("ent", "blk")), 4)
    group_total = own_rows * lax.axis_size(("ent", "blk")) // group_size
    shaped = (
        head_ids.reshape(group_total, group_size, triple_count),
        tail_ids.reshape(group_total, group_size, triple_count),
        weights.reshape(group_total, group_size, triple_count),
    )
    results = lax.map(grouped, shaped)
    target = lax.psum_scatter(
        results.reshape(own_rows * lax.axis_size(("ent", "blk")), rank_width, rank_width),
        ("ent", "blk"),
        scatter_dimension=0,
        tiled=True,
    )
    fitted = jnp.zeros_like(target)
    residual = target
    image_map = apply_normal(gram_matrix, residual)
    norm_now, product = two_products(residual, image_map)
    step_size = norm_now / product
    direction = residual
    along = image_map
    for step_index in range(ITERS):
        fitted = fitted + step_size * direction
        residual = residual - step_size * along
        if step_index + 1 < ITERS:
            image_map = apply_normal(gram_matrix, residual)
            norm_next, product = two_products(residual, image_map)
            ratio_next = norm_next / norm_now
            step_size = norm_next / (product - ratio_next * norm_next / step_size)
            direction = residual + ratio_next * direction
            along = image_map + ratio_next * along
            norm_now = norm_next
    return (fitted, residual)


MESH = pl.DeviceIdType.MESH
COPIES = 21
CHUNKS = 4
PIECES = 7


def fused_kernel(
    z_count, scale_gram, scale_target,
    factors_hbm, heads_hbm, tails_hbm, values_hbm,
    pieces, mix_ref,
    factors_ref, heads_ref, tails_ref, values_ref, head_ids, tail_ids,
    first_heads, first_tails, factor_sem, load_sem, ready,
    turned, left_rows, right_rows,
    gram_part, gram_in, gram_half, gram_xy, gram_line, gram_full, gram_pair,
    pair_out, pair_in, own_sum, first_a, first_b, second_a, second_b,
    basis, early, late, send_sem, recv_sem,
):
    f32, bf16 = jnp.float32, jnp.bfloat16
    width = factors_ref.shape[1]
    half = width // 2
    share = half // z_count
    part = share // 2
    triples = heads_ref.shape[3]
    e = lax.axis_index("ent")
    b = lax.axis_index("blk")
    z = lax.axis_index("rel")
    y = b // 2
    c = b % 2
    pair_peer = (e, y * 2 + 1 - c, z)
    x_peer = (1 - e, b, z)
    y_peer = (e, (1 - y) * 2 + c, z)

    def group_peer(mask):
        me, my, mc = mask // 4, (mask // 2) % 2, mask % 2
        return (
            (1 - e) if me else e,
            ((1 - y) if my else y) * 2 + ((1 - c) if mc else c),
            z,
        )

    def z_peer(hop):
        return (e, b, lax.rem(z + hop, z_count))

    near = [group_peer(m) for m in (1, 2, 4)]
    inner = ((z > 0, -1), (z < z_count - 1, 1))

    def tell(semaphore):
        for present, hop in inner:
            @pl.when(present)
            def _():
                pl.semaphore_signal(
                    semaphore, inc=1, device_id=(e, b, z + hop), device_id_type=MESH
                )

    line_count = jnp.where(z > 0, 1, 0) + jnp.where(z < z_count - 1, 1, 0)
    barrier = pltpu.get_barrier_semaphore()
    for peer in near:
        pl.semaphore_signal(barrier, inc=1, device_id=peer, device_id_type=MESH)
    tell(barrier)
    first_q = (1 - e) * 4 + (1 - y) * 2 + 1 - c
    chunk = factors_ref.shape[0] // CHUNKS
    factor_loads = []
    for slot in range(CHUNKS):
        rows = pl.ds(slot * chunk, chunk)
        factor_loads.append(
            pltpu.make_async_copy(
                factors_hbm.at[rows], factors_ref.at[rows], factor_sem.at[slot]
            )
        )
        factor_loads[-1].start()
    loads = []
    for slot, (source, dest) in enumerate(
        (
            (heads_hbm.at[pl.ds(first_q, 1)], first_heads),
            (tails_hbm.at[pl.ds(first_q, 1)], first_tails),
            (heads_hbm, heads_ref),
            (values_hbm, values_ref),
            (tails_hbm, tails_ref),
            (heads_hbm, head_ids),
            (tails_hbm, tail_ids),
        )
    ):
        loads.append(pltpu.make_async_copy(source, dest, load_sem.at[slot]))
        loads[-1].start()

    counter = [0]

    def spare():
        slot = counter[0]
        counter[0] += 1
        return send_sem.at[slot], recv_sem.at[slot]

    def copy_to(source, dest, peer, pair):
        return pltpu.make_async_remote_copy(
            src_ref=source, dst_ref=dest, send_sem=pair[0], recv_sem=pair[1],
            device_id=peer, device_id_type=MESH,
        )

    def send(source, dest, peer):
        copy = copy_to(source, dest, peer, spare())
        copy.start()
        return copy

    far_peers = [
        (m, hop) for hop in range(z_count - 1, -1, -1) for m in (7, 6, 5, 3, 4, 2, 1, 0) if m or hop
    ]

    def spread(table):
        pair = spare()
        for m, hop in far_peers:
            peer = group_peer(m)[:2] + (lax.rem(z + hop, z_count),)
            place = m * z_count + (z_count - hop) % z_count
            copy_to(table.at[0], table.at[place], peer, pair).start()
        others = table.at[pl.ds(1, 8 * z_count - 1)]
        return copy_to(others, others, pair_peer, pair)

    flipped = []
    for slot in range(CHUNKS):
        factor_loads[slot].wait()
        flipped.append(factors_ref[slot * chunk : (slot + 1) * chunk, :].T)
        for step in range(chunk // tile_width):
            turned[slot * (chunk // tile_width) + step] = flipped[-1][
                :, step * tile_width : (step + 1) * tile_width
            ]
    own_rows = pl.ds(pl.multiple_of(c * half, half), half)
    other_rows = pl.ds(pl.multiple_of((1 - c) * half, half), half)
    own_share = pl.ds(pl.multiple_of(c * half + z * share, share), share)
    other_share = pl.ds(pl.multiple_of((1 - c) * half + z * share, share), share)

    row_number = lax.broadcasted_iota(jnp.int32, (tile_width, tile_width), 0)
    blank = jnp.zeros((tile_width, tile_width), bf16)

    def gathered(ids_ref, scalar_ref, q, place, first):
        picks, blocks = [], []
        for tile in (first, first + 1):
            start = tile * tile_width
            inside = lax.rem(ids_ref[q, 0, :, start : start + tile_width], tile_width)
            picks.append(jnp.where(row_number == inside, 1.0, 0.0).astype(bf16))
            blocks.append(turned[lax.div(scalar_ref[place, 0, 0, start], tile_width)])
        mixed = jnp.concatenate(
            [
                jnp.concatenate([picks[0], blank], axis=1),
                jnp.concatenate([blank, picks[1]], axis=1),
            ],
            axis=0,
        )
        return jnp.dot(jnp.concatenate(blocks, axis=1), mixed, preferred_element_type=f32)

    def partial(pe, py, pc, head_blocks=head_ids, tail_blocks=tail_ids, place=None):
        q = pe * 4 + py * 2 + pc
        place = q if place is None else place
        for first in range(0, triples // tile_width, 2):
            cols = slice(first * tile_width, (first + 2) * tile_width)
            rows = gathered(heads_ref, head_blocks, q, place, first)
            left_rows[:, cols] = (values_ref[q, 0, :, cols] * rows).astype(bf16)
            right_rows[:, cols] = gathered(tails_ref, tail_blocks, q, place, first).astype(bf16)
        return lax.dot_general(
            left_rows[...], right_rows[...], (((1,), (1,)), ((), ())), preferred_element_type=f32
        )

    targets = ((1 - e, 1 - y), (1 - e, y), (e, 1 - y), (e, y))
    pair_copies = []

    def give(index):
        pe, py = targets[index]
        pair_out[index] = partial(pe, py, 1 - c)
        pair_copies.append(send(pair_out.at[index], pair_in.at[index], pair_peer))

    def keep(index):
        pe, py = targets[index]
        own_sum[index] = partial(pe, py, c)

    def join(index):
        pair_copies[index].wait()
        own_sum[index] = own_sum[index] + pair_in[index]

    top, low = pl.ds(0, half), pl.ds(half, half)
    for load in loads[:5]:
        load.wait()
    pair_out[0] = partial(1 - e, 1 - y, 1 - c, first_heads, first_tails, 0)
    pl.semaphore_wait(barrier, len(near) + line_count)
    pair_copies.append(send(pair_out.at[0], pair_in.at[0], pair_peer))
    if z_count > 2:
        tell(ready.at[0])
    gram_part[...] = jnp.dot(
        jnp.concatenate(flipped, axis=1), factors_ref[...], preferred_element_type=f32
    )
    g_pair = send(gram_part.at[other_share], gram_in, pair_peer)
    for load in loads[5:]:
        load.wait()
    keep(0)
    g_pair.wait()
    gram_half[0] = gram_part[own_share, :] + gram_in[...]
    upper, lower = pl.ds(0, part), pl.ds(part, part)
    g_a1 = send(gram_half.at[0, upper], gram_xy.at[0, upper], x_peer)
    g_b1 = send(gram_half.at[0, lower], gram_xy.at[0, lower], y_peer)
    join(0)
    a_diag = send(own_sum.at[0, top], first_a.at[0], x_peer)
    b_diag = send(own_sum.at[0, low], first_b.at[0], y_peer)
    give(1)
    give(2)
    for step in range(1, z_count - 2):
        pl.semaphore_wait(ready.at[step - 1], line_count)
        tell(ready.at[step])
    keep(1)
    g_a1.wait()
    g_b1.wait()
    gram_half[1] = gram_half[0] + gram_xy[0]
    g_a2 = send(gram_half.at[1, upper], gram_xy.at[1, upper], y_peer)
    g_b2 = send(gram_half.at[1, lower], gram_xy.at[1, lower], x_peer)
    join(1)
    a_side = send(own_sum.at[1, top], first_a.at[1], x_peer)
    keep(2)
    join(2)
    b_side = send(own_sum.at[2, low], first_b.at[1], y_peer)
    give(3)
    keep(3)
    a_diag.wait()
    second_a[0] = own_sum[2, :half, :] + first_a[0]
    a_last = send(second_a.at[0], second_a.at[1], y_peer)
    b_diag.wait()
    second_b[0] = own_sum[1, half:, :] + first_b[0]
    b_last = send(second_b.at[0], second_b.at[1], x_peer)
    g_a2.wait()
    g_b2.wait()
    gram_line[0] = gram_half[1] + gram_xy[1]
    if z_count > 2:
        pl.semaphore_wait(ready.at[z_count - 3], line_count)
    line_copies = [
        send(gram_line.at[0], gram_line.at[z_count - hop], z_peer(hop))
        for hop in range(1, z_count)
    ]
    join(3)
    for copy in line_copies:
        copy.wait()
    for hop in range(z_count):
        place = lax.rem(z + hop, z_count)
        gram_pair[0, pl.ds(pl.multiple_of(place * share, share), share), :] = gram_line[hop]
    g_full = send(gram_pair.at[0], gram_pair.at[1], pair_peer)
    g_full.wait()
    gram_full[own_rows, :] = gram_pair[0] * scale_gram
    gram_full[other_rows, :] = gram_pair[1] * scale_gram

    def split(value):
        high = value.astype(bf16)
        return high, (value - high.astype(f32)).astype(bf16)

    def total(value):
        return jnp.sum(jnp.sum(value, axis=0, keepdims=True), axis=1, keepdims=True)

    def two_sided(matrix):
        matrix_high, matrix_low = split(matrix)
        matrix_both = jnp.concatenate([matrix_high, matrix_low], axis=0)

        def apply(value):
            high, low_part = split(value)
            both = jnp.dot(matrix_both, high, preferred_element_type=f32)
            inner = both[:width] + (
                both[width:] + jnp.dot(matrix_high, low_part, preferred_element_type=f32)
            )
            high, low_part = split(inner)
            both = jnp.dot(
                jnp.concatenate([high, low_part], axis=0),
                matrix_high,
                preferred_element_type=f32,
            )
            return both[:width] + (
                both[width:] + jnp.dot(high, matrix_low, preferred_element_type=f32)
            )

        return apply

    gram = gram_full[...]
    gram_high, gram_low = split(gram)
    gram_twice = jnp.dot(gram_high, gram_high, preferred_element_type=f32) + (
        jnp.dot(gram_high, gram_low, preferred_element_type=f32)
        + jnp.dot(gram_low, gram_high, preferred_element_type=f32)
    )
    once, twice = two_sided(gram), two_sided(gram_twice)
    a_side.wait()
    b_side.wait()
    a_last.wait()
    b_last.wait()
    basis[0, :half, :] = ((own_sum[3, :half, :] + first_a[1]) + second_a[1]) * scale_target
    basis[0, half:, :] = ((own_sum[3, half:, :] + first_b[1]) + second_b[1]) * scale_target

    lane = lax.broadcasted_iota(jnp.int32, (1, 128), 1)
    record = jnp.zeros((1, 128), f32)

    def noted(record, place, value):
        return jnp.where(lane == place, value, record)

    def sized(vector):
        square = total(vector * vector)
        inverse = jnp.where(square > 0.0, lax.rsqrt(square), 0.0)
        return inverse, square * inverse

    inverses, lengths, diagonals = [], [], []
    for index in range(0, ITERS, 2):
        vector = basis[index]
        image = once(vector)
        image_twice = twice(vector)
        inverse, length = sized(vector)
        diagonal = (total(vector * image) * inverse) * inverse
        following = (image - diagonal * vector) * inverse
        beyond = (image_twice - diagonal * image) * inverse
        if index > 0:
            ratio = length * inverses[-1]
            following = following - ratio * basis[index - 1]
            beyond = beyond - ratio * mapped
        mapped = beyond
        basis[index + 1] = following
        next_inverse, next_length = sized(following)
        next_diagonal = (total(following * beyond) * next_inverse) * next_inverse
        basis[index + 2] = (beyond - next_diagonal * following) * next_inverse - (
            next_length * inverse
        ) * vector
        inverses += [inverse, next_inverse]
        lengths += [length, next_length]
        diagonals += [diagonal + ridge_weight, next_diagonal + ridge_weight]
        for place in (index, index + 1):
            record = noted(record, place, diagonals[place])
            record = noted(record, ITERS + place, lengths[place])
        if index + 4 == ITERS:
            early[0] = record
            early_copy = spread(early)
    late[0] = record
    late_copy = spread(late)
    inverses.append(jnp.ones((1, 1), f32))
    lengths.append(jnp.ones((1, 1), f32))

    def lanes_of(table):
        lines = table[...].reshape(8 * z_count, 128)
        blank_lines = jnp.zeros((128 - 8 * z_count, 128), f32)
        return jnp.concatenate([lines, blank_lines], axis=0).T

    def reduced(rows):
        added = rows[0]
        for row in rows[1:]:
            added = added + row
        return jnp.sum(added, axis=1, keepdims=True)

    def small_map(rows, alpha, beta):
        count = len(rows)
        made = []
        for j in range(min(count + 1, len(beta))):
            entry = None
            if j < count:
                entry = alpha[j] * rows[j]
            if j > 0:
                term = beta[j] * rows[j - 1]
                entry = term if entry is None else entry + term
            if j + 1 < count:
                entry = entry + beta[j + 1] * rows[j + 1]
            made.append(entry)
        return made

    def mixed_sum(first, ratio, second):
        return [
            one + ratio * second[j] if j < len(second) else one for j, one in enumerate(first)
        ]

    def products(residual, image):
        return (
            reduced([row * row for row in residual]),
            reduced([row * image[j] for j, row in enumerate(residual)]),
        )

    early_copy.wait()
    filled = lanes_of(early)
    known = ITERS - 2
    alpha = [filled[j : j + 1, :] for j in range(known)]
    beta = [filled[ITERS + j : ITERS + j + 1, :] for j in range(known)]
    residual = [beta[0]]
    image = small_map(residual, alpha, beta)
    norm_now, product = products(residual, image)
    step_size = norm_now / product
    direction, along = residual, image
    fitted = []
    for index in range(known):
        if index == 0:
            fitted = [step_size * row for row in direction]
        else:
            fitted = [
                fitted[j] + step_size * row if j < len(fitted) else step_size * row
                for j, row in enumerate(direction)
            ]
        residual = [
            residual[j] - step_size * row if j < len(residual) else -(step_size * row)
            for j, row in enumerate(along)
        ]
        if index + 1 < known:
            image = small_map(residual, alpha, beta)
            norm_next, product = products(residual, image)
            ratio = norm_next / norm_now
            step_size = norm_next / (product - ratio * norm_next / step_size)
            direction = mixed_sum(residual, ratio, direction)
            along = mixed_sum(image, ratio, along)
            norm_now = norm_next

    def own(rows):
        return [row[:, 0:1] for row in rows]

    own_step = step_size[:, 0:1]
    own_direction = own(direction)
    own_along = own(along) + [lengths[known] * own_direction[-1]]
    own_residual = own(residual) + [-(own_step * own_along[-1])]
    own_image = small_map(own_residual, diagonals, lengths)
    weight_sets = (
        own(fitted),
        own_direction,
        own_residual,
        own_along,
        own_image,
        small_map(own_along, diagonals, lengths),
        small_map(own_image, diagonals, lengths),
    )
    for place, weights in enumerate(weight_sets):
        added = (weights[0] * inverses[0]) * basis[0]
        for j in range(1, len(weights)):
            added = added + (weights[j] * inverses[j]) * basis[j]
        pieces[place] = added

    late_copy.wait()
    filled = lanes_of(late)
    alpha += [filled[j : j + 1, :] for j in range(known, ITERS)]
    beta += [filled[ITERS + j : ITERS + j + 1, :] for j in range(known, ITERS)]
    beta.append(jnp.ones((1, 128), f32))
    along = along + [beta[known] * direction[-1]]
    residual = residual + [-(step_size * along[-1])]
    image = small_map(residual, alpha, beta)
    norm_next, product = products(residual, image)
    ratio = norm_next / norm_now
    step_next = norm_next / (product - ratio * norm_next / step_size)
    residual = [
        residual[j] - step_next * row if j < len(residual) else -(step_next * row)
        for j, row in enumerate(mixed_sum(image, ratio, along))
    ]
    norm_last, product = products(residual, small_map(residual, alpha, beta))
    ratio_last = norm_last / norm_next
    step_last = norm_last / (product - ratio_last * norm_last / step_next)
    longer = step_next + step_last * ratio_last
    both_steps = step_last * step_next
    for place, value in enumerate(
        (longer + step_last, longer * ratio, both_steps, both_steps * ratio)
    ):
        mix_ref[place : place + 1, :] = jnp.broadcast_to(value, (1, 128))


def finish_kernel(pieces, mix_ref, fit_hbm, res_hbm, fit_rows, res_rows, fit_sem, res_sem):
    mixes = [mix_ref[place : place + 1, 0:1] for place in range(4)]
    height = fit_rows.shape[0] // CHUNKS
    copies = []
    for slot in range(CHUNKS):
        rows = pl.ds(slot * height, height)
        fitted, direction, residual, along, image, second_along, second_image = [
            pieces[place, slot * height : (slot + 1) * height, :] for place in range(PIECES)
        ]
        fit_rows[rows, :] = (
            fitted
            + mixes[0] * residual
            + mixes[1] * direction
            - mixes[2] * image
            - mixes[3] * along
        )
        copies.append(
            pltpu.make_async_copy(fit_rows.at[rows], fit_hbm.at[0, rows], fit_sem.at[slot])
        )
        copies[-1].start()
        res_rows[rows, :] = (
            residual
            - mixes[0] * image
            - mixes[1] * along
            + mixes[2] * second_image
            + mixes[3] * second_along
        )
        copies.append(
            pltpu.make_async_copy(res_rows.at[rows], res_hbm.at[0, rows], res_sem.at[slot])
        )
        copies[-1].start()
    for copy in copies:
        copy.wait()


def fused_body(factors, heads, tails, values):
    shards = lax.axis_size(("ent", "blk"))
    z_count = lax.axis_size("rel")
    ent_dev, width = factors.shape
    triples = heads.shape[3]
    half = width // 2
    f32, bf16 = jnp.float32, jnp.bfloat16
    vmem = pl.BlockSpec(memory_space=pltpu.VMEM)
    share = half // z_count
    pieces, mix = pl.pallas_call(
        functools.partial(
            fused_kernel, z_count, 1.0 / (ent_dev * shards), 1.0 / math.sqrt(shards * triples)
        ),
        out_shape=(pltpu.VMEM((PIECES, width, width), f32), pltpu.VMEM((8, 128), f32)),
        in_specs=[pl.BlockSpec(memory_space=pl.ANY)] * 4,
        out_specs=(vmem, vmem),
        scratch_shapes=[
            pltpu.VMEM(factors.shape, bf16),
            pltpu.VMEM(heads.shape, jnp.int32),
            pltpu.VMEM(tails.shape, jnp.int32),
            pltpu.VMEM(values.shape, f32),
            pltpu.SMEM(heads.shape, jnp.int32),
            pltpu.SMEM(tails.shape, jnp.int32),
            pltpu.SMEM((1,) + heads.shape[1:], jnp.int32),
            pltpu.SMEM((1,) + heads.shape[1:], jnp.int32),
            pltpu.SemaphoreType.DMA((CHUNKS,)),
            pltpu.SemaphoreType.DMA((7,)),
            pltpu.SemaphoreType.REGULAR((max(z_count - 2, 1),)),
            pltpu.VMEM((ent_dev // tile_width, width, tile_width), bf16),
            pltpu.VMEM((width, triples), bf16),
            pltpu.VMEM((width, triples), bf16),
            pltpu.VMEM((width, width), f32),
            pltpu.VMEM((share, width), f32),
            pltpu.VMEM((2, share, width), f32),
            pltpu.VMEM((2, share, width), f32),
            pltpu.VMEM((z_count, share, width), f32),
            pltpu.VMEM((width, width), f32),
            pltpu.VMEM((2, half, width), f32),
            pltpu.VMEM((4, width, width), f32),
            pltpu.VMEM((4, width, width), f32),
            pltpu.VMEM((4, width, width), f32),
            pltpu.VMEM((2, half, width), f32),
            pltpu.VMEM((2, half, width), f32),
            pltpu.VMEM((2, half, width), f32),
            pltpu.VMEM((2, half, width), f32),
            pltpu.VMEM((ITERS + 1, width, width), f32),
            pltpu.VMEM((8 * z_count, 1, 128), f32),
            pltpu.VMEM((8 * z_count, 1, 128), f32),
            pltpu.SemaphoreType.DMA((COPIES,)),
            pltpu.SemaphoreType.DMA((COPIES,)),
        ],
        compiler_params=pltpu.CompilerParams(collective_id=0, has_side_effects=True),
    )(factors, heads, tails, values)
    out = jax.ShapeDtypeStruct((1, width, width), f32)
    anywhere = pl.BlockSpec(memory_space=pl.ANY)
    return pl.pallas_call(
        finish_kernel,
        out_shape=(out, out),
        in_specs=[vmem, vmem],
        out_specs=(anywhere, anywhere),
        scratch_shapes=[
            pltpu.VMEM((width, width), f32),
            pltpu.VMEM((width, width), f32),
            pltpu.SemaphoreType.DMA((CHUNKS,)),
            pltpu.SemaphoreType.DMA((CHUNKS,)),
        ],
        compiler_params=pltpu.CompilerParams(vmem_limit_bytes=16 * width * width * 4),
    )(pieces, mix)


def solution(mesh):
    placed = (
        P(("ent", "blk"), None),
        P(None, "rel", None, ("ent", "blk")),
        P(None, "rel", None, ("ent", "blk")),
        P(None, "rel", None, ("ent", "blk")),
    )
    sizes = dict(mesh.shape)
    fused = sizes["ent"] == 2 and sizes["blk"] == 4 and sizes["rel"] in (2, 4, 8)
    return jax.shard_map(
        fused_body if fused else body,
        mesh=mesh,
        in_specs=placed,
        out_specs=(P(("ent", "blk", "rel"), None, None), P(("ent", "blk", "rel"), None, None)),
        check_vma=False,
    )
```

```python
import functools
import math

import jax
import jax.numpy as jnp
from jax import lax
from jax.experimental import pallas as pl
from jax.experimental.pallas import tpu as pltpu
from jax.sharding import PartitionSpec as P

ITERS = 8


ridge_weight = 0.01
tile_width = 128


def apply_normal(gram_matrix, stacked):
    left_side = jnp.einsum("ab,kbc->kac", gram_matrix, stacked, precision=lax.Precision.HIGHEST)
    return (
        jnp.einsum("kac,cd->kad", left_side, gram_matrix, precision=lax.Precision.HIGHEST)
        + ridge_weight * stacked
    )


def two_products(residual, image_map):
    return lax.psum(
        (jnp.sum(residual * residual), jnp.sum(residual * image_map)), ("ent", "blk", "rel")
    )


def select_rows(entity_ids, block_table):
    group_size, width = entity_ids.shape
    tile_count = width // tile_width
    block_count = block_table.shape[0]
    tiled_ids = entity_ids.reshape(group_size, tile_count, tile_width)
    block_of = tiled_ids[:, :, 0] // tile_width
    block_pick = (
        block_of[:, :, None] == jnp.arange(block_count, dtype=jnp.int32)[None, None, :]
    ).astype(jnp.bfloat16)
    chosen = jnp.einsum(
        "gtb,bcr->gtcr", block_pick, block_table, preferred_element_type=jnp.float32
    ).astype(jnp.bfloat16)
    inside = tiled_ids % tile_width
    slot_pick = (
        inside[:, :, :, None] == jnp.arange(tile_width, dtype=jnp.int32)[None, None, None, :]
    ).astype(jnp.bfloat16)
    return jnp.einsum("gtoc,gtcr->gtor", slot_pick, chosen, preferred_element_type=jnp.float32)


def body(factors, heads, tails, values):
    shards = lax.axis_size(("ent", "blk"))
    ent_dev = factors.shape[0]
    rank_width = factors.shape[1]
    triple_count = heads.shape[3]
    relation_rows = heads.shape[0] * heads.shape[2]
    norm_scale = 1.0 / math.sqrt(shards * triple_count)
    gram_total = lax.psum(
        jnp.dot(factors.T, factors, preferred_element_type=jnp.float32), ("ent", "blk")
    )
    gram_matrix = gram_total / (ent_dev * shards)
    block_table = factors.reshape(ent_dev // tile_width, tile_width, rank_width)
    head_ids = heads.reshape(relation_rows, triple_count)
    tail_ids = tails.reshape(relation_rows, triple_count)
    weights = values.reshape(relation_rows, triple_count)

    def grouped(operands):
        head_group, tail_group, weight_group = operands
        group_size = head_group.shape[0]
        tile_count = triple_count // tile_width
        head_rows = select_rows(head_group, block_table)
        weighted = (
            weight_group.reshape(group_size, tile_count, tile_width)[:, :, :, None] * head_rows
        ).astype(jnp.bfloat16)
        tail_rows = select_rows(tail_group, block_table).astype(jnp.bfloat16)
        product = jnp.einsum(
            "gtci,gtcj->gij", weighted, tail_rows, preferred_element_type=jnp.float32
        )
        return product * norm_scale

    own_rows = relation_rows // shards
    group_size = math.gcd(own_rows * lax.axis_size(("ent", "blk")), 4)
    group_total = own_rows * lax.axis_size(("ent", "blk")) // group_size
    shaped = (
        head_ids.reshape(group_total, group_size, triple_count),
        tail_ids.reshape(group_total, group_size, triple_count),
        weights.reshape(group_total, group_size, triple_count),
    )
    results = lax.map(grouped, shaped)
    target = lax.psum_scatter(
        results.reshape(own_rows * lax.axis_size(("ent", "blk")), rank_width, rank_width),
        ("ent", "blk"),
        scatter_dimension=0,
        tiled=True,
    )
    fitted = jnp.zeros_like(target)
    residual = target
    image_map = apply_normal(gram_matrix, residual)
    norm_now, product = two_products(residual, image_map)
    step_size = norm_now / product
    direction = residual
    along = image_map
    for step_index in range(ITERS):
        fitted = fitted + step_size * direction
        residual = residual - step_size * along
        if step_index + 1 < ITERS:
            image_map = apply_normal(gram_matrix, residual)
            norm_next, product = two_products(residual, image_map)
            ratio_next = norm_next / norm_now
            step_size = norm_next / (product - ratio_next * norm_next / step_size)
            direction = residual + ratio_next * direction
            along = image_map + ratio_next * along
            norm_now = norm_next
    return (fitted, residual)


MESH = pl.DeviceIdType.MESH
COPIES = 21
CHUNKS = 4
STRIP = 32


def fused_kernel(
    z_count, scale_gram, scale_target,
    factors_hbm, heads_hbm, tails_hbm, values_hbm,
    basis, mix_ref,
    factors_ref, heads_ref, tails_ref, values_ref, head_ids, tail_ids,
    first_heads, first_tails, factor_sem, load_sem, ready,
    turned, left_rows, right_rows,
    gram_part, gram_in, gram_half, gram_xy, gram_line, gram_full, gram_pair,
    pair_out, pair_in, own_sum, first_a, first_b, second_a, second_b,
    early, late, send_sem, recv_sem,
):
    f32, bf16 = jnp.float32, jnp.bfloat16
    width = factors_ref.shape[1]
    half = width // 2
    share = half // z_count
    part = share // 2
    triples = heads_ref.shape[3]
    e = lax.axis_index("ent")
    b = lax.axis_index("blk")
    z = lax.axis_index("rel")
    y = b // 2
    c = b % 2
    pair_peer = (e, y * 2 + 1 - c, z)
    x_peer = (1 - e, b, z)
    y_peer = (e, (1 - y) * 2 + c, z)

    def group_peer(mask):
        me, my, mc = mask // 4, (mask // 2) % 2, mask % 2
        return (
            (1 - e) if me else e,
            ((1 - y) if my else y) * 2 + ((1 - c) if mc else c),
            z,
        )

    def z_peer(hop):
        return (e, b, lax.rem(z + hop, z_count))

    near = [group_peer(m) for m in (1, 2, 4)]
    inner = ((z > 0, -1), (z < z_count - 1, 1))

    def tell(semaphore):
        for present, hop in inner:
            @pl.when(present)
            def _():
                pl.semaphore_signal(
                    semaphore, inc=1, device_id=(e, b, z + hop), device_id_type=MESH
                )

    line_count = jnp.where(z > 0, 1, 0) + jnp.where(z < z_count - 1, 1, 0)
    barrier = pltpu.get_barrier_semaphore()
    for peer in near:
        pl.semaphore_signal(barrier, inc=1, device_id=peer, device_id_type=MESH)
    tell(barrier)
    first_q = (1 - e) * 4 + (1 - y) * 2 + 1 - c
    chunk = factors_ref.shape[0] // CHUNKS
    factor_loads = []
    for slot in range(CHUNKS):
        rows = pl.ds(slot * chunk, chunk)
        factor_loads.append(
            pltpu.make_async_copy(
                factors_hbm.at[rows], factors_ref.at[rows], factor_sem.at[slot]
            )
        )
        factor_loads[-1].start()
    loads = []
    for slot, (source, dest) in enumerate(
        (
            (heads_hbm.at[pl.ds(first_q, 1)], first_heads),
            (tails_hbm.at[pl.ds(first_q, 1)], first_tails),
            (heads_hbm, heads_ref),
            (values_hbm, values_ref),
            (tails_hbm, tails_ref),
            (heads_hbm, head_ids),
            (tails_hbm, tail_ids),
        )
    ):
        loads.append(pltpu.make_async_copy(source, dest, load_sem.at[slot]))
        loads[-1].start()

    counter = [0]

    def spare():
        slot = counter[0]
        counter[0] += 1
        return send_sem.at[slot], recv_sem.at[slot]

    def copy_to(source, dest, peer, pair):
        return pltpu.make_async_remote_copy(
            src_ref=source, dst_ref=dest, send_sem=pair[0], recv_sem=pair[1],
            device_id=peer, device_id_type=MESH,
        )

    def send(source, dest, peer):
        copy = copy_to(source, dest, peer, spare())
        copy.start()
        return copy

    far_peers = [
        (m, hop) for hop in (*range(1, z_count), 0) for m in (7, 6, 5, 3, 4, 2, 1, 0) if m or hop
    ]

    def spread(table):
        pair = spare()
        for m, hop in far_peers:
            peer = group_peer(m)[:2] + (lax.rem(z + hop, z_count),)
            place = m * z_count + (z_count - hop) % z_count
            copy_to(table.at[0], table.at[place], peer, pair).start()
        others = table.at[pl.ds(1, 8 * z_count - 1)]
        return copy_to(others, others, pair_peer, pair)

    flipped = []
    for slot in range(CHUNKS):
        factor_loads[slot].wait()
        flipped.append(factors_ref[slot * chunk : (slot + 1) * chunk, :].T)
        for step in range(chunk // tile_width):
            turned[slot * (chunk // tile_width) + step] = flipped[-1][
                :, step * tile_width : (step + 1) * tile_width
            ]
    own_rows = pl.ds(pl.multiple_of(c * half, half), half)
    other_rows = pl.ds(pl.multiple_of((1 - c) * half, half), half)
    own_share = pl.ds(pl.multiple_of(c * half + z * share, share), share)
    other_share = pl.ds(pl.multiple_of((1 - c) * half + z * share, share), share)

    row_number = lax.broadcasted_iota(jnp.int32, (tile_width, tile_width), 0)
    blank = jnp.zeros((tile_width, tile_width), bf16)

    def gathered(ids_ref, scalar_ref, q, place, first):
        picks, blocks = [], []
        for tile in (first, first + 1):
            start = tile * tile_width
            inside = lax.rem(ids_ref[q, 0, :, start : start + tile_width], tile_width)
            picks.append(jnp.where(row_number == inside, 1.0, 0.0).astype(bf16))
            blocks.append(turned[lax.div(scalar_ref[place, 0, 0, start], tile_width)])
        mixed = jnp.concatenate(
            [
                jnp.concatenate([picks[0], blank], axis=1),
                jnp.concatenate([blank, picks[1]], axis=1),
            ],
            axis=0,
        )
        return jnp.dot(jnp.concatenate(blocks, axis=1), mixed, preferred_element_type=f32)

    def partial(pe, py, pc, head_blocks=head_ids, tail_blocks=tail_ids, place=None):
        q = pe * 4 + py * 2 + pc
        place = q if place is None else place
        for first in range(0, triples // tile_width, 2):
            cols = slice(first * tile_width, (first + 2) * tile_width)
            rows = gathered(heads_ref, head_blocks, q, place, first)
            left_rows[:, cols] = (values_ref[q, 0, :, cols] * rows).astype(bf16)
            right_rows[:, cols] = gathered(tails_ref, tail_blocks, q, place, first).astype(bf16)
        return lax.dot_general(
            left_rows[...], right_rows[...], (((1,), (1,)), ((), ())), preferred_element_type=f32
        )

    targets = ((1 - e, 1 - y), (1 - e, y), (e, 1 - y), (e, y))
    pair_copies = []

    def give(index):
        pe, py = targets[index]
        pair_out[index] = partial(pe, py, 1 - c)
        pair_copies.append(send(pair_out.at[index], pair_in.at[index], pair_peer))

    def keep(index):
        pe, py = targets[index]
        own_sum[index] = partial(pe, py, c)

    def join(index):
        pair_copies[index].wait()
        own_sum[index] = own_sum[index] + pair_in[index]

    top, low = pl.ds(0, half), pl.ds(half, half)
    for load in loads[:5]:
        load.wait()
    pair_out[0] = partial(1 - e, 1 - y, 1 - c, first_heads, first_tails, 0)
    pl.semaphore_wait(barrier, len(near) + line_count)
    pair_copies.append(send(pair_out.at[0], pair_in.at[0], pair_peer))
    if z_count > 2:
        tell(ready.at[0])
    gram_part[...] = jnp.dot(
        jnp.concatenate(flipped, axis=1), factors_ref[...], preferred_element_type=f32
    )
    g_pair = send(gram_part.at[other_share], gram_in, pair_peer)
    for load in loads[5:]:
        load.wait()
    keep(0)
    g_pair.wait()
    gram_half[0] = gram_part[own_share, :] + gram_in[...]
    upper, lower = pl.ds(0, part), pl.ds(part, part)
    g_a1 = send(gram_half.at[0, upper], gram_xy.at[0, upper], x_peer)
    g_b1 = send(gram_half.at[0, lower], gram_xy.at[0, lower], y_peer)
    join(0)
    a_diag = send(own_sum.at[0, top], first_a.at[0], x_peer)
    b_diag = send(own_sum.at[0, low], first_b.at[0], y_peer)
    give(1)
    give(2)
    for step in range(1, z_count - 2):
        pl.semaphore_wait(ready.at[step - 1], line_count)
        tell(ready.at[step])
    keep(1)
    g_a1.wait()
    g_b1.wait()
    gram_half[1] = gram_half[0] + gram_xy[0]
    g_a2 = send(gram_half.at[1, upper], gram_xy.at[1, upper], y_peer)
    g_b2 = send(gram_half.at[1, lower], gram_xy.at[1, lower], x_peer)
    join(1)
    a_side = send(own_sum.at[1, top], first_a.at[1], x_peer)
    keep(2)
    join(2)
    b_side = send(own_sum.at[2, low], first_b.at[1], y_peer)
    give(3)
    keep(3)
    a_diag.wait()
    second_a[0] = own_sum[2, :half, :] + first_a[0]
    a_last = send(second_a.at[0], second_a.at[1], y_peer)
    b_diag.wait()
    second_b[0] = own_sum[1, half:, :] + first_b[0]
    b_last = send(second_b.at[0], second_b.at[1], x_peer)
    g_a2.wait()
    g_b2.wait()
    gram_line[0] = gram_half[1] + gram_xy[1]
    if z_count > 2:
        pl.semaphore_wait(ready.at[z_count - 3], line_count)
    line_copies = [
        send(gram_line.at[0], gram_line.at[z_count - hop], z_peer(hop))
        for hop in range(1, z_count)
    ]
    join(3)
    for copy in line_copies:
        copy.wait()
    for hop in range(z_count):
        place = lax.rem(z + hop, z_count)
        gram_pair[0, pl.ds(pl.multiple_of(place * share, share), share), :] = gram_line[hop]
    g_full = send(gram_pair.at[0], gram_pair.at[1], pair_peer)
    g_full.wait()
    gram_full[own_rows, :] = gram_pair[0] * scale_gram
    gram_full[other_rows, :] = gram_pair[1] * scale_gram

    def split(value):
        high = value.astype(bf16)
        return high, (value - high.astype(f32)).astype(bf16)

    def total(value):
        return jnp.sum(jnp.sum(value, axis=0, keepdims=True), axis=1, keepdims=True)

    def two_sided(matrix):
        matrix_high, matrix_low = split(matrix)
        matrix_both = jnp.concatenate([matrix_high, matrix_low], axis=0)

        def left(value):
            high, low_part = split(value)
            both = jnp.dot(matrix_both, high, preferred_element_type=f32)
            return both[:width] + (
                both[width:] + jnp.dot(matrix_high, low_part, preferred_element_type=f32)
            )

        def right(value):
            high, low_part = split(value)
            both = jnp.dot(
                jnp.concatenate([high, low_part], axis=0),
                matrix_high,
                preferred_element_type=f32,
            )
            return both[:width] + (
                both[width:] + jnp.dot(high, matrix_low, preferred_element_type=f32)
            )

        return left, right

    gram = gram_full[...]
    gram_high, gram_low = split(gram)
    gram_twice = jnp.dot(gram_high, gram_high, preferred_element_type=f32) + (
        jnp.dot(gram_high, gram_low, preferred_element_type=f32)
        + jnp.dot(gram_low, gram_high, preferred_element_type=f32)
    )
    once, twice = two_sided(gram), two_sided(gram_twice)
    a_side.wait()
    b_side.wait()
    a_last.wait()
    b_last.wait_recv()
    basis[0, :half, :] = ((own_sum[3, :half, :] + first_a[1]) + second_a[1]) * scale_target
    basis[0, half:, :] = ((own_sum[3, half:, :] + first_b[1]) + second_b[1]) * scale_target

    lane = lax.broadcasted_iota(jnp.int32, (1, 128), 1)
    record = jnp.zeros((1, 128), f32)

    def noted(record, place, value):
        return jnp.where(lane == place, value, record)

    def sized(vector):
        square = total(vector * vector)
        inverse = jnp.where(square > 0.0, lax.rsqrt(square), 0.0)
        return inverse, square * inverse

    inverses, lengths, diagonals = [], [], []
    for index in range(0, ITERS, 2):
        vector = basis[index]
        inner, inner_twice = once[0](vector), twice[0](vector)
        if index + 2 == ITERS:
            b_last.wait_send()
        image, image_twice = once[1](inner), twice[1](inner_twice)
        inverse, length = sized(vector)
        diagonal = (total(vector * image) * inverse) * inverse
        following = (image - diagonal * vector) * inverse
        beyond = (image_twice - diagonal * image) * inverse
        if index > 0:
            ratio = length * inverses[-1]
            following = following - ratio * basis[index - 1]
            beyond = beyond - ratio * mapped
        mapped = beyond
        basis[index + 1] = following
        next_inverse, next_length = sized(following)
        next_diagonal = (total(following * beyond) * next_inverse) * next_inverse
        basis[index + 2] = (beyond - next_diagonal * following) * next_inverse - (
            next_length * inverse
        ) * vector
        inverses += [inverse, next_inverse]
        lengths += [length, next_length]
        diagonals += [diagonal + ridge_weight, next_diagonal + ridge_weight]
        for place in (index, index + 1):
            record = noted(record, place, diagonals[place])
            record = noted(record, ITERS + place, lengths[place])
        if index + 4 == ITERS:
            early[0] = record
            early_copy = spread(early)
    late[0] = record
    late_copy = spread(late)
    inverses.append(jnp.ones((1, 1), f32))
    lengths.append(jnp.ones((1, 1), f32))

    def lanes_of(table):
        lines = table[...].reshape(8 * z_count, 128)
        blank_lines = jnp.zeros((128 - 8 * z_count, 128), f32)
        return jnp.concatenate([lines, blank_lines], axis=0).T

    def reduced(rows):
        added = rows[0]
        for row in rows[1:]:
            added = added + row
        return jnp.sum(added, axis=1, keepdims=True)

    def small_map(rows, alpha, beta):
        count = len(rows)
        made = []
        for j in range(min(count + 1, len(beta))):
            entry = None
            if j < count:
                entry = alpha[j] * rows[j]
            if j > 0:
                term = beta[j] * rows[j - 1]
                entry = term if entry is None else entry + term
            if j + 1 < count:
                entry = entry + beta[j + 1] * rows[j + 1]
            made.append(entry)
        return made

    def mixed_sum(first, ratio, second):
        return [
            one + ratio * second[j] if j < len(second) else one for j, one in enumerate(first)
        ]

    def products(residual, image):
        return (
            reduced([row * row for row in residual]),
            reduced([row * image[j] for j, row in enumerate(residual)]),
        )

    early_copy.wait()
    filled = lanes_of(early)
    known = ITERS - 2
    alpha = [filled[j : j + 1, :] for j in range(known)]
    beta = [filled[ITERS + j : ITERS + j + 1, :] for j in range(known)]
    residual = [beta[0]]
    image = small_map(residual, alpha, beta)
    norm_now, product = products(residual, image)
    step_size = norm_now / product
    direction, along = residual, image
    fitted = []
    for index in range(known):
        if index == 0:
            fitted = [step_size * row for row in direction]
        else:
            fitted = [
                fitted[j] + step_size * row if j < len(fitted) else step_size * row
                for j, row in enumerate(direction)
            ]
        residual = [
            residual[j] - step_size * row if j < len(residual) else -(step_size * row)
            for j, row in enumerate(along)
        ]
        if index + 1 < known:
            image = small_map(residual, alpha, beta)
            norm_next, product = products(residual, image)
            ratio = norm_next / norm_now
            step_size = norm_next / (product - ratio * norm_next / step_size)
            direction = mixed_sum(residual, ratio, direction)
            along = mixed_sum(image, ratio, along)
            norm_now = norm_next

    late_copy.wait()
    filled = lanes_of(late)
    alpha += [filled[j : j + 1, :] for j in range(known, ITERS)]
    beta += [filled[ITERS + j : ITERS + j + 1, :] for j in range(known, ITERS)]
    beta.append(jnp.ones((1, 128), f32))
    along = along + [beta[known] * direction[-1]]
    residual = residual + [-(step_size * along[-1])]
    image = small_map(residual, alpha, beta)
    norm_next, product = products(residual, image)
    ratio = norm_next / norm_now
    step_next = norm_next / (product - ratio * norm_next / step_size)
    residual_before, image_before = residual, image
    residual = [
        residual[j] - step_next * row if j < len(residual) else -(step_next * row)
        for j, row in enumerate(mixed_sum(image, ratio, along))
    ]
    fitted = [
        fitted[j] + step_next * row if j < len(fitted) else step_next * row
        for j, row in enumerate(mixed_sum(residual_before, ratio, direction))
    ]
    image = small_map(residual, alpha, beta)
    norm_last, product = products(residual, image)
    ratio_last = norm_last / norm_next
    step_last = norm_last / (product - ratio_last * norm_last / step_next)
    direction = mixed_sum(residual, ratio_last, mixed_sum(residual_before, ratio, direction))
    along = mixed_sum(image, ratio_last, mixed_sum(image_before, ratio, along))
    fitted = [
        fitted[j] + step_last * row if j < len(fitted) else step_last * row
        for j, row in enumerate(direction)
    ]
    residual = [
        residual[j] - step_last * row if j < len(residual) else -(step_last * row)
        for j, row in enumerate(along)
    ]
    for place, row in enumerate(fitted + residual):
        weight = row[:, 0:1] * inverses[place if place < ITERS else place - ITERS]
        mix_ref[place : place + 1, :] = jnp.broadcast_to(weight, (1, width))


def finish_kernel(basis, mix_ref, fit_hbm, res_hbm, fit_rows, res_rows, fit_sem, res_sem):
    count = basis.shape[0] - 1
    weights = [mix_ref[place : place + 1, :] for place in range(2 * count + 1)]
    height = fit_rows.shape[0] // CHUNKS
    copies = []
    for slot in range(CHUNKS):
        for first in range(slot * height, (slot + 1) * height, STRIP):
            strip = slice(first, first + STRIP)
            vector = basis[0, strip, :]
            fit, res = weights[0] * vector, weights[count] * vector
            for j in range(1, count + 1):
                vector = basis[j, strip, :]
                res = res + weights[count + j] * vector
                if j < count:
                    fit = fit + weights[j] * vector
            fit_rows[strip, :] = fit
            res_rows[strip, :] = res
        rows = pl.ds(slot * height, height)
        for source, dest, sem in ((fit_rows, fit_hbm, fit_sem), (res_rows, res_hbm, res_sem)):
            copies.append(
                pltpu.make_async_copy(source.at[rows], dest.at[0, rows], sem.at[slot])
            )
            copies[-1].start()
    for copy in copies:
        copy.wait()


def fused_body(factors, heads, tails, values):
    shards = lax.axis_size(("ent", "blk"))
    z_count = lax.axis_size("rel")
    ent_dev, width = factors.shape
    triples = heads.shape[3]
    half = width // 2
    f32, bf16 = jnp.float32, jnp.bfloat16
    vmem = pl.BlockSpec(memory_space=pltpu.VMEM)
    share = half // z_count
    basis, mix = pl.pallas_call(
        functools.partial(
            fused_kernel, z_count, 1.0 / (ent_dev * shards), 1.0 / math.sqrt(shards * triples)
        ),
        out_shape=(
            pltpu.VMEM((ITERS + 1, width, width), f32),
            pltpu.VMEM((3 * ITERS, width), f32),
        ),
        in_specs=[pl.BlockSpec(memory_space=pl.ANY)] * 4,
        out_specs=(vmem, vmem),
        scratch_shapes=[
            pltpu.VMEM(factors.shape, bf16),
            pltpu.VMEM(heads.shape, jnp.int32),
            pltpu.VMEM(tails.shape, jnp.int32),
            pltpu.VMEM(values.shape, f32),
            pltpu.SMEM(heads.shape, jnp.int32),
            pltpu.SMEM(tails.shape, jnp.int32),
            pltpu.SMEM((1,) + heads.shape[1:], jnp.int32),
            pltpu.SMEM((1,) + heads.shape[1:], jnp.int32),
            pltpu.SemaphoreType.DMA((CHUNKS,)),
            pltpu.SemaphoreType.DMA((7,)),
            pltpu.SemaphoreType.REGULAR((max(z_count - 2, 1),)),
            pltpu.VMEM((ent_dev // tile_width, width, tile_width), bf16),
            pltpu.VMEM((width, triples), bf16),
            pltpu.VMEM((width, triples), bf16),
            pltpu.VMEM((width, width), f32),
            pltpu.VMEM((share, width), f32),
            pltpu.VMEM((2, share, width), f32),
            pltpu.VMEM((2, share, width), f32),
            pltpu.VMEM((z_count, share, width), f32),
            pltpu.VMEM((width, width), f32),
            pltpu.VMEM((2, half, width), f32),
            pltpu.VMEM((4, width, width), f32),
            pltpu.VMEM((4, width, width), f32),
            pltpu.VMEM((4, width, width), f32),
            pltpu.VMEM((2, half, width), f32),
            pltpu.VMEM((2, half, width), f32),
            pltpu.VMEM((2, half, width), f32),
            pltpu.VMEM((2, half, width), f32),
            pltpu.VMEM((8 * z_count, 1, 128), f32),
            pltpu.VMEM((8 * z_count, 1, 128), f32),
            pltpu.SemaphoreType.DMA((COPIES,)),
            pltpu.SemaphoreType.DMA((COPIES,)),
        ],
        compiler_params=pltpu.CompilerParams(collective_id=0, has_side_effects=True),
    )(factors, heads, tails, values)
    out = jax.ShapeDtypeStruct((1, width, width), f32)
    anywhere = pl.BlockSpec(memory_space=pl.ANY)
    return pl.pallas_call(
        finish_kernel,
        out_shape=(out, out),
        in_specs=[vmem, vmem],
        out_specs=(anywhere, anywhere),
        scratch_shapes=[
            pltpu.VMEM((width, width), f32),
            pltpu.VMEM((width, width), f32),
            pltpu.SemaphoreType.DMA((CHUNKS,)),
            pltpu.SemaphoreType.DMA((CHUNKS,)),
        ],
        compiler_params=pltpu.CompilerParams(vmem_limit_bytes=16 * width * width * 4),
    )(basis, mix)


def solution(mesh):
    placed = (
        P(("ent", "blk"), None),
        P(None, "rel", None, ("ent", "blk")),
        P(None, "rel", None, ("ent", "blk")),
        P(None, "rel", None, ("ent", "blk")),
    )
    sizes = dict(mesh.shape)
    fused = sizes["ent"] == 2 and sizes["blk"] == 4 and sizes["rel"] in (2, 4, 8)
    return jax.shard_map(
        fused_body if fused else body,
        mesh=mesh,
        in_specs=placed,
        out_specs=(P(("ent", "blk", "rel"), None, None), P(("ent", "blk", "rel"), None, None)),
        check_vma=False,
    )
```

```python
import functools
import math

import jax
import jax.numpy as jnp
from jax import lax
from jax.experimental import pallas as pl
from jax.experimental.pallas import tpu as pltpu
from jax.sharding import PartitionSpec as P

ITERS = 8


ridge_weight = 0.01
tile_width = 128


def apply_normal(gram_matrix, stacked):
    left_side = jnp.einsum("ab,kbc->kac", gram_matrix, stacked, precision=lax.Precision.HIGHEST)
    return (
        jnp.einsum("kac,cd->kad", left_side, gram_matrix, precision=lax.Precision.HIGHEST)
        + ridge_weight * stacked
    )


def two_products(residual, image_map):
    return lax.psum(
        (jnp.sum(residual * residual), jnp.sum(residual * image_map)), ("ent", "blk", "rel")
    )


def select_rows(entity_ids, block_table):
    group_size, width = entity_ids.shape
    tile_count = width // tile_width
    block_count = block_table.shape[0]
    tiled_ids = entity_ids.reshape(group_size, tile_count, tile_width)
    block_of = tiled_ids[:, :, 0] // tile_width
    block_pick = (
        block_of[:, :, None] == jnp.arange(block_count, dtype=jnp.int32)[None, None, :]
    ).astype(jnp.bfloat16)
    chosen = jnp.einsum(
        "gtb,bcr->gtcr", block_pick, block_table, preferred_element_type=jnp.float32
    ).astype(jnp.bfloat16)
    inside = tiled_ids % tile_width
    slot_pick = (
        inside[:, :, :, None] == jnp.arange(tile_width, dtype=jnp.int32)[None, None, None, :]
    ).astype(jnp.bfloat16)
    return jnp.einsum("gtoc,gtcr->gtor", slot_pick, chosen, preferred_element_type=jnp.float32)


def body(factors, heads, tails, values):
    shards = lax.axis_size(("ent", "blk"))
    ent_dev = factors.shape[0]
    rank_width = factors.shape[1]
    triple_count = heads.shape[3]
    relation_rows = heads.shape[0] * heads.shape[2]
    norm_scale = 1.0 / math.sqrt(shards * triple_count)
    gram_total = lax.psum(
        jnp.dot(factors.T, factors, preferred_element_type=jnp.float32), ("ent", "blk")
    )
    gram_matrix = gram_total / (ent_dev * shards)
    block_table = factors.reshape(ent_dev // tile_width, tile_width, rank_width)
    head_ids = heads.reshape(relation_rows, triple_count)
    tail_ids = tails.reshape(relation_rows, triple_count)
    weights = values.reshape(relation_rows, triple_count)

    def grouped(operands):
        head_group, tail_group, weight_group = operands
        group_size = head_group.shape[0]
        tile_count = triple_count // tile_width
        head_rows = select_rows(head_group, block_table)
        weighted = (
            weight_group.reshape(group_size, tile_count, tile_width)[:, :, :, None] * head_rows
        ).astype(jnp.bfloat16)
        tail_rows = select_rows(tail_group, block_table).astype(jnp.bfloat16)
        product = jnp.einsum(
            "gtci,gtcj->gij", weighted, tail_rows, preferred_element_type=jnp.float32
        )
        return product * norm_scale

    own_rows = relation_rows // shards
    group_size = math.gcd(own_rows * lax.axis_size(("ent", "blk")), 4)
    group_total = own_rows * lax.axis_size(("ent", "blk")) // group_size
    shaped = (
        head_ids.reshape(group_total, group_size, triple_count),
        tail_ids.reshape(group_total, group_size, triple_count),
        weights.reshape(group_total, group_size, triple_count),
    )
    results = lax.map(grouped, shaped)
    target = lax.psum_scatter(
        results.reshape(own_rows * lax.axis_size(("ent", "blk")), rank_width, rank_width),
        ("ent", "blk"),
        scatter_dimension=0,
        tiled=True,
    )
    fitted = jnp.zeros_like(target)
    residual = target
    image_map = apply_normal(gram_matrix, residual)
    norm_now, product = two_products(residual, image_map)
    step_size = norm_now / product
    direction = residual
    along = image_map
    for step_index in range(ITERS):
        fitted = fitted + step_size * direction
        residual = residual - step_size * along
        if step_index + 1 < ITERS:
            image_map = apply_normal(gram_matrix, residual)
            norm_next, product = two_products(residual, image_map)
            ratio_next = norm_next / norm_now
            step_size = norm_next / (product - ratio_next * norm_next / step_size)
            direction = residual + ratio_next * direction
            along = image_map + ratio_next * along
            norm_now = norm_next
    return (fitted, residual)


MESH = pl.DeviceIdType.MESH
COPIES = 21
CHUNKS = 4
STRIP = 32
PANEL = 128


def fused_kernel(
    z_count, scale_gram, scale_target,
    factors_hbm, heads_hbm, tails_hbm, values_hbm,
    basis, mix_ref,
    factors_ref, heads_ref, tails_ref, values_ref, head_ids, tail_ids,
    first_heads, first_tails, factor_sem, load_sem, ready,
    turned, left_rows, right_rows,
    gram_part, gram_in, gram_half, gram_xy, gram_line, gram_full, gram_pair,
    pair_out, pair_in, own_sum, first_a, first_b, second_a, second_b,
    factor_left, factor_right, vector_parts, inner_parts, image, image_twice, mapped,
    early, late, send_sem, recv_sem,
):
    f32, bf16 = jnp.float32, jnp.bfloat16
    width = factors_ref.shape[1]
    half = width // 2
    share = half // z_count
    part = share // 2
    triples = heads_ref.shape[3]
    e = lax.axis_index("ent")
    b = lax.axis_index("blk")
    z = lax.axis_index("rel")
    y = b // 2
    c = b % 2
    pair_peer = (e, y * 2 + 1 - c, z)
    x_peer = (1 - e, b, z)
    y_peer = (e, (1 - y) * 2 + c, z)

    def group_peer(mask):
        me, my, mc = mask // 4, (mask // 2) % 2, mask % 2
        return (
            (1 - e) if me else e,
            ((1 - y) if my else y) * 2 + ((1 - c) if mc else c),
            z,
        )

    def z_peer(hop):
        return (e, b, lax.rem(z + hop, z_count))

    near = [group_peer(m) for m in (1, 2, 4)]
    inner = ((z > 0, -1), (z < z_count - 1, 1))

    def tell(semaphore):
        for present, hop in inner:
            @pl.when(present)
            def _():
                pl.semaphore_signal(
                    semaphore, inc=1, device_id=(e, b, z + hop), device_id_type=MESH
                )

    line_count = jnp.where(z > 0, 1, 0) + jnp.where(z < z_count - 1, 1, 0)
    barrier = pltpu.get_barrier_semaphore()
    for peer in near:
        pl.semaphore_signal(barrier, inc=1, device_id=peer, device_id_type=MESH)
    tell(barrier)
    first_q = (1 - e) * 4 + (1 - y) * 2 + 1 - c
    chunk = factors_ref.shape[0] // CHUNKS
    factor_loads = []
    for slot in range(CHUNKS):
        rows = pl.ds(slot * chunk, chunk)
        factor_loads.append(
            pltpu.make_async_copy(
                factors_hbm.at[rows], factors_ref.at[rows], factor_sem.at[slot]
            )
        )
        factor_loads[-1].start()
    loads = []
    for slot, (source, dest) in enumerate(
        (
            (heads_hbm.at[pl.ds(first_q, 1)], first_heads),
            (tails_hbm.at[pl.ds(first_q, 1)], first_tails),
            (heads_hbm, heads_ref),
            (values_hbm, values_ref),
            (tails_hbm, tails_ref),
            (heads_hbm, head_ids),
            (tails_hbm, tail_ids),
        )
    ):
        loads.append(pltpu.make_async_copy(source, dest, load_sem.at[slot]))
        loads[-1].start()

    counter = [0]

    def spare():
        slot = counter[0]
        counter[0] += 1
        return send_sem.at[slot], recv_sem.at[slot]

    def copy_to(source, dest, peer, pair):
        return pltpu.make_async_remote_copy(
            src_ref=source, dst_ref=dest, send_sem=pair[0], recv_sem=pair[1],
            device_id=peer, device_id_type=MESH,
        )

    def send(source, dest, peer):
        copy = copy_to(source, dest, peer, spare())
        copy.start()
        return copy

    far_peers = [
        (m, hop) for hop in (*range(1, z_count), 0) for m in (7, 6, 5, 3, 4, 2, 1, 0) if m or hop
    ]

    def spread(table):
        pair = spare()
        for m, hop in far_peers:
            peer = group_peer(m)[:2] + (lax.rem(z + hop, z_count),)
            place = m * z_count + (z_count - hop) % z_count
            copy_to(table.at[0], table.at[place], peer, pair).start()
        others = table.at[pl.ds(1, 8 * z_count - 1)]
        return copy_to(others, others, pair_peer, pair)

    flipped = []
    for slot in range(CHUNKS):
        factor_loads[slot].wait()
        flipped.append(factors_ref[slot * chunk : (slot + 1) * chunk, :].T)
        for step in range(chunk // tile_width):
            turned[slot * (chunk // tile_width) + step] = flipped[-1][
                :, step * tile_width : (step + 1) * tile_width
            ]
    own_rows = pl.ds(pl.multiple_of(c * half, half), half)
    other_rows = pl.ds(pl.multiple_of((1 - c) * half, half), half)
    own_share = pl.ds(pl.multiple_of(c * half + z * share, share), share)
    other_share = pl.ds(pl.multiple_of((1 - c) * half + z * share, share), share)

    row_number = lax.broadcasted_iota(jnp.int32, (tile_width, tile_width), 0)
    blank = jnp.zeros((tile_width, tile_width), bf16)

    def gathered(ids_ref, scalar_ref, q, place, first):
        picks, blocks = [], []
        for tile in (first, first + 1):
            start = tile * tile_width
            inside = lax.rem(ids_ref[q, 0, :, start : start + tile_width], tile_width)
            picks.append(jnp.where(row_number == inside, 1.0, 0.0).astype(bf16))
            blocks.append(turned[lax.div(scalar_ref[place, 0, 0, start], tile_width)])
        mixed = jnp.concatenate(
            [
                jnp.concatenate([picks[0], blank], axis=1),
                jnp.concatenate([blank, picks[1]], axis=1),
            ],
            axis=0,
        )
        return jnp.dot(jnp.concatenate(blocks, axis=1), mixed, preferred_element_type=f32)

    def partial(pe, py, pc, head_blocks=head_ids, tail_blocks=tail_ids, place=None):
        q = pe * 4 + py * 2 + pc
        place = q if place is None else place
        for first in range(0, triples // tile_width, 2):
            cols = slice(first * tile_width, (first + 2) * tile_width)
            rows = gathered(heads_ref, head_blocks, q, place, first)
            left_rows[:, cols] = (values_ref[q, 0, :, cols] * rows).astype(bf16)
            right_rows[:, cols] = gathered(tails_ref, tail_blocks, q, place, first).astype(bf16)
        return lax.dot_general(
            left_rows[...], right_rows[...], (((1,), (1,)), ((), ())), preferred_element_type=f32
        )

    targets = ((1 - e, 1 - y), (1 - e, y), (e, 1 - y), (e, y))
    pair_copies = []

    def give(index):
        pe, py = targets[index]
        pair_out[index] = partial(pe, py, 1 - c)
        pair_copies.append(send(pair_out.at[index], pair_in.at[index], pair_peer))

    def keep(index):
        pe, py = targets[index]
        own_sum[index] = partial(pe, py, c)

    def join(index):
        pair_copies[index].wait()
        own_sum[index] = own_sum[index] + pair_in[index]

    top, low = pl.ds(0, half), pl.ds(half, half)
    for load in loads[:5]:
        load.wait()
    pair_out[0] = partial(1 - e, 1 - y, 1 - c, first_heads, first_tails, 0)
    pl.semaphore_wait(barrier, len(near) + line_count)
    pair_copies.append(send(pair_out.at[0], pair_in.at[0], pair_peer))
    if z_count > 2:
        tell(ready.at[0])
    gram_part[...] = jnp.dot(
        jnp.concatenate(flipped, axis=1), factors_ref[...], preferred_element_type=f32
    )
    g_pair = send(gram_part.at[other_share], gram_in, pair_peer)
    for load in loads[5:]:
        load.wait()
    keep(0)
    g_pair.wait()
    gram_half[0] = gram_part[own_share, :] + gram_in[...]
    upper, lower = pl.ds(0, part), pl.ds(part, part)
    g_a1 = send(gram_half.at[0, upper], gram_xy.at[0, upper], x_peer)
    g_b1 = send(gram_half.at[0, lower], gram_xy.at[0, lower], y_peer)
    join(0)
    a_diag = send(own_sum.at[0, top], first_a.at[0], x_peer)
    b_diag = send(own_sum.at[0, low], first_b.at[0], y_peer)
    give(1)
    give(2)
    for step in range(1, z_count - 2):
        pl.semaphore_wait(ready.at[step - 1], line_count)
        tell(ready.at[step])
    keep(1)
    g_a1.wait()
    g_b1.wait()
    gram_half[1] = gram_half[0] + gram_xy[0]
    g_a2 = send(gram_half.at[1, upper], gram_xy.at[1, upper], y_peer)
    g_b2 = send(gram_half.at[1, lower], gram_xy.at[1, lower], x_peer)
    join(1)
    a_side = send(own_sum.at[1, top], first_a.at[1], x_peer)
    keep(2)
    join(2)
    b_side = send(own_sum.at[2, low], first_b.at[1], y_peer)
    give(3)
    keep(3)
    a_diag.wait()
    second_a[0] = own_sum[2, :half, :] + first_a[0]
    a_last = send(second_a.at[0], second_a.at[1], y_peer)
    b_diag.wait()
    second_b[0] = own_sum[1, half:, :] + first_b[0]
    b_last = send(second_b.at[0], second_b.at[1], x_peer)
    g_a2.wait()
    g_b2.wait()
    gram_line[0] = gram_half[1] + gram_xy[1]
    if z_count > 2:
        pl.semaphore_wait(ready.at[z_count - 3], line_count)
    line_copies = [
        send(gram_line.at[0], gram_line.at[z_count - hop], z_peer(hop))
        for hop in range(1, z_count)
    ]
    join(3)
    for copy in line_copies:
        copy.wait()
    for hop in range(z_count):
        place = lax.rem(z + hop, z_count)
        gram_pair[0, pl.ds(pl.multiple_of(place * share, share), share), :] = gram_line[hop]
    g_full = send(gram_pair.at[0], gram_pair.at[1], pair_peer)
    g_full.wait()
    gram_full[own_rows, :] = gram_pair[0] * scale_gram
    gram_full[other_rows, :] = gram_pair[1] * scale_gram

    def split(value):
        high = value.astype(bf16)
        return high, (value - high.astype(f32)).astype(bf16)

    def fold(value):
        return jnp.sum(value.reshape(-1, 8, value.shape[1]), axis=0)

    def total(parts):
        added = parts[0]
        for piece in parts[1:]:
            added = added + piece
        return jnp.sum(jnp.sum(added, axis=0, keepdims=True), axis=1, keepdims=True)

    strips = [slice(first, first + STRIP) for first in range(0, width, STRIP)]
    panels = range(0, width, PANEL)
    gram = gram_full[...]
    gram_high, gram_low = split(gram)
    gram_twice = jnp.dot(gram_high, gram_high, preferred_element_type=f32) + (
        jnp.dot(gram_high, gram_low, preferred_element_type=f32)
        + jnp.dot(gram_low, gram_high, preferred_element_type=f32)
    )
    for power, (high, low_part) in enumerate(((gram_high, gram_low), split(gram_twice))):
        for third, piece in enumerate((high, low_part, high)):
            span = slice(third * width, (third + 1) * width)
            factor_left[power, :, span] = piece
            factor_right[power, span, :] = piece

    def spread_out(strip, value):
        high, low_part = split(value)
        for third, piece in enumerate((high, high, low_part)):
            vector_parts[
                slice(third * width + strip.start, third * width + strip.stop), :
            ] = piece
        return fold(value * value)

    a_side.wait()
    b_side.wait()
    a_last.wait_recv()
    b_last.wait_recv()
    squares = []
    for strip in strips:
        later = strip.start >= half
        inside = slice(strip.start - half, strip.stop - half) if later else strip
        side, last = (first_b, second_b) if later else (first_a, second_a)
        value = ((own_sum[3, strip, :] + side[1, inside, :]) + last[1, inside, :]) * scale_target
        basis[0, strip, :] = value
        squares.append(spread_out(strip, value))

    lane = lax.broadcasted_iota(jnp.int32, (1, 128), 1)
    record = jnp.zeros((1, 128), f32)

    def noted(record, place, value):
        return jnp.where(lane == place, value, record)

    def sized(square):
        inverse = jnp.where(square > 0.0, lax.rsqrt(square), 0.0)
        return inverse, square * inverse

    inverses, lengths, diagonals = [], [], []
    for index in range(0, ITERS, 2):
        for power in (0, 1):
            for first in panels:
                inner = jnp.dot(
                    factor_left[power, first : first + PANEL, :],
                    vector_parts[...],
                    preferred_element_type=f32,
                )
                for step in range(0, PANEL, STRIP):
                    high, low_part = split(inner[step : step + STRIP])
                    rows = slice(first + step, first + step + STRIP)
                    for third, piece in enumerate((high, high, low_part)):
                        inner_parts[power, rows, third * width : (third + 1) * width] = piece
        if index + 2 == ITERS:
            b_last.wait_send()
        crosses = []
        for power, dest in ((0, image), (1, image_twice)):
            for first in panels:
                outer = jnp.dot(
                    inner_parts[power, first : first + PANEL, :],
                    factor_right[power],
                    preferred_element_type=f32,
                )
                dest[first : first + PANEL, :] = outer
                for step in range(0, PANEL, STRIP):
                    if power == 0:
                        rows = slice(first + step, first + step + STRIP)
                        crosses.append(fold(outer[step : step + STRIP] * basis[index, rows, :]))
        inverse, length = sized(total(squares))
        diagonal = (total(crosses) * inverse) * inverse
        scaled = diagonal * inverse
        ratio = length * inverses[-1] if index > 0 else None
        squares, crosses = [], []
        for strip in strips:
            value = image[strip, :] * inverse - scaled * basis[index, strip, :]
            if index > 0:
                value = value - ratio * basis[index - 1, strip, :]
            basis[index + 1, strip, :] = value
            squares.append(fold(value * value))
            crosses.append(fold(value * image_twice[strip, :]))
        next_inverse, next_length = sized(total(squares))
        next_diagonal = (
            ((total(crosses) * inverse) * next_inverse) * next_inverse - diagonal
        )
        inverses += [inverse, next_inverse]
        lengths += [length, next_length]
        diagonals += [diagonal + ridge_weight, next_diagonal + ridge_weight]
        for place in (index, index + 1):
            record = noted(record, place, diagonals[place])
            record = noted(record, ITERS + place, lengths[place])
        if index + 4 == ITERS:
            early[0] = record
            early_copy = spread(early)
        if index + 2 == ITERS:
            late[0] = record
            late_copy = spread(late)
            a_last.wait_send()
        now, before = (index // 2) % 2, (index // 2 + 1) % 2
        for strip in strips:
            value = image_twice[strip, :] * inverse - scaled * image[strip, :]
            if index > 0:
                value = value - ratio * mapped[before, strip, :]
            mapped[now, strip, :] = value
        next_scaled, next_ratio = next_diagonal * next_inverse, next_length * inverse
        squares = []
        for strip in strips:
            value = (
                mapped[now, strip, :] * next_inverse - next_ratio * basis[index, strip, :]
            ) - next_scaled * basis[index + 1, strip, :]
            basis[index + 2, strip, :] = value
            if index + 2 < ITERS:
                squares.append(spread_out(strip, value))
    inverses.append(jnp.ones((1, 1), f32))

    def lanes_of(table):
        lines = table[...].reshape(8 * z_count, 128)
        blank_lines = jnp.zeros((128 - 8 * z_count, 128), f32)
        return jnp.concatenate([lines, blank_lines], axis=0).T

    def reduced(rows):
        added = rows[0]
        for row in rows[1:]:
            added = added + row
        return jnp.sum(added, axis=1, keepdims=True)

    def small_map(rows, alpha, beta):
        count = len(rows)
        made = []
        for j in range(min(count + 1, len(beta))):
            entry = None
            if j < count:
                entry = alpha[j] * rows[j]
            if j > 0:
                term = beta[j] * rows[j - 1]
                entry = term if entry is None else entry + term
            if j + 1 < count:
                entry = entry + beta[j + 1] * rows[j + 1]
            made.append(entry)
        return made

    def mixed_sum(first, ratio, second):
        return [
            one + ratio * second[j] if j < len(second) else one for j, one in enumerate(first)
        ]

    def products(residual, image):
        return (
            reduced([row * row for row in residual]),
            reduced([row * image[j] for j, row in enumerate(residual)]),
        )

    early_copy.wait()
    filled = lanes_of(early)
    known = ITERS - 2
    alpha = [filled[j : j + 1, :] for j in range(known)]
    beta = [filled[ITERS + j : ITERS + j + 1, :] for j in range(known)]
    residual = [beta[0]]
    image = small_map(residual, alpha, beta)
    norm_now, product = products(residual, image)
    step_size = norm_now / product
    direction, along = residual, image
    fitted = []
    for index in range(known):
        if index == 0:
            fitted = [step_size * row for row in direction]
        else:
            fitted = [
                fitted[j] + step_size * row if j < len(fitted) else step_size * row
                for j, row in enumerate(direction)
            ]
        residual = [
            residual[j] - step_size * row if j < len(residual) else -(step_size * row)
            for j, row in enumerate(along)
        ]
        if index + 1 < known:
            image = small_map(residual, alpha, beta)
            norm_next, product = products(residual, image)
            ratio = norm_next / norm_now
            step_size = norm_next / (product - ratio * norm_next / step_size)
            direction = mixed_sum(residual, ratio, direction)
            along = mixed_sum(image, ratio, along)
            norm_now = norm_next

    late_copy.wait()
    filled = lanes_of(late)
    alpha += [filled[j : j + 1, :] for j in range(known, ITERS)]
    beta += [filled[ITERS + j : ITERS + j + 1, :] for j in range(known, ITERS)]
    beta.append(jnp.ones((1, 128), f32))
    along = along + [beta[known] * direction[-1]]
    residual = residual + [-(step_size * along[-1])]
    image = small_map(residual, alpha, beta)
    norm_next, product = products(residual, image)
    ratio = norm_next / norm_now
    step_next = norm_next / (product - ratio * norm_next / step_size)
    residual_before, image_before = residual, image
    residual = [
        residual[j] - step_next * row if j < len(residual) else -(step_next * row)
        for j, row in enumerate(mixed_sum(image, ratio, along))
    ]
    fitted = [
        fitted[j] + step_next * row if j < len(fitted) else step_next * row
        for j, row in enumerate(mixed_sum(residual_before, ratio, direction))
    ]
    image = small_map(residual, alpha, beta)
    norm_last, product = products(residual, image)
    ratio_last = norm_last / norm_next
    step_last = norm_last / (product - ratio_last * norm_last / step_next)
    direction = mixed_sum(residual, ratio_last, mixed_sum(residual_before, ratio, direction))
    along = mixed_sum(image, ratio_last, mixed_sum(image_before, ratio, along))
    fitted = [
        fitted[j] + step_last * row if j < len(fitted) else step_last * row
        for j, row in enumerate(direction)
    ]
    residual = [
        residual[j] - step_last * row if j < len(residual) else -(step_last * row)
        for j, row in enumerate(along)
    ]
    for place, row in enumerate(fitted + residual):
        weight = row[:, 0:1] * inverses[place if place < ITERS else place - ITERS]
        mix_ref[place : place + 1, :] = jnp.broadcast_to(weight, (1, width))


def finish_kernel(basis, mix_ref, fit_hbm, res_hbm, fit_rows, res_rows, fit_sem, res_sem):
    count = basis.shape[0] - 1
    weights = [mix_ref[place : place + 1, :] for place in range(2 * count + 1)]
    height = fit_rows.shape[0] // CHUNKS
    copies = []
    for slot in range(CHUNKS):
        for first in range(slot * height, (slot + 1) * height, STRIP):
            strip = slice(first, first + STRIP)
            vector = basis[0, strip, :]
            fit, res = weights[0] * vector, weights[count] * vector
            for j in range(1, count + 1):
                vector = basis[j, strip, :]
                res = res + weights[count + j] * vector
                if j < count:
                    fit = fit + weights[j] * vector
            fit_rows[strip, :] = fit
            res_rows[strip, :] = res
        rows = pl.ds(slot * height, height)
        for source, dest, sem in ((fit_rows, fit_hbm, fit_sem), (res_rows, res_hbm, res_sem)):
            copies.append(
                pltpu.make_async_copy(source.at[rows], dest.at[0, rows], sem.at[slot])
            )
            copies[-1].start()
    for copy in copies:
        copy.wait()


def fused_body(factors, heads, tails, values):
    shards = lax.axis_size(("ent", "blk"))
    z_count = lax.axis_size("rel")
    ent_dev, width = factors.shape
    triples = heads.shape[3]
    half = width // 2
    f32, bf16 = jnp.float32, jnp.bfloat16
    vmem = pl.BlockSpec(memory_space=pltpu.VMEM)
    share = half // z_count
    basis, mix = pl.pallas_call(
        functools.partial(
            fused_kernel, z_count, 1.0 / (ent_dev * shards), 1.0 / math.sqrt(shards * triples)
        ),
        out_shape=(
            pltpu.VMEM((ITERS + 1, width, width), f32),
            pltpu.VMEM((3 * ITERS, width), f32),
        ),
        in_specs=[pl.BlockSpec(memory_space=pl.ANY)] * 4,
        out_specs=(vmem, vmem),
        scratch_shapes=[
            pltpu.VMEM(factors.shape, bf16),
            pltpu.VMEM(heads.shape, jnp.int32),
            pltpu.VMEM(tails.shape, jnp.int32),
            pltpu.VMEM(values.shape, f32),
            pltpu.SMEM(heads.shape, jnp.int32),
            pltpu.SMEM(tails.shape, jnp.int32),
            pltpu.SMEM((1,) + heads.shape[1:], jnp.int32),
            pltpu.SMEM((1,) + heads.shape[1:], jnp.int32),
            pltpu.SemaphoreType.DMA((CHUNKS,)),
            pltpu.SemaphoreType.DMA((7,)),
            pltpu.SemaphoreType.REGULAR((max(z_count - 2, 1),)),
            pltpu.VMEM((ent_dev // tile_width, width, tile_width), bf16),
            pltpu.VMEM((width, triples), bf16),
            pltpu.VMEM((width, triples), bf16),
            pltpu.VMEM((width, width), f32),
            pltpu.VMEM((share, width), f32),
            pltpu.VMEM((2, share, width), f32),
            pltpu.VMEM((2, share, width), f32),
            pltpu.VMEM((z_count, share, width), f32),
            pltpu.VMEM((width, width), f32),
            pltpu.VMEM((2, half, width), f32),
            pltpu.VMEM((4, width, width), f32),
            pltpu.VMEM((4, width, width), f32),
            pltpu.VMEM((4, width, width), f32),
            pltpu.VMEM((2, half, width), f32),
            pltpu.VMEM((2, half, width), f32),
            pltpu.VMEM((2, half, width), f32),
            pltpu.VMEM((2, half, width), f32),
            pltpu.VMEM((2, width, 3 * width), bf16),
            pltpu.VMEM((2, 3 * width, width), bf16),
            pltpu.VMEM((3 * width, width), bf16),
            pltpu.VMEM((2, width, 3 * width), bf16),
            pltpu.VMEM((width, width), f32),
            pltpu.VMEM((width, width), f32),
            pltpu.VMEM((2, width, width), f32),
            pltpu.VMEM((8 * z_count, 1, 128), f32),
            pltpu.VMEM((8 * z_count, 1, 128), f32),
            pltpu.SemaphoreType.DMA((COPIES,)),
            pltpu.SemaphoreType.DMA((COPIES,)),
        ],
        compiler_params=pltpu.CompilerParams(collective_id=0, has_side_effects=True),
    )(factors, heads, tails, values)
    out = jax.ShapeDtypeStruct((1, width, width), f32)
    anywhere = pl.BlockSpec(memory_space=pl.ANY)
    return pl.pallas_call(
        finish_kernel,
        out_shape=(out, out),
        in_specs=[vmem, vmem],
        out_specs=(anywhere, anywhere),
        scratch_shapes=[
            pltpu.VMEM((width, width), f32),
            pltpu.VMEM((width, width), f32),
            pltpu.SemaphoreType.DMA((CHUNKS,)),
            pltpu.SemaphoreType.DMA((CHUNKS,)),
        ],
        compiler_params=pltpu.CompilerParams(vmem_limit_bytes=16 * width * width * 4),
    )(basis, mix)


def solution(mesh):
    placed = (
        P(("ent", "blk"), None),
        P(None, "rel", None, ("ent", "blk")),
        P(None, "rel", None, ("ent", "blk")),
        P(None, "rel", None, ("ent", "blk")),
    )
    sizes = dict(mesh.shape)
    fused = sizes["ent"] == 2 and sizes["blk"] == 4 and sizes["rel"] in (2, 4, 8)
    return jax.shard_map(
        fused_body if fused else body,
        mesh=mesh,
        in_specs=placed,
        out_specs=(P(("ent", "blk", "rel"), None, None), P(("ent", "blk", "rel"), None, None)),
        check_vma=False,
    )
```

```python
import functools
import math

import jax
import jax.numpy as jnp
from jax import lax
from jax.experimental import pallas as pl
from jax.experimental.pallas import tpu as pltpu
from jax.sharding import PartitionSpec as P

ITERS = 8


ridge_weight = 0.01
tile_width = 128


def apply_normal(gram_matrix, stacked):
    left_side = jnp.einsum("ab,kbc->kac", gram_matrix, stacked, precision=lax.Precision.HIGHEST)
    return (
        jnp.einsum("kac,cd->kad", left_side, gram_matrix, precision=lax.Precision.HIGHEST)
        + ridge_weight * stacked
    )


def two_products(residual, image_map):
    return lax.psum(
        (jnp.sum(residual * residual), jnp.sum(residual * image_map)), ("ent", "blk", "rel")
    )


def select_rows(entity_ids, block_table):
    group_size, width = entity_ids.shape
    tile_count = width // tile_width
    block_count = block_table.shape[0]
    tiled_ids = entity_ids.reshape(group_size, tile_count, tile_width)
    block_of = tiled_ids[:, :, 0] // tile_width
    block_pick = (
        block_of[:, :, None] == jnp.arange(block_count, dtype=jnp.int32)[None, None, :]
    ).astype(jnp.bfloat16)
    chosen = jnp.einsum(
        "gtb,bcr->gtcr", block_pick, block_table, preferred_element_type=jnp.float32
    ).astype(jnp.bfloat16)
    inside = tiled_ids % tile_width
    slot_pick = (
        inside[:, :, :, None] == jnp.arange(tile_width, dtype=jnp.int32)[None, None, None, :]
    ).astype(jnp.bfloat16)
    return jnp.einsum("gtoc,gtcr->gtor", slot_pick, chosen, preferred_element_type=jnp.float32)


def body(factors, heads, tails, values):
    shards = lax.axis_size(("ent", "blk"))
    ent_dev = factors.shape[0]
    rank_width = factors.shape[1]
    triple_count = heads.shape[3]
    relation_rows = heads.shape[0] * heads.shape[2]
    norm_scale = 1.0 / math.sqrt(shards * triple_count)
    gram_total = lax.psum(
        jnp.dot(factors.T, factors, preferred_element_type=jnp.float32), ("ent", "blk")
    )
    gram_matrix = gram_total / (ent_dev * shards)
    block_table = factors.reshape(ent_dev // tile_width, tile_width, rank_width)
    head_ids = heads.reshape(relation_rows, triple_count)
    tail_ids = tails.reshape(relation_rows, triple_count)
    weights = values.reshape(relation_rows, triple_count)

    def grouped(operands):
        head_group, tail_group, weight_group = operands
        group_size = head_group.shape[0]
        tile_count = triple_count // tile_width
        head_rows = select_rows(head_group, block_table)
        weighted = (
            weight_group.reshape(group_size, tile_count, tile_width)[:, :, :, None] * head_rows
        ).astype(jnp.bfloat16)
        tail_rows = select_rows(tail_group, block_table).astype(jnp.bfloat16)
        product = jnp.einsum(
            "gtci,gtcj->gij", weighted, tail_rows, preferred_element_type=jnp.float32
        )
        return product * norm_scale

    own_rows = relation_rows // shards
    group_size = math.gcd(own_rows * lax.axis_size(("ent", "blk")), 4)
    group_total = own_rows * lax.axis_size(("ent", "blk")) // group_size
    shaped = (
        head_ids.reshape(group_total, group_size, triple_count),
        tail_ids.reshape(group_total, group_size, triple_count),
        weights.reshape(group_total, group_size, triple_count),
    )
    results = lax.map(grouped, shaped)
    target = lax.psum_scatter(
        results.reshape(own_rows * lax.axis_size(("ent", "blk")), rank_width, rank_width),
        ("ent", "blk"),
        scatter_dimension=0,
        tiled=True,
    )
    fitted = jnp.zeros_like(target)
    residual = target
    image_map = apply_normal(gram_matrix, residual)
    norm_now, product = two_products(residual, image_map)
    step_size = norm_now / product
    direction = residual
    along = image_map
    for step_index in range(ITERS):
        fitted = fitted + step_size * direction
        residual = residual - step_size * along
        if step_index + 1 < ITERS:
            image_map = apply_normal(gram_matrix, residual)
            norm_next, product = two_products(residual, image_map)
            ratio_next = norm_next / norm_now
            step_size = norm_next / (product - ratio_next * norm_next / step_size)
            direction = residual + ratio_next * direction
            along = image_map + ratio_next * along
            norm_now = norm_next
    return (fitted, residual)


MESH = pl.DeviceIdType.MESH
COPIES = 21
CHUNKS = 4
STRIP = 32
PANEL = 128


def fused_kernel(
    z_count, scale_gram, scale_target,
    factors_hbm, heads_hbm, tails_hbm, values_hbm,
    basis, mix_ref,
    factors_ref, heads_ref, tails_ref, values_ref, head_ids, tail_ids,
    first_heads, first_tails, factor_sem, load_sem, ready,
    turned, left_rows, right_rows,
    gram_part, gram_in, gram_half, gram_xy, gram_line, gram_full, gram_pair,
    pair_out, pair_in, own_sum, first_a, first_b, second_a, second_b,
    factor_left, factor_right, vector_parts, inner_parts, image, image_twice, mapped,
    early, late, send_sem, recv_sem,
):
    f32, bf16 = jnp.float32, jnp.bfloat16
    width = factors_ref.shape[1]
    half = width // 2
    share = half // z_count
    part = share // 2
    triples = heads_ref.shape[3]
    e = lax.axis_index("ent")
    b = lax.axis_index("blk")
    z = lax.axis_index("rel")
    y = b // 2
    c = b % 2
    pair_peer = (e, y * 2 + 1 - c, z)
    x_peer = (1 - e, b, z)
    y_peer = (e, (1 - y) * 2 + c, z)

    def group_peer(mask):
        me, my, mc = mask // 4, (mask // 2) % 2, mask % 2
        return (
            (1 - e) if me else e,
            ((1 - y) if my else y) * 2 + ((1 - c) if mc else c),
            z,
        )

    def z_peer(hop):
        return (e, b, lax.rem(z + hop, z_count))

    near = [group_peer(m) for m in (1, 2, 4)]
    inner = ((z > 0, -1), (z < z_count - 1, 1))

    def tell(semaphore):
        for present, hop in inner:
            @pl.when(present)
            def _():
                pl.semaphore_signal(
                    semaphore, inc=1, device_id=(e, b, z + hop), device_id_type=MESH
                )

    line_count = jnp.where(z > 0, 1, 0) + jnp.where(z < z_count - 1, 1, 0)
    barrier = pltpu.get_barrier_semaphore()
    for peer in near:
        pl.semaphore_signal(barrier, inc=1, device_id=peer, device_id_type=MESH)
    tell(barrier)
    first_q = (1 - e) * 4 + (1 - y) * 2 + 1 - c
    chunk = factors_ref.shape[0] // CHUNKS
    factor_loads = []
    for slot in range(CHUNKS):
        rows = pl.ds(slot * chunk, chunk)
        factor_loads.append(
            pltpu.make_async_copy(
                factors_hbm.at[rows], factors_ref.at[rows], factor_sem.at[slot]
            )
        )
        factor_loads[-1].start()
    loads = []
    for slot, (source, dest) in enumerate(
        (
            (heads_hbm.at[pl.ds(first_q, 1)], first_heads),
            (tails_hbm.at[pl.ds(first_q, 1)], first_tails),
            (heads_hbm, heads_ref),
            (values_hbm, values_ref),
            (tails_hbm, tails_ref),
            (heads_hbm, head_ids),
            (tails_hbm, tail_ids),
        )
    ):
        loads.append(pltpu.make_async_copy(source, dest, load_sem.at[slot]))
        loads[-1].start()

    counter = [0]

    def spare():
        slot = counter[0]
        counter[0] += 1
        return send_sem.at[slot], recv_sem.at[slot]

    def copy_to(source, dest, peer, pair):
        return pltpu.make_async_remote_copy(
            src_ref=source, dst_ref=dest, send_sem=pair[0], recv_sem=pair[1],
            device_id=peer, device_id_type=MESH,
        )

    def send(source, dest, peer):
        copy = copy_to(source, dest, peer, spare())
        copy.start()
        return copy

    far_peers = [
        (m, hop) for hop in (*range(1, z_count), 0) for m in (7, 6, 5, 3, 4, 2, 1, 0) if m or hop
    ]

    def spread(table):
        pair = spare()
        for m, hop in far_peers:
            peer = group_peer(m)[:2] + (lax.rem(z + hop, z_count),)
            place = m * z_count + (z_count - hop) % z_count
            copy_to(table.at[0], table.at[place], peer, pair).start()
        others = table.at[pl.ds(1, 8 * z_count - 1)]
        return copy_to(others, others, pair_peer, pair)

    flipped = []
    for slot in range(CHUNKS):
        factor_loads[slot].wait()
        flipped.append(factors_ref[slot * chunk : (slot + 1) * chunk, :].T)
        for step in range(chunk // tile_width):
            turned[slot * (chunk // tile_width) + step] = flipped[-1][
                :, step * tile_width : (step + 1) * tile_width
            ]
    own_rows = pl.ds(pl.multiple_of(c * half, half), half)
    other_rows = pl.ds(pl.multiple_of((1 - c) * half, half), half)
    own_share = pl.ds(pl.multiple_of(c * half + z * share, share), share)
    other_share = pl.ds(pl.multiple_of((1 - c) * half + z * share, share), share)

    row_number = lax.broadcasted_iota(jnp.int32, (tile_width, tile_width), 0)
    blank = jnp.zeros((tile_width, tile_width), bf16)

    def gathered(ids_ref, scalar_ref, q, place, first):
        picks, blocks = [], []
        for tile in (first, first + 1):
            start = tile * tile_width
            inside = lax.rem(ids_ref[q, 0, :, start : start + tile_width], tile_width)
            picks.append(jnp.where(row_number == inside, 1.0, 0.0).astype(bf16))
            blocks.append(turned[lax.div(scalar_ref[place, 0, 0, start], tile_width)])
        mixed = jnp.concatenate(
            [
                jnp.concatenate([picks[0], blank], axis=1),
                jnp.concatenate([blank, picks[1]], axis=1),
            ],
            axis=0,
        )
        return jnp.dot(jnp.concatenate(blocks, axis=1), mixed, preferred_element_type=f32)

    def partial(pe, py, pc, head_blocks=head_ids, tail_blocks=tail_ids, place=None):
        q = pe * 4 + py * 2 + pc
        place = q if place is None else place
        for first in range(0, triples // tile_width, 2):
            cols = slice(first * tile_width, (first + 2) * tile_width)
            rows = gathered(heads_ref, head_blocks, q, place, first)
            left_rows[:, cols] = (values_ref[q, 0, :, cols] * rows).astype(bf16)
            right_rows[:, cols] = gathered(tails_ref, tail_blocks, q, place, first).astype(bf16)
        return lax.dot_general(
            left_rows[...], right_rows[...], (((1,), (1,)), ((), ())), preferred_element_type=f32
        )

    targets = ((1 - e, 1 - y), (1 - e, y), (e, 1 - y), (e, y))
    pair_copies = []

    def give(index):
        pe, py = targets[index]
        pair_out[index] = partial(pe, py, 1 - c)
        pair_copies.append(send(pair_out.at[index], pair_in.at[index], pair_peer))

    def keep(index):
        pe, py = targets[index]
        own_sum[index] = partial(pe, py, c)

    def join(index):
        pair_copies[index].wait()
        own_sum[index] = own_sum[index] + pair_in[index]

    top, low = pl.ds(0, half), pl.ds(half, half)
    for load in loads[:5]:
        load.wait()
    pair_out[0] = partial(1 - e, 1 - y, 1 - c, first_heads, first_tails, 0)
    pl.semaphore_wait(barrier, len(near) + line_count)
    pair_copies.append(send(pair_out.at[0], pair_in.at[0], pair_peer))
    if z_count > 2:
        tell(ready.at[0])
    gram_part[...] = jnp.dot(
        jnp.concatenate(flipped, axis=1), factors_ref[...], preferred_element_type=f32
    )
    g_pair = send(gram_part.at[other_share], gram_in, pair_peer)
    for load in loads[5:]:
        load.wait()
    keep(0)
    g_pair.wait()
    gram_half[0] = gram_part[own_share, :] + gram_in[...]
    upper, lower = pl.ds(0, part), pl.ds(part, part)
    g_a1 = send(gram_half.at[0, upper], gram_xy.at[0, upper], x_peer)
    g_b1 = send(gram_half.at[0, lower], gram_xy.at[0, lower], y_peer)
    join(0)
    a_diag = send(own_sum.at[0, top], first_a.at[0], x_peer)
    b_diag = send(own_sum.at[0, low], first_b.at[0], y_peer)
    give(1)
    give(2)
    for step in range(1, z_count - 2):
        pl.semaphore_wait(ready.at[step - 1], line_count)
        tell(ready.at[step])
    keep(1)
    g_a1.wait()
    g_b1.wait()
    gram_half[1] = gram_half[0] + gram_xy[0]
    g_a2 = send(gram_half.at[1, upper], gram_xy.at[1, upper], y_peer)
    g_b2 = send(gram_half.at[1, lower], gram_xy.at[1, lower], x_peer)
    join(1)
    a_side = send(own_sum.at[1, top], first_a.at[1], x_peer)
    keep(2)
    join(2)
    b_side = send(own_sum.at[2, low], first_b.at[1], y_peer)
    give(3)
    keep(3)
    a_diag.wait()
    second_a[0] = own_sum[2, :half, :] + first_a[0]
    a_last = send(second_a.at[0], second_a.at[1], y_peer)
    b_diag.wait()
    second_b[0] = own_sum[1, half:, :] + first_b[0]
    b_last = send(second_b.at[0], second_b.at[1], x_peer)
    g_a2.wait()
    g_b2.wait()
    gram_line[0] = gram_half[1] + gram_xy[1]
    if z_count > 2:
        pl.semaphore_wait(ready.at[z_count - 3], line_count)
    line_copies = [
        send(gram_line.at[0], gram_line.at[z_count - hop], z_peer(hop))
        for hop in range(1, z_count)
    ]
    join(3)
    for copy in line_copies:
        copy.wait()
    for hop in range(z_count):
        place = lax.rem(z + hop, z_count)
        gram_pair[0, pl.ds(pl.multiple_of(place * share, share), share), :] = gram_line[hop]
    g_full = send(gram_pair.at[0], gram_pair.at[1], pair_peer)
    g_full.wait()
    gram_full[own_rows, :] = gram_pair[0] * scale_gram
    gram_full[other_rows, :] = gram_pair[1] * scale_gram

    def split(value):
        high = value.astype(bf16)
        return high, (value - high.astype(f32)).astype(bf16)

    def fold(value):
        return jnp.sum(value.reshape(-1, 8, value.shape[1]), axis=0)

    def total(parts):
        added = parts[0]
        for piece in parts[1:]:
            added = added + piece
        return jnp.sum(jnp.sum(added, axis=0, keepdims=True), axis=1, keepdims=True)

    strips = [slice(first, first + STRIP) for first in range(0, width, STRIP)]
    panels = range(0, width, PANEL)
    gram = gram_full[...]
    gram_high, gram_low = split(gram)
    gram_twice = jnp.dot(gram_high, gram_high, preferred_element_type=f32) + (
        jnp.dot(gram_high, gram_low, preferred_element_type=f32)
        + jnp.dot(gram_low, gram_high, preferred_element_type=f32)
    )
    for power, (high, low_part) in enumerate(((gram_high, gram_low), split(gram_twice))):
        for third, piece in enumerate((high, low_part, high)):
            span = slice(third * width, (third + 1) * width)
            factor_left[power, :, span] = piece
            factor_right[power, span, :] = piece

    def spread_out(strip, value):
        high, low_part = split(value)
        for third, piece in enumerate((high, high, low_part)):
            vector_parts[
                slice(third * width + strip.start, third * width + strip.stop), :
            ] = piece
        return fold(value * value)

    a_side.wait()
    b_side.wait()
    a_last.wait_recv()
    b_last.wait_recv()
    squares = []
    for strip in strips:
        later = strip.start >= half
        inside = slice(strip.start - half, strip.stop - half) if later else strip
        side, last = (first_b, second_b) if later else (first_a, second_a)
        value = ((own_sum[3, strip, :] + side[1, inside, :]) + last[1, inside, :]) * scale_target
        basis[0, strip, :] = value
        squares.append(spread_out(strip, value))

    lane = lax.broadcasted_iota(jnp.int32, (1, 128), 1)
    record = jnp.zeros((1, 128), f32)

    def noted(record, place, value):
        return jnp.where(lane == place, value, record)

    def sized(square):
        inverse = jnp.where(square > 0.0, lax.rsqrt(square), 0.0)
        return inverse, square * inverse

    inverses, lengths, diagonals = [], [], []
    for index in range(0, ITERS, 2):
        for power in (0, 1):
            for first in panels:
                inner = jnp.dot(
                    factor_left[power, first : first + PANEL, :],
                    vector_parts[...],
                    preferred_element_type=f32,
                )
                for step in range(0, PANEL, STRIP):
                    high, low_part = split(inner[step : step + STRIP])
                    rows = slice(first + step, first + step + STRIP)
                    for third, piece in enumerate((high, high, low_part)):
                        inner_parts[power, rows, third * width : (third + 1) * width] = piece
        if index + 2 == ITERS:
            b_last.wait_send()
        crosses = []
        for power, dest in ((0, image), (1, image_twice)):
            for first in panels:
                outer = jnp.dot(
                    inner_parts[power, first : first + PANEL, :],
                    factor_right[power],
                    preferred_element_type=f32,
                )
                dest[first : first + PANEL, :] = outer
                for step in range(0, PANEL, STRIP):
                    if power == 0:
                        rows = slice(first + step, first + step + STRIP)
                        crosses.append(fold(outer[step : step + STRIP] * basis[index, rows, :]))
        inverse, length = sized(total(squares))
        diagonal = (total(crosses) * inverse) * inverse
        scaled = diagonal * inverse
        ratio = length * inverses[-1] if index > 0 else None
        squares, crosses = [], []
        now, before = (index // 2) % 2, (index // 2 + 1) % 2
        for strip in strips:
            value = image[strip, :] * inverse - scaled * basis[index, strip, :]
            if index > 0:
                value = value - ratio * basis[index - 1, strip, :]
            basis[index + 1, strip, :] = value
            squares.append(fold(value * value))
            beyond = image_twice[strip, :] * inverse - scaled * image[strip, :]
            if index > 0:
                beyond = beyond - ratio * mapped[before, strip, :]
            mapped[now, strip, :] = beyond
            crosses.append(fold(value * beyond))
        next_inverse, next_length = sized(total(squares))
        next_diagonal = (total(crosses) * next_inverse) * next_inverse
        inverses += [inverse, next_inverse]
        lengths += [length, next_length]
        diagonals += [diagonal + ridge_weight, next_diagonal + ridge_weight]
        for place in (index, index + 1):
            record = noted(record, place, diagonals[place])
            record = noted(record, ITERS + place, lengths[place])
        if index + 4 == ITERS:
            early[0] = record
            early_copy = spread(early)
        if index + 2 == ITERS:
            late[0] = record
            late_copy = spread(late)
            a_last.wait_send()
        next_scaled, next_ratio = next_diagonal * next_inverse, next_length * inverse
        squares = []
        for strip in strips:
            value = (
                mapped[now, strip, :] * next_inverse - next_ratio * basis[index, strip, :]
            ) - next_scaled * basis[index + 1, strip, :]
            basis[index + 2, strip, :] = value
            if index + 2 < ITERS:
                squares.append(spread_out(strip, value))
    inverses.append(jnp.ones((1, 1), f32))

    def lanes_of(table):
        lines = table[...].reshape(8 * z_count, 128)
        blank_lines = jnp.zeros((128 - 8 * z_count, 128), f32)
        return jnp.concatenate([lines, blank_lines], axis=0).T

    def reduced(rows):
        added = rows[0]
        for row in rows[1:]:
            added = added + row
        return jnp.sum(added, axis=1, keepdims=True)

    def small_map(rows, alpha, beta):
        count = len(rows)
        made = []
        for j in range(min(count + 1, len(beta))):
            entry = None
            if j < count:
                entry = alpha[j] * rows[j]
            if j > 0:
                term = beta[j] * rows[j - 1]
                entry = term if entry is None else entry + term
            if j + 1 < count:
                entry = entry + beta[j + 1] * rows[j + 1]
            made.append(entry)
        return made

    def mixed_sum(first, ratio, second):
        return [
            one + ratio * second[j] if j < len(second) else one for j, one in enumerate(first)
        ]

    def products(residual, image):
        return (
            reduced([row * row for row in residual]),
            reduced([row * image[j] for j, row in enumerate(residual)]),
        )

    early_copy.wait()
    filled = lanes_of(early)
    known = ITERS - 2
    alpha = [filled[j : j + 1, :] for j in range(known)]
    beta = [filled[ITERS + j : ITERS + j + 1, :] for j in range(known)]
    residual = [beta[0]]
    image = small_map(residual, alpha, beta)
    norm_now, product = products(residual, image)
    step_size = norm_now / product
    direction, along = residual, image
    fitted = []
    for index in range(known):
        if index == 0:
            fitted = [step_size * row for row in direction]
        else:
            fitted = [
                fitted[j] + step_size * row if j < len(fitted) else step_size * row
                for j, row in enumerate(direction)
            ]
        residual = [
            residual[j] - step_size * row if j < len(residual) else -(step_size * row)
            for j, row in enumerate(along)
        ]
        if index + 1 < known:
            image = small_map(residual, alpha, beta)
            norm_next, product = products(residual, image)
            ratio = norm_next / norm_now
            step_size = norm_next / (product - ratio * norm_next / step_size)
            direction = mixed_sum(residual, ratio, direction)
            along = mixed_sum(image, ratio, along)
            norm_now = norm_next

    late_copy.wait()
    filled = lanes_of(late)
    alpha += [filled[j : j + 1, :] for j in range(known, ITERS)]
    beta += [filled[ITERS + j : ITERS + j + 1, :] for j in range(known, ITERS)]
    beta.append(jnp.ones((1, 128), f32))
    along = along + [beta[known] * direction[-1]]
    residual = residual + [-(step_size * along[-1])]
    image = small_map(residual, alpha, beta)
    norm_next, product = products(residual, image)
    ratio = norm_next / norm_now
    step_next = norm_next / (product - ratio * norm_next / step_size)
    residual_before, image_before = residual, image
    residual = [
        residual[j] - step_next * row if j < len(residual) else -(step_next * row)
        for j, row in enumerate(mixed_sum(image, ratio, along))
    ]
    fitted = [
        fitted[j] + step_next * row if j < len(fitted) else step_next * row
        for j, row in enumerate(mixed_sum(residual_before, ratio, direction))
    ]
    image = small_map(residual, alpha, beta)
    norm_last, product = products(residual, image)
    ratio_last = norm_last / norm_next
    step_last = norm_last / (product - ratio_last * norm_last / step_next)
    direction = mixed_sum(residual, ratio_last, mixed_sum(residual_before, ratio, direction))
    along = mixed_sum(image, ratio_last, mixed_sum(image_before, ratio, along))
    fitted = [
        fitted[j] + step_last * row if j < len(fitted) else step_last * row
        for j, row in enumerate(direction)
    ]
    residual = [
        residual[j] - step_last * row if j < len(residual) else -(step_last * row)
        for j, row in enumerate(along)
    ]
    for place, row in enumerate(fitted + residual):
        weight = row[:, 0:1] * inverses[place if place < ITERS else place - ITERS]
        mix_ref[place : place + 1, :] = jnp.broadcast_to(weight, (1, width))


def finish_kernel(basis, mix_ref, fit_hbm, res_hbm, fit_rows, res_rows, fit_sem, res_sem):
    count = basis.shape[0] - 1
    weights = [mix_ref[place : place + 1, :] for place in range(2 * count + 1)]
    height = fit_rows.shape[0] // CHUNKS
    copies = []
    for slot in range(CHUNKS):
        for first in range(slot * height, (slot + 1) * height, STRIP):
            strip = slice(first, first + STRIP)
            vector = basis[0, strip, :]
            fit, res = weights[0] * vector, weights[count] * vector
            for j in range(1, count + 1):
                vector = basis[j, strip, :]
                res = res + weights[count + j] * vector
                if j < count:
                    fit = fit + weights[j] * vector
            fit_rows[strip, :] = fit
            res_rows[strip, :] = res
        rows = pl.ds(slot * height, height)
        for source, dest, sem in ((fit_rows, fit_hbm, fit_sem), (res_rows, res_hbm, res_sem)):
            copies.append(
                pltpu.make_async_copy(source.at[rows], dest.at[0, rows], sem.at[slot])
            )
            copies[-1].start()
    for copy in copies:
        copy.wait()


def fused_body(factors, heads, tails, values):
    shards = lax.axis_size(("ent", "blk"))
    z_count = lax.axis_size("rel")
    ent_dev, width = factors.shape
    triples = heads.shape[3]
    half = width // 2
    f32, bf16 = jnp.float32, jnp.bfloat16
    vmem = pl.BlockSpec(memory_space=pltpu.VMEM)
    share = half // z_count
    basis, mix = pl.pallas_call(
        functools.partial(
            fused_kernel, z_count, 1.0 / (ent_dev * shards), 1.0 / math.sqrt(shards * triples)
        ),
        out_shape=(
            pltpu.VMEM((ITERS + 1, width, width), f32),
            pltpu.VMEM((4 * ITERS, width), f32),
        ),
        in_specs=[pl.BlockSpec(memory_space=pl.ANY)] * 4,
        out_specs=(vmem, vmem),
        scratch_shapes=[
            pltpu.VMEM(factors.shape, bf16),
            pltpu.VMEM(heads.shape, jnp.int32),
            pltpu.VMEM(tails.shape, jnp.int32),
            pltpu.VMEM(values.shape, f32),
            pltpu.SMEM(heads.shape, jnp.int32),
            pltpu.SMEM(tails.shape, jnp.int32),
            pltpu.SMEM((1,) + heads.shape[1:], jnp.int32),
            pltpu.SMEM((1,) + heads.shape[1:], jnp.int32),
            pltpu.SemaphoreType.DMA((CHUNKS,)),
            pltpu.SemaphoreType.DMA((7,)),
            pltpu.SemaphoreType.REGULAR((max(z_count - 2, 1),)),
            pltpu.VMEM((ent_dev // tile_width, width, tile_width), bf16),
            pltpu.VMEM((width, triples), bf16),
            pltpu.VMEM((width, triples), bf16),
            pltpu.VMEM((width, width), f32),
            pltpu.VMEM((share, width), f32),
            pltpu.VMEM((2, share, width), f32),
            pltpu.VMEM((2, share, width), f32),
            pltpu.VMEM((z_count, share, width), f32),
            pltpu.VMEM((width, width), f32),
            pltpu.VMEM((2, half, width), f32),
            pltpu.VMEM((4, width, width), f32),
            pltpu.VMEM((4, width, width), f32),
            pltpu.VMEM((4, width, width), f32),
            pltpu.VMEM((2, half, width), f32),
            pltpu.VMEM((2, half, width), f32),
            pltpu.VMEM((2, half, width), f32),
            pltpu.VMEM((2, half, width), f32),
            pltpu.VMEM((2, width, 3 * width), bf16),
            pltpu.VMEM((2, 3 * width, width), bf16),
            pltpu.VMEM((3 * width, width), bf16),
            pltpu.VMEM((2, width, 3 * width), bf16),
            pltpu.VMEM((width, width), f32),
            pltpu.VMEM((width, width), f32),
            pltpu.VMEM((2, width, width), f32),
            pltpu.VMEM((8 * z_count, 1, 128), f32),
            pltpu.VMEM((8 * z_count, 1, 128), f32),
            pltpu.SemaphoreType.DMA((COPIES,)),
            pltpu.SemaphoreType.DMA((COPIES,)),
        ],
        compiler_params=pltpu.CompilerParams(collective_id=0, has_side_effects=True),
    )(factors, heads, tails, values)
    out = jax.ShapeDtypeStruct((1, width, width), f32)
    anywhere = pl.BlockSpec(memory_space=pl.ANY)
    return pl.pallas_call(
        finish_kernel,
        out_shape=(out, out),
        in_specs=[vmem, vmem],
        out_specs=(anywhere, anywhere),
        scratch_shapes=[
            pltpu.VMEM((width, width), f32),
            pltpu.VMEM((width, width), f32),
            pltpu.SemaphoreType.DMA((CHUNKS,)),
            pltpu.SemaphoreType.DMA((CHUNKS,)),
        ],
        compiler_params=pltpu.CompilerParams(vmem_limit_bytes=16 * width * width * 4),
    )(basis, mix)


def solution(mesh):
    placed = (
        P(("ent", "blk"), None),
        P(None, "rel", None, ("ent", "blk")),
        P(None, "rel", None, ("ent", "blk")),
        P(None, "rel", None, ("ent", "blk")),
    )
    sizes = dict(mesh.shape)
    fused = sizes["ent"] == 2 and sizes["blk"] == 4 and sizes["rel"] in (2, 4, 8)
    return jax.shard_map(
        fused_body if fused else body,
        mesh=mesh,
        in_specs=placed,
        out_specs=(P(("ent", "blk", "rel"), None, None), P(("ent", "blk", "rel"), None, None)),
        check_vma=False,
    )
```

```python
import functools
import math

import jax
import jax.numpy as jnp
from jax import lax
from jax.experimental import pallas as pl
from jax.experimental.pallas import tpu as pltpu
from jax.sharding import PartitionSpec as P

ITERS = 8


ridge_weight = 0.01
tile_width = 128


def apply_normal(gram_matrix, stacked):
    left_side = jnp.einsum("ab,kbc->kac", gram_matrix, stacked, precision=lax.Precision.HIGHEST)
    return (
        jnp.einsum("kac,cd->kad", left_side, gram_matrix, precision=lax.Precision.HIGHEST)
        + ridge_weight * stacked
    )


def two_products(residual, image_map):
    return lax.psum(
        (jnp.sum(residual * residual), jnp.sum(residual * image_map)), ("ent", "blk", "rel")
    )


def select_rows(entity_ids, block_table):
    group_size, width = entity_ids.shape
    tile_count = width // tile_width
    block_count = block_table.shape[0]
    tiled_ids = entity_ids.reshape(group_size, tile_count, tile_width)
    block_of = tiled_ids[:, :, 0] // tile_width
    block_pick = (
        block_of[:, :, None] == jnp.arange(block_count, dtype=jnp.int32)[None, None, :]
    ).astype(jnp.bfloat16)
    chosen = jnp.einsum(
        "gtb,bcr->gtcr", block_pick, block_table, preferred_element_type=jnp.float32
    ).astype(jnp.bfloat16)
    inside = tiled_ids % tile_width
    slot_pick = (
        inside[:, :, :, None] == jnp.arange(tile_width, dtype=jnp.int32)[None, None, None, :]
    ).astype(jnp.bfloat16)
    return jnp.einsum("gtoc,gtcr->gtor", slot_pick, chosen, preferred_element_type=jnp.float32)


def body(factors, heads, tails, values):
    shards = lax.axis_size(("ent", "blk"))
    ent_dev = factors.shape[0]
    rank_width = factors.shape[1]
    triple_count = heads.shape[3]
    relation_rows = heads.shape[0] * heads.shape[2]
    norm_scale = 1.0 / math.sqrt(shards * triple_count)
    gram_total = lax.psum(
        jnp.dot(factors.T, factors, preferred_element_type=jnp.float32), ("ent", "blk")
    )
    gram_matrix = gram_total / (ent_dev * shards)
    block_table = factors.reshape(ent_dev // tile_width, tile_width, rank_width)
    head_ids = heads.reshape(relation_rows, triple_count)
    tail_ids = tails.reshape(relation_rows, triple_count)
    weights = values.reshape(relation_rows, triple_count)

    def grouped(operands):
        head_group, tail_group, weight_group = operands
        group_size = head_group.shape[0]
        tile_count = triple_count // tile_width
        head_rows = select_rows(head_group, block_table)
        weighted = (
            weight_group.reshape(group_size, tile_count, tile_width)[:, :, :, None] * head_rows
        ).astype(jnp.bfloat16)
        tail_rows = select_rows(tail_group, block_table).astype(jnp.bfloat16)
        product = jnp.einsum(
            "gtci,gtcj->gij", weighted, tail_rows, preferred_element_type=jnp.float32
        )
        return product * norm_scale

    own_rows = relation_rows // shards
    group_size = math.gcd(own_rows * lax.axis_size(("ent", "blk")), 4)
    group_total = own_rows * lax.axis_size(("ent", "blk")) // group_size
    shaped = (
        head_ids.reshape(group_total, group_size, triple_count),
        tail_ids.reshape(group_total, group_size, triple_count),
        weights.reshape(group_total, group_size, triple_count),
    )
    results = lax.map(grouped, shaped)
    target = lax.psum_scatter(
        results.reshape(own_rows * lax.axis_size(("ent", "blk")), rank_width, rank_width),
        ("ent", "blk"),
        scatter_dimension=0,
        tiled=True,
    )
    fitted = jnp.zeros_like(target)
    residual = target
    image_map = apply_normal(gram_matrix, residual)
    norm_now, product = two_products(residual, image_map)
    step_size = norm_now / product
    direction = residual
    along = image_map
    for step_index in range(ITERS):
        fitted = fitted + step_size * direction
        residual = residual - step_size * along
        if step_index + 1 < ITERS:
            image_map = apply_normal(gram_matrix, residual)
            norm_next, product = two_products(residual, image_map)
            ratio_next = norm_next / norm_now
            step_size = norm_next / (product - ratio_next * norm_next / step_size)
            direction = residual + ratio_next * direction
            along = image_map + ratio_next * along
            norm_now = norm_next
    return (fitted, residual)


MESH = pl.DeviceIdType.MESH
COPIES = 24
CHUNKS = 4
STRIP = 32
PANEL = 128


def fused_kernel(
    z_count, scale_gram, scale_target,
    factors_hbm, heads_hbm, tails_hbm, values_hbm,
    basis, mix_ref, scale_ref,
    factors_ref, heads_ref, tails_ref, values_ref, head_ids, tail_ids,
    first_heads, first_tails, factor_sem, load_sem, ready,
    turned, left_rows, right_rows,
    gram_part, gram_in, gram_half, gram_xy, gram_line, gram_full, gram_pair,
    pair_out, pair_in, own_sum, first_a, first_b, second_a, second_b,
    factor_left, factor_right, vector_parts, inner_parts, image, image_twice, mapped,
    early, late, send_sem, recv_sem,
):
    f32, bf16 = jnp.float32, jnp.bfloat16
    width = factors_ref.shape[2]
    half = width // 2
    share = half // z_count
    part = share // 2
    triples = heads_ref.shape[3]
    e = lax.axis_index("ent")
    b = lax.axis_index("blk")
    z = lax.axis_index("rel")
    y = b // 2
    c = b % 2
    pair_peer = (e, y * 2 + 1 - c, z)
    x_peer = (1 - e, b, z)
    y_peer = (e, (1 - y) * 2 + c, z)

    def group_peer(mask):
        me, my, mc = mask // 4, (mask // 2) % 2, mask % 2
        return (
            (1 - e) if me else e,
            ((1 - y) if my else y) * 2 + ((1 - c) if mc else c),
            z,
        )

    def z_peer(hop):
        return (e, b, lax.rem(z + hop, z_count))

    near = [group_peer(m) for m in (1, 2, 4)]
    inner = ((z > 0, -1), (z < z_count - 1, 1))

    def tell(semaphore):
        for present, hop in inner:
            @pl.when(present)
            def _():
                pl.semaphore_signal(
                    semaphore, inc=1, device_id=(e, b, z + hop), device_id_type=MESH
                )

    line_count = jnp.where(z > 0, 1, 0) + jnp.where(z < z_count - 1, 1, 0)
    barrier = pltpu.get_barrier_semaphore()
    for peer in near:
        pl.semaphore_signal(barrier, inc=1, device_id=peer, device_id_type=MESH)
    tell(barrier)
    first_q = (1 - e) * 4 + (1 - y) * 2 + 1 - c
    block_count = factors_ref.shape[0]
    factor_loads = []
    for block in range(block_count):
        rows = pl.ds(block * tile_width, tile_width)
        factor_loads.append(
            pltpu.make_async_copy(
                factors_hbm.at[rows], factors_ref.at[block], factor_sem.at[block]
            )
        )
        factor_loads[-1].start()
    loads = []
    for slot, (source, dest) in enumerate(
        (
            (heads_hbm.at[pl.ds(first_q, 1)], first_heads),
            (tails_hbm.at[pl.ds(first_q, 1)], first_tails),
            (heads_hbm, heads_ref),
            (values_hbm, values_ref),
            (tails_hbm, tails_ref),
            (heads_hbm, head_ids),
            (tails_hbm, tail_ids),
        )
    ):
        loads.append(pltpu.make_async_copy(source, dest, load_sem.at[slot]))
        loads[-1].start()

    counter = [0]
    sent = []

    def spare():
        slot = counter[0]
        counter[0] += 1
        return send_sem.at[slot], recv_sem.at[slot]

    def copy_to(source, dest, peer, pair):
        return pltpu.make_async_remote_copy(
            src_ref=source, dst_ref=dest, send_sem=pair[0], recv_sem=pair[1],
            device_id=peer, device_id_type=MESH,
        )

    def send(source, dest, peer):
        copy = copy_to(source, dest, peer, spare())
        copy.start()
        sent.append(copy)
        return copy

    far_peers = [
        (m, hop) for hop in (*range(1, z_count), 0) for m in (7, 6, 5, 3, 4, 2, 1, 0) if m or hop
    ]

    def spread(table):
        pair = spare()
        for m, hop in far_peers:
            peer = group_peer(m)[:2] + (lax.rem(z + hop, z_count),)
            place = m * z_count + (z_count - hop) % z_count
            copy_to(table.at[0], table.at[place], peer, pair).start()
        others = table.at[pl.ds(1, 8 * z_count - 1)]
        return copy_to(others, others, pair_peer, pair)

    flipped = []
    for block in range(block_count):
        factor_loads[block].wait()
        flipped.append(factors_ref[block].T)
        turned[block] = flipped[-1]
    own_rows = pl.ds(pl.multiple_of(c * half, half), half)
    other_rows = pl.ds(pl.multiple_of((1 - c) * half, half), half)
    own_share = pl.ds(pl.multiple_of(c * half + z * share, share), share)
    other_share = pl.ds(pl.multiple_of((1 - c) * half + z * share, share), share)

    row_number = lax.broadcasted_iota(jnp.int32, (tile_width, tile_width), 0)
    blank = jnp.zeros((tile_width, tile_width), bf16)

    top, low = slice(0, half), slice(half, width)

    def by_halves(left, right):
        return jnp.concatenate(
            [
                jnp.dot(left[rows], right, preferred_element_type=f32)
                for rows in (slice(0, half), slice(half, width))
            ],
            axis=0,
        )

    def picked(ids_ref, q, first):
        picks = []
        for tile in (first, first + 1):
            start = tile * tile_width
            inside = lax.rem(ids_ref[q, 0, :, start : start + tile_width], tile_width)
            picks.append(jnp.where(row_number == inside, 1.0, 0.0).astype(bf16))
        return picks

    def paired(picks):
        return jnp.concatenate(
            [
                jnp.concatenate([picks[0], blank], axis=1),
                jnp.concatenate([blank, picks[1]], axis=1),
            ],
            axis=0,
        )

    def block_of(scalar_ref, place, tile):
        return lax.div(scalar_ref[place, 0, 0, tile * tile_width], tile_width)

    def partial(pe, py, pc, head_blocks=head_ids, tail_blocks=tail_ids, place=None):
        q = pe * 4 + py * 2 + pc
        place = q if place is None else place
        for first in range(0, triples // tile_width, 2):
            cols = slice(first * tile_width, (first + 2) * tile_width)
            picks = picked(heads_ref, q, first)
            blocks = [turned[block_of(head_blocks, place, tile)] for tile in (first, first + 1)]
            rows = jnp.dot(
                jnp.concatenate(blocks, axis=1), paired(picks), preferred_element_type=f32
            )
            left_rows[:, cols] = (values_ref[q, 0, :, cols] * rows).astype(bf16)
            picks = [pick.T for pick in picked(tails_ref, q, first)]
            blocks = [
                factors_ref[block_of(tail_blocks, place, tile)] for tile in (first, first + 1)
            ]
            right_rows[cols, :] = jnp.dot(
                paired(picks), jnp.concatenate(blocks, axis=0), preferred_element_type=f32
            ).astype(bf16)
        return [
            jnp.dot(left_rows[rows, :], right_rows[...], preferred_element_type=f32)
            for rows in (top, low)
        ]

    targets = ((1 - e, 1 - y), (1 - e, y), (e, 1 - y), (e, y))
    pair_copies = []

    def give(index):
        pe, py = targets[index]
        pair_out[index, top], pair_out[index, low] = partial(pe, py, 1 - c)
        pair_copies.append(send(pair_out.at[index], pair_in.at[index], pair_peer))

    def keep(index):
        pe, py = targets[index]
        own_sum[index, top], own_sum[index, low] = partial(pe, py, c)

    def join(index):
        pair_copies[index].wait_recv()
        own_sum[index] = own_sum[index] + pair_in[index]

    for load in loads[:5]:
        load.wait()
    pair_out[0, top], pair_out[0, low] = partial(
        1 - e, 1 - y, 1 - c, first_heads, first_tails, 0
    )
    pl.semaphore_wait(barrier, len(near) + line_count)
    pair_top = send(pair_out.at[0, pl.ds(0, half)], pair_in.at[0, pl.ds(0, half)], pair_peer)
    pair_low = send(pair_out.at[0, pl.ds(half, half)], pair_in.at[0, pl.ds(half, half)], pair_peer)
    pair_copies.append(None)
    if z_count > 2:
        tell(ready.at[0])
    gram_part[...] = by_halves(
        jnp.concatenate(flipped, axis=1),
        jnp.concatenate([factors_ref[block] for block in range(block_count)], axis=0),
    )
    g_pair = send(gram_part.at[other_share], gram_in, pair_peer)
    for load in loads[5:]:
        load.wait()
    keep(0)
    lead, rest = pl.ds(0, half // 2), pl.ds(half // 2, half // 2)
    pair_top.wait_recv()
    own_sum[0, top] = own_sum[0, top] + pair_in[0, top]
    diag_copies = [send(own_sum.at[0, lead], first_a.at[0, lead], x_peer)]
    pair_low.wait_recv()
    own_sum[0, low] = own_sum[0, low] + pair_in[0, low]
    diag_copies.append(
        send(own_sum.at[0, pl.ds(half, half // 2)], first_b.at[0, lead], y_peer)
    )
    g_pair.wait_recv()
    gram_half[0] = gram_part[own_share, :] + gram_in[...]
    upper, lower = pl.ds(0, part), pl.ds(part, part)
    g_a1 = send(gram_half.at[0, upper], gram_xy.at[0, upper], x_peer)
    g_b1 = send(gram_half.at[0, lower], gram_xy.at[0, lower], y_peer)
    a_diag = send(own_sum.at[0, rest], first_a.at[0, rest], x_peer)
    b_diag = send(own_sum.at[0, pl.ds(half + half // 2, half // 2)], first_b.at[0, rest], y_peer)
    give(1)
    give(2)
    for step in range(1, z_count - 2):
        pl.semaphore_wait(ready.at[step - 1], line_count)
        tell(ready.at[step])
    keep(1)
    g_a1.wait_recv()
    g_b1.wait_recv()
    gram_half[1] = gram_half[0] + gram_xy[0]
    g_a2 = send(gram_half.at[1, upper], gram_xy.at[1, upper], y_peer)
    g_b2 = send(gram_half.at[1, lower], gram_xy.at[1, lower], x_peer)
    join(1)
    a_side = send(own_sum.at[1, pl.ds(0, half)], first_a.at[1], x_peer)
    keep(2)
    join(2)
    b_side = send(own_sum.at[2, pl.ds(half, half)], first_b.at[1], y_peer)
    give(3)
    keep(3)
    diag_copies[0].wait_recv()
    a_diag.wait_recv()
    second_a[0] = own_sum[2, :half, :] + first_a[0]
    a_last = send(second_a.at[0], second_a.at[1], y_peer)
    diag_copies[1].wait_recv()
    b_diag.wait_recv()
    second_b[0] = own_sum[1, half:, :] + first_b[0]
    b_last = send(second_b.at[0], second_b.at[1], x_peer)
    g_a2.wait_recv()
    g_b2.wait_recv()
    gram_line[0] = gram_half[1] + gram_xy[1]
    if z_count > 2:
        pl.semaphore_wait(ready.at[z_count - 3], line_count)
    line_copies = [
        send(gram_line.at[0], gram_line.at[z_count - hop], z_peer(hop))
        for hop in range(1, z_count)
    ]
    join(3)
    for copy in line_copies:
        copy.wait_recv()
    for hop in range(z_count):
        place = lax.rem(z + hop, z_count)
        gram_pair[0, pl.ds(pl.multiple_of(place * share, share), share), :] = gram_line[hop]
    g_full = send(gram_pair.at[0], gram_pair.at[1], pair_peer)
    g_full.wait_recv()
    gram_full[own_rows, :] = gram_pair[0] * scale_gram
    gram_full[other_rows, :] = gram_pair[1] * scale_gram

    def split(value):
        high = value.astype(bf16)
        return high, (value - high.astype(f32)).astype(bf16)

    def fold(value):
        return jnp.sum(value.reshape(-1, 8, value.shape[1]), axis=0)

    def total(parts):
        added = parts[0]
        for piece in parts[1:]:
            added = added + piece
        return jnp.sum(jnp.sum(added, axis=0, keepdims=True), axis=1, keepdims=True)

    strips = [slice(first, first + STRIP) for first in range(0, width, STRIP)]
    panels = range(0, width, PANEL)
    gram = gram_full[...]
    gram_high, gram_low = split(gram)
    gram_twice = jnp.dot(gram_high, gram_high, preferred_element_type=f32) + (
        jnp.dot(gram_high, gram_low, preferred_element_type=f32)
        + jnp.dot(gram_low, gram_high, preferred_element_type=f32)
    )
    for power, (high, low_part) in enumerate(((gram_high, gram_low), split(gram_twice))):
        for third, piece in enumerate((high, low_part, high)):
            span = slice(third * width, (third + 1) * width)
            factor_left[power, :, span] = piece
            factor_right[power, span, :] = piece

    def spread_out(strip, value):
        high, low_part = split(value)
        for third, piece in enumerate((high, high, low_part)):
            vector_parts[
                slice(third * width + strip.start, third * width + strip.stop), :
            ] = piece
        return fold(value * value)

    a_side.wait_recv()
    b_side.wait_recv()
    a_last.wait_recv()
    b_last.wait_recv()
    squares = []
    for strip in strips:
        later = strip.start >= half
        inside = slice(strip.start - half, strip.stop - half) if later else strip
        side, last = (first_b, second_b) if later else (first_a, second_a)
        value = ((own_sum[3, strip, :] + side[1, inside, :]) + last[1, inside, :]) * scale_target
        basis[0, strip, :] = value
        squares.append(spread_out(strip, value))

    lane = lax.broadcasted_iota(jnp.int32, (1, 128), 1)
    record = jnp.zeros((1, 128), f32)

    def noted(record, place, value):
        return jnp.where(lane == place, value, record)

    def sized(square):
        inverse = jnp.where(square > 0.0, lax.rsqrt(square), 0.0)
        return inverse, square * inverse

    inverses, lengths, diagonals = [], [], []
    for index in range(0, ITERS, 2):
        for power in (0, 1):
            for first in panels:
                inner = jnp.dot(
                    factor_left[power, first : first + PANEL, :],
                    vector_parts[...],
                    preferred_element_type=f32,
                )
                for step in range(0, PANEL, STRIP):
                    high, low_part = split(inner[step : step + STRIP])
                    rows = slice(first + step, first + step + STRIP)
                    for third, piece in enumerate((high, high, low_part)):
                        inner_parts[power, rows, third * width : (third + 1) * width] = piece
        if index + 2 == ITERS:
            b_last.wait_send()
        crosses = []
        for power, dest in ((0, image), (1, image_twice)):
            for first in panels:
                outer = jnp.dot(
                    inner_parts[power, first : first + PANEL, :],
                    factor_right[power],
                    preferred_element_type=f32,
                )
                dest[first : first + PANEL, :] = outer
                for step in range(0, PANEL, STRIP):
                    if power == 0:
                        rows = slice(first + step, first + step + STRIP)
                        crosses.append(fold(outer[step : step + STRIP] * basis[index, rows, :]))
        inverse, length = sized(total(squares))
        diagonal = (total(crosses) * inverse) * inverse
        ready_now = diagonal == diagonal
        step_inverse = inverse
        scaled = diagonal * inverse
        ratio = length * inverses[-1] if index > 0 else None
        squares, crosses = [], []
        now, before = (index // 2) % 2, (index // 2 + 1) % 2
        for strip in strips:
            value = image[strip, :] * step_inverse - scaled * basis[index, strip, :]
            if index > 0:
                value = value - ratio * basis[index - 1, strip, :]
            basis[index + 1, strip, :] = value
            squares.append(fold(value * value))
            beyond = image_twice[strip, :] * step_inverse - scaled * image[strip, :]
            if index > 0:
                beyond = beyond - ratio * mapped[before, strip, :]
            mapped[now, strip, :] = beyond
            crosses.append(fold(value * beyond))
        next_inverse, next_length = sized(total(squares))
        next_diagonal = (total(crosses) * next_inverse) * next_inverse
        inverses += [inverse, next_inverse]
        lengths += [length, next_length]
        diagonals += [diagonal + ridge_weight, next_diagonal + ridge_weight]
        for place in (index, index + 1):
            record = noted(record, place, diagonals[place])
            record = noted(record, ITERS + place, lengths[place])
        if index + 4 == ITERS:
            early[0] = record
            early_copy = spread(early)
        if index + 2 == ITERS:
            late[0] = record
            late_copy = spread(late)
            a_last.wait_send()
        next_scaled, next_ratio = next_diagonal * next_inverse, next_length * inverse
        squares = []
        for strip in strips:
            value = (
                mapped[now, strip, :] * next_inverse - next_ratio * basis[index, strip, :]
            ) - next_scaled * basis[index + 1, strip, :]
            basis[index + 2, strip, :] = value
            if index + 2 < ITERS:
                squares.append(spread_out(strip, value))
    inverses.append(jnp.ones((1, 1), f32))
    for copy in sent:
        if copy is not a_last and copy is not b_last:
            copy.wait_send()

    def lanes_of(table):
        lines = table[...].reshape(8 * z_count, 128)
        blank_lines = jnp.zeros((128 - 8 * z_count, 128), f32)
        return jnp.concatenate([lines, blank_lines], axis=0).T

    def reduced(rows):
        added = rows[0]
        for row in rows[1:]:
            added = added + row
        return jnp.sum(added, axis=1, keepdims=True)

    def small_map(rows, alpha, beta):
        count = len(rows)
        made = []
        for j in range(min(count + 1, len(beta))):
            entry = None
            if j < count:
                entry = alpha[j] * rows[j]
            if j > 0:
                term = beta[j] * rows[j - 1]
                entry = term if entry is None else entry + term
            if j + 1 < count:
                entry = entry + beta[j + 1] * rows[j + 1]
            made.append(entry)
        return made

    def mixed_sum(first, ratio, second):
        return [
            one + ratio * second[j] if j < len(second) else one for j, one in enumerate(first)
        ]

    def products(residual, image):
        return (
            reduced([row * row for row in residual]),
            reduced([row * image[j] for j, row in enumerate(residual)]),
        )

    for place in range(2 * ITERS + 1):
        inverse = inverses[place if place < ITERS else place - ITERS]
        scale_ref[place : place + 1, :] = jnp.broadcast_to(inverse, (1, 128))
    early_copy.wait()
    filled = lanes_of(early)
    known = ITERS - 2
    alpha = [filled[j : j + 1, :] for j in range(known)]
    beta = [filled[ITERS + j : ITERS + j + 1, :] for j in range(known)]
    residual = [beta[0]]
    image = small_map(residual, alpha, beta)
    norm_now, product = products(residual, image)
    step_size = norm_now / product
    direction, along = residual, image
    fitted = []
    for index in range(known):
        if index == 0:
            fitted = [step_size * row for row in direction]
        else:
            fitted = [
                fitted[j] + step_size * row if j < len(fitted) else step_size * row
                for j, row in enumerate(direction)
            ]
        residual = [
            residual[j] - step_size * row if j < len(residual) else -(step_size * row)
            for j, row in enumerate(along)
        ]
        if index + 1 < known:
            image = small_map(residual, alpha, beta)
            norm_next, product = products(residual, image)
            ratio = norm_next / norm_now
            step_size = norm_next / (product - ratio * norm_next / step_size)
            direction = mixed_sum(residual, ratio, direction)
            along = mixed_sum(image, ratio, along)
            norm_now = norm_next

    late_copy.wait()
    filled = lanes_of(late)
    alpha += [filled[j : j + 1, :] for j in range(known, ITERS)]
    beta += [filled[ITERS + j : ITERS + j + 1, :] for j in range(known, ITERS)]
    beta.append(jnp.ones((1, 128), f32))
    along = along + [beta[known] * direction[-1]]
    residual = residual + [-(step_size * along[-1])]
    image = small_map(residual, alpha, beta)
    norm_next, product = products(residual, image)
    ratio = norm_next / norm_now
    step_next = norm_next / (product - ratio * norm_next / step_size)
    residual_before, image_before = residual, image
    residual = [
        residual[j] - step_next * row if j < len(residual) else -(step_next * row)
        for j, row in enumerate(mixed_sum(image, ratio, along))
    ]
    fitted = [
        fitted[j] + step_next * row if j < len(fitted) else step_next * row
        for j, row in enumerate(mixed_sum(residual_before, ratio, direction))
    ]
    image = small_map(residual, alpha, beta)
    norm_last, product = products(residual, image)
    ratio_last = norm_last / norm_next
    step_last = norm_last / (product - ratio_last * norm_last / step_next)
    direction = mixed_sum(residual, ratio_last, mixed_sum(residual_before, ratio, direction))
    along = mixed_sum(image, ratio_last, mixed_sum(image_before, ratio, along))
    fitted = [
        fitted[j] + step_last * row if j < len(fitted) else step_last * row
        for j, row in enumerate(direction)
    ]
    residual = [
        residual[j] - step_last * row if j < len(residual) else -(step_last * row)
        for j, row in enumerate(along)
    ]
    for place, row in enumerate(fitted + residual):
        mix_ref[place : place + 1, :] = row


def finish_kernel(
    basis, mix_ref, scale_ref, fit_hbm, res_hbm, fit_rows, res_rows, fit_sem, res_sem
):
    count = basis.shape[0] - 1
    width = basis.shape[2]
    own_weights = mix_ref[0 : 2 * count + 1, 0:1] * scale_ref[0 : 2 * count + 1, 0:1]
    spread_weights = jnp.broadcast_to(own_weights, (2 * count + 1, width))
    weights = [spread_weights[place : place + 1, :] for place in range(2 * count + 1)]
    height = fit_rows.shape[0] // CHUNKS
    copies = []
    for slot in range(CHUNKS):
        for first in range(slot * height, (slot + 1) * height, STRIP):
            strip = slice(first, first + STRIP)
            vector = basis[0, strip, :]
            fit, res = weights[0] * vector, weights[count] * vector
            for j in range(1, count + 1):
                vector = basis[j, strip, :]
                res = res + weights[count + j] * vector
                if j < count:
                    fit = fit + weights[j] * vector
            fit_rows[strip, :] = fit
            res_rows[strip, :] = res
        rows = pl.ds(slot * height, height)
        for source, dest, sem in ((fit_rows, fit_hbm, fit_sem), (res_rows, res_hbm, res_sem)):
            copies.append(
                pltpu.make_async_copy(source.at[rows], dest.at[0, rows], sem.at[slot])
            )
            copies[-1].start()
    for copy in copies:
        copy.wait()


def fused_body(factors, heads, tails, values):
    shards = lax.axis_size(("ent", "blk"))
    z_count = lax.axis_size("rel")
    ent_dev, width = factors.shape
    triples = heads.shape[3]
    half = width // 2
    f32, bf16 = jnp.float32, jnp.bfloat16
    vmem = pl.BlockSpec(memory_space=pltpu.VMEM)
    share = half // z_count
    basis, mix, scale = pl.pallas_call(
        functools.partial(
            fused_kernel, z_count, 1.0 / (ent_dev * shards), 1.0 / math.sqrt(shards * triples)
        ),
        out_shape=(
            pltpu.VMEM((ITERS + 1, width, width), f32),
            pltpu.VMEM((4 * ITERS, 128), f32),
            pltpu.VMEM((4 * ITERS, 128), f32),
        ),
        in_specs=[pl.BlockSpec(memory_space=pl.ANY)] * 4,
        out_specs=(vmem, vmem, vmem),
        scratch_shapes=[
            pltpu.VMEM((ent_dev // tile_width, tile_width, width), bf16),
            pltpu.VMEM(heads.shape, jnp.int32),
            pltpu.VMEM(tails.shape, jnp.int32),
            pltpu.VMEM(values.shape, f32),
            pltpu.SMEM(heads.shape, jnp.int32),
            pltpu.SMEM(tails.shape, jnp.int32),
            pltpu.SMEM((1,) + heads.shape[1:], jnp.int32),
            pltpu.SMEM((1,) + heads.shape[1:], jnp.int32),
            pltpu.SemaphoreType.DMA((ent_dev // tile_width,)),
            pltpu.SemaphoreType.DMA((7,)),
            pltpu.SemaphoreType.REGULAR((max(z_count - 2, 1),)),
            pltpu.VMEM((ent_dev // tile_width, width, tile_width), bf16),
            pltpu.VMEM((width, triples), bf16),
            pltpu.VMEM((triples, width), bf16),
            pltpu.VMEM((width, width), f32),
            pltpu.VMEM((share, width), f32),
            pltpu.VMEM((2, share, width), f32),
            pltpu.VMEM((2, share, width), f32),
            pltpu.VMEM((z_count, share, width), f32),
            pltpu.VMEM((width, width), f32),
            pltpu.VMEM((2, half, width), f32),
            pltpu.VMEM((4, width, width), f32),
            pltpu.VMEM((4, width, width), f32),
            pltpu.VMEM((4, width, width), f32),
            pltpu.VMEM((2, half, width), f32),
            pltpu.VMEM((2, half, width), f32),
            pltpu.VMEM((2, half, width), f32),
            pltpu.VMEM((2, half, width), f32),
            pltpu.VMEM((2, width, 3 * width), bf16),
            pltpu.VMEM((2, 3 * width, width), bf16),
            pltpu.VMEM((3 * width, width), bf16),
            pltpu.VMEM((2, width, 3 * width), bf16),
            pltpu.VMEM((width, width), f32),
            pltpu.VMEM((width, width), f32),
            pltpu.VMEM((2, width, width), f32),
            pltpu.VMEM((8 * z_count, 1, 128), f32),
            pltpu.VMEM((8 * z_count, 1, 128), f32),
            pltpu.SemaphoreType.DMA((COPIES,)),
            pltpu.SemaphoreType.DMA((COPIES,)),
        ],
        compiler_params=pltpu.CompilerParams(collective_id=0, has_side_effects=True),
    )(factors, heads, tails, values)
    out = jax.ShapeDtypeStruct((1, width, width), f32)
    anywhere = pl.BlockSpec(memory_space=pl.ANY)
    return pl.pallas_call(
        finish_kernel,
        out_shape=(out, out),
        in_specs=[vmem, vmem, vmem],
        out_specs=(anywhere, anywhere),
        scratch_shapes=[
            pltpu.VMEM((width, width), f32),
            pltpu.VMEM((width, width), f32),
            pltpu.SemaphoreType.DMA((CHUNKS,)),
            pltpu.SemaphoreType.DMA((CHUNKS,)),
        ],
        compiler_params=pltpu.CompilerParams(vmem_limit_bytes=16 * width * width * 4),
    )(basis, mix, scale)


def solution(mesh):
    placed = (
        P(("ent", "blk"), None),
        P(None, "rel", None, ("ent", "blk")),
        P(None, "rel", None, ("ent", "blk")),
        P(None, "rel", None, ("ent", "blk")),
    )
    sizes = dict(mesh.shape)
    fused = sizes["ent"] == 2 and sizes["blk"] == 4 and sizes["rel"] in (2, 4, 8)
    return jax.shard_map(
        fused_body if fused else body,
        mesh=mesh,
        in_specs=placed,
        out_specs=(P(("ent", "blk", "rel"), None, None), P(("ent", "blk", "rel"), None, None)),
        check_vma=False,
    )
```

```python
import functools
import math

import jax
import jax.numpy as jnp
from jax import lax
from jax.experimental import pallas as pl
from jax.experimental.pallas import tpu as pltpu
from jax.sharding import PartitionSpec as P

ITERS = 8


ridge_weight = 0.01
tile_width = 128


def apply_normal(gram_matrix, stacked):
    left_side = jnp.einsum("ab,kbc->kac", gram_matrix, stacked, precision=lax.Precision.HIGHEST)
    return (
        jnp.einsum("kac,cd->kad", left_side, gram_matrix, precision=lax.Precision.HIGHEST)
        + ridge_weight * stacked
    )


def two_products(residual, image_map):
    return lax.psum(
        (jnp.sum(residual * residual), jnp.sum(residual * image_map)), ("ent", "blk", "rel")
    )


def select_rows(entity_ids, block_table):
    group_size, width = entity_ids.shape
    tile_count = width // tile_width
    block_count = block_table.shape[0]
    tiled_ids = entity_ids.reshape(group_size, tile_count, tile_width)
    block_of = tiled_ids[:, :, 0] // tile_width
    block_pick = (
        block_of[:, :, None] == jnp.arange(block_count, dtype=jnp.int32)[None, None, :]
    ).astype(jnp.bfloat16)
    chosen = jnp.einsum(
        "gtb,bcr->gtcr", block_pick, block_table, preferred_element_type=jnp.float32
    ).astype(jnp.bfloat16)
    inside = tiled_ids % tile_width
    slot_pick = (
        inside[:, :, :, None] == jnp.arange(tile_width, dtype=jnp.int32)[None, None, None, :]
    ).astype(jnp.bfloat16)
    return jnp.einsum("gtoc,gtcr->gtor", slot_pick, chosen, preferred_element_type=jnp.float32)


def body(factors, heads, tails, values):
    shards = lax.axis_size(("ent", "blk"))
    ent_dev = factors.shape[0]
    rank_width = factors.shape[1]
    triple_count = heads.shape[3]
    relation_rows = heads.shape[0] * heads.shape[2]
    norm_scale = 1.0 / math.sqrt(shards * triple_count)
    gram_total = lax.psum(
        jnp.dot(factors.T, factors, preferred_element_type=jnp.float32), ("ent", "blk")
    )
    gram_matrix = gram_total / (ent_dev * shards)
    block_table = factors.reshape(ent_dev // tile_width, tile_width, rank_width)
    head_ids = heads.reshape(relation_rows, triple_count)
    tail_ids = tails.reshape(relation_rows, triple_count)
    weights = values.reshape(relation_rows, triple_count)

    def grouped(operands):
        head_group, tail_group, weight_group = operands
        group_size = head_group.shape[0]
        tile_count = triple_count // tile_width
        head_rows = select_rows(head_group, block_table)
        weighted = (
            weight_group.reshape(group_size, tile_count, tile_width)[:, :, :, None] * head_rows
        ).astype(jnp.bfloat16)
        tail_rows = select_rows(tail_group, block_table).astype(jnp.bfloat16)
        product = jnp.einsum(
            "gtci,gtcj->gij", weighted, tail_rows, preferred_element_type=jnp.float32
        )
        return product * norm_scale

    own_rows = relation_rows // shards
    group_size = math.gcd(own_rows * lax.axis_size(("ent", "blk")), 4)
    group_total = own_rows * lax.axis_size(("ent", "blk")) // group_size
    shaped = (
        head_ids.reshape(group_total, group_size, triple_count),
        tail_ids.reshape(group_total, group_size, triple_count),
        weights.reshape(group_total, group_size, triple_count),
    )
    results = lax.map(grouped, shaped)
    target = lax.psum_scatter(
        results.reshape(own_rows * lax.axis_size(("ent", "blk")), rank_width, rank_width),
        ("ent", "blk"),
        scatter_dimension=0,
        tiled=True,
    )
    fitted = jnp.zeros_like(target)
    residual = target
    image_map = apply_normal(gram_matrix, residual)
    norm_now, product = two_products(residual, image_map)
    step_size = norm_now / product
    direction = residual
    along = image_map
    for step_index in range(ITERS):
        fitted = fitted + step_size * direction
        residual = residual - step_size * along
        if step_index + 1 < ITERS:
            image_map = apply_normal(gram_matrix, residual)
            norm_next, product = two_products(residual, image_map)
            ratio_next = norm_next / norm_now
            step_size = norm_next / (product - ratio_next * norm_next / step_size)
            direction = residual + ratio_next * direction
            along = image_map + ratio_next * along
            norm_now = norm_next
    return (fitted, residual)


MESH = pl.DeviceIdType.MESH
COPIES = 22
CHUNKS = 4
STRIP = 32
PANEL = 128


def fused_kernel(
    z_count, scale_gram, scale_target,
    factors_hbm, heads_hbm, tails_hbm, values_hbm,
    basis, mix_ref, scale_ref,
    factors_ref, heads_ref, tails_ref, values_ref, head_ids, tail_ids,
    first_heads, first_tails, factor_sem, load_sem, ready,
    turned, left_rows, right_rows,
    gram_part, gram_in, gram_half, gram_xy, gram_line, gram_full, gram_pair,
    pair_out, pair_in, own_sum, first_a, first_b, second_a, second_b,
    factor_left, factor_right, vector_parts, inner_parts, image, image_twice, mapped,
    early, late, send_sem, recv_sem,
):
    f32, bf16 = jnp.float32, jnp.bfloat16
    width = factors_ref.shape[2]
    half = width // 2
    share = half // z_count
    part = share // 2
    triples = heads_ref.shape[3]
    e = lax.axis_index("ent")
    b = lax.axis_index("blk")
    z = lax.axis_index("rel")
    y = b // 2
    c = b % 2
    pair_peer = (e, y * 2 + 1 - c, z)
    x_peer = (1 - e, b, z)
    y_peer = (e, (1 - y) * 2 + c, z)

    def group_peer(mask):
        me, my, mc = mask // 4, (mask // 2) % 2, mask % 2
        return (
            (1 - e) if me else e,
            ((1 - y) if my else y) * 2 + ((1 - c) if mc else c),
            z,
        )

    def z_peer(hop):
        return (e, b, lax.rem(z + hop, z_count))

    near = [group_peer(m) for m in (1, 2, 4)]
    inner = ((z > 0, -1), (z < z_count - 1, 1))

    def tell(semaphore):
        for present, hop in inner:
            @pl.when(present)
            def _():
                pl.semaphore_signal(
                    semaphore, inc=1, device_id=(e, b, z + hop), device_id_type=MESH
                )

    line_count = jnp.where(z > 0, 1, 0) + jnp.where(z < z_count - 1, 1, 0)
    barrier = pltpu.get_barrier_semaphore()
    for peer in near:
        pl.semaphore_signal(barrier, inc=1, device_id=peer, device_id_type=MESH)
    tell(barrier)
    first_q = (1 - e) * 4 + (1 - y) * 2 + 1 - c
    block_count = factors_ref.shape[0]
    factor_loads = []
    for block in range(block_count):
        rows = pl.ds(block * tile_width, tile_width)
        factor_loads.append(
            pltpu.make_async_copy(
                factors_hbm.at[rows], factors_ref.at[block], factor_sem.at[block]
            )
        )
        factor_loads[-1].start()
    loads = []
    for slot, (source, dest) in enumerate(
        (
            (heads_hbm.at[pl.ds(first_q, 1)], first_heads),
            (tails_hbm.at[pl.ds(first_q, 1)], first_tails),
            (heads_hbm, heads_ref),
            (values_hbm, values_ref),
            (tails_hbm, tails_ref),
            (heads_hbm, head_ids),
            (tails_hbm, tail_ids),
        )
    ):
        loads.append(pltpu.make_async_copy(source, dest, load_sem.at[slot]))
        loads[-1].start()

    counter = [0]
    sent = []

    def spare():
        slot = counter[0]
        counter[0] += 1
        return send_sem.at[slot], recv_sem.at[slot]

    def copy_to(source, dest, peer, pair):
        return pltpu.make_async_remote_copy(
            src_ref=source, dst_ref=dest, send_sem=pair[0], recv_sem=pair[1],
            device_id=peer, device_id_type=MESH,
        )

    def send(source, dest, peer):
        copy = copy_to(source, dest, peer, spare())
        copy.start()
        sent.append(copy)
        return copy

    far_peers = [
        (m, hop) for hop in (*range(1, z_count), 0) for m in (7, 6, 5, 3, 4, 2, 1, 0) if m or hop
    ]

    def spread(table):
        pair = spare()
        for m, hop in far_peers:
            peer = group_peer(m)[:2] + (lax.rem(z + hop, z_count),)
            place = m * z_count + (z_count - hop) % z_count
            copy_to(table.at[0], table.at[place], peer, pair).start()
        others = table.at[pl.ds(1, 8 * z_count - 1)]
        return copy_to(others, others, pair_peer, pair)

    flipped = []
    for block in range(block_count):
        factor_loads[block].wait()
        flipped.append(factors_ref[block].T)
        turned[block] = flipped[-1]
    own_rows = pl.ds(pl.multiple_of(c * half, half), half)
    other_rows = pl.ds(pl.multiple_of((1 - c) * half, half), half)
    own_share = pl.ds(pl.multiple_of(c * half + z * share, share), share)
    other_share = pl.ds(pl.multiple_of((1 - c) * half + z * share, share), share)

    row_number = lax.broadcasted_iota(jnp.int32, (tile_width, tile_width), 0)
    blank = jnp.zeros((tile_width, tile_width), bf16)

    top, low = slice(0, half), slice(half, width)

    def by_halves(left, right):
        return jnp.concatenate(
            [
                jnp.dot(left[rows], right, preferred_element_type=f32)
                for rows in (slice(0, half), slice(half, width))
            ],
            axis=0,
        )

    def picked(ids_ref, q, first):
        picks = []
        for tile in (first, first + 1):
            start = tile * tile_width
            inside = lax.rem(ids_ref[q, 0, :, start : start + tile_width], tile_width)
            picks.append(jnp.where(row_number == inside, 1.0, 0.0).astype(bf16))
        return picks

    def paired(picks):
        return jnp.concatenate(
            [
                jnp.concatenate([picks[0], blank], axis=1),
                jnp.concatenate([blank, picks[1]], axis=1),
            ],
            axis=0,
        )

    def block_of(scalar_ref, place, tile):
        return lax.div(scalar_ref[place, 0, 0, tile * tile_width], tile_width)

    def partial(pe, py, pc, head_blocks=head_ids, tail_blocks=tail_ids, place=None):
        q = pe * 4 + py * 2 + pc
        place = q if place is None else place
        for first in range(0, triples // tile_width, 2):
            cols = slice(first * tile_width, (first + 2) * tile_width)
            picks = picked(heads_ref, q, first)
            blocks = [turned[block_of(head_blocks, place, tile)] for tile in (first, first + 1)]
            rows = jnp.dot(
                jnp.concatenate(blocks, axis=1), paired(picks), preferred_element_type=f32
            )
            left_rows[:, cols] = (values_ref[q, 0, :, cols] * rows).astype(bf16)
            picks = [pick.T for pick in picked(tails_ref, q, first)]
            blocks = [
                factors_ref[block_of(tail_blocks, place, tile)] for tile in (first, first + 1)
            ]
            right_rows[cols, :] = jnp.dot(
                paired(picks), jnp.concatenate(blocks, axis=0), preferred_element_type=f32
            ).astype(bf16)
        return [
            jnp.dot(left_rows[rows, :], right_rows[...], preferred_element_type=f32)
            for rows in (top, low)
        ]

    targets = ((1 - e, 1 - y), (1 - e, y), (e, 1 - y), (e, y))
    pair_copies = []

    def give(index):
        pe, py = targets[index]
        pair_out[index, top], pair_out[index, low] = partial(pe, py, 1 - c)
        pair_copies.append(send(pair_out.at[index], pair_in.at[index], pair_peer))

    def keep(index):
        pe, py = targets[index]
        own_sum[index, top], own_sum[index, low] = partial(pe, py, c)

    def join(index):
        pair_copies[index].wait_recv()
        own_sum[index] = own_sum[index] + pair_in[index]

    for load in loads[:5]:
        load.wait()
    pair_out[0, top], pair_out[0, low] = partial(
        1 - e, 1 - y, 1 - c, first_heads, first_tails, 0
    )
    pl.semaphore_wait(barrier, len(near) + line_count)
    pair_top = send(pair_out.at[0, pl.ds(0, half)], pair_in.at[0, pl.ds(0, half)], pair_peer)
    pair_low = send(pair_out.at[0, pl.ds(half, half)], pair_in.at[0, pl.ds(half, half)], pair_peer)
    pair_copies.append(None)
    if z_count > 2:
        tell(ready.at[0])
    gram_part[...] = by_halves(
        jnp.concatenate(flipped, axis=1),
        jnp.concatenate([factors_ref[block] for block in range(block_count)], axis=0),
    )
    g_pair = send(gram_part.at[other_share], gram_in, pair_peer)
    for load in loads[5:]:
        load.wait()
    keep(0)
    g_pair.wait_recv()
    gram_half[0] = gram_part[own_share, :] + gram_in[...]
    upper, lower = pl.ds(0, part), pl.ds(part, part)
    g_a1 = send(gram_half.at[0, upper], gram_xy.at[0, upper], x_peer)
    g_b1 = send(gram_half.at[0, lower], gram_xy.at[0, lower], y_peer)
    pair_top.wait_recv()
    own_sum[0, top] = own_sum[0, top] + pair_in[0, top]
    a_diag = send(own_sum.at[0, pl.ds(0, half)], first_a.at[0], x_peer)
    pair_low.wait_recv()
    own_sum[0, low] = own_sum[0, low] + pair_in[0, low]
    b_diag = send(own_sum.at[0, pl.ds(half, half)], first_b.at[0], y_peer)
    give(1)
    give(2)
    for step in range(1, z_count - 2):
        pl.semaphore_wait(ready.at[step - 1], line_count)
        tell(ready.at[step])
    keep(1)
    g_a1.wait_recv()
    g_b1.wait_recv()
    gram_half[1] = gram_half[0] + gram_xy[0]
    g_a2 = send(gram_half.at[1, upper], gram_xy.at[1, upper], y_peer)
    g_b2 = send(gram_half.at[1, lower], gram_xy.at[1, lower], x_peer)
    join(1)
    a_side = send(own_sum.at[1, pl.ds(0, half)], first_a.at[1], x_peer)
    keep(2)
    join(2)
    b_side = send(own_sum.at[2, pl.ds(half, half)], first_b.at[1], y_peer)
    give(3)
    keep(3)
    a_diag.wait_recv()
    second_a[0] = own_sum[2, :half, :] + first_a[0]
    a_last = send(second_a.at[0], second_a.at[1], y_peer)
    b_diag.wait_recv()
    second_b[0] = own_sum[1, half:, :] + first_b[0]
    b_last = send(second_b.at[0], second_b.at[1], x_peer)
    g_a2.wait_recv()
    g_b2.wait_recv()
    gram_line[0] = gram_half[1] + gram_xy[1]
    if z_count > 2:
        pl.semaphore_wait(ready.at[z_count - 3], line_count)
    line_copies = [
        send(gram_line.at[0], gram_line.at[z_count - hop], z_peer(hop))
        for hop in range(1, z_count)
    ]
    join(3)
    for copy in line_copies:
        copy.wait_recv()
    for hop in range(z_count):
        place = lax.rem(z + hop, z_count)
        gram_pair[0, pl.ds(pl.multiple_of(place * share, share), share), :] = gram_line[hop]
    g_full = send(gram_pair.at[0], gram_pair.at[1], pair_peer)
    g_full.wait_recv()
    gram_full[own_rows, :] = gram_pair[0] * scale_gram
    gram_full[other_rows, :] = gram_pair[1] * scale_gram

    def split(value):
        high = value.astype(bf16)
        return high, (value - high.astype(f32)).astype(bf16)

    def fold(value):
        return jnp.sum(value.reshape(-1, 8, value.shape[1]), axis=0)

    def total(parts):
        added = parts[0]
        for piece in parts[1:]:
            added = added + piece
        return jnp.sum(jnp.sum(added, axis=0, keepdims=True), axis=1, keepdims=True)

    strips = [slice(first, first + STRIP) for first in range(0, width, STRIP)]
    panels = range(0, width, PANEL)
    gram = gram_full[...]
    gram_high, gram_low = split(gram)
    gram_twice = jnp.dot(gram_high, gram_high, preferred_element_type=f32) + (
        jnp.dot(gram_high, gram_low, preferred_element_type=f32)
        + jnp.dot(gram_low, gram_high, preferred_element_type=f32)
    )
    for power, (high, low_part) in enumerate(((gram_high, gram_low), split(gram_twice))):
        for third, piece in enumerate((high, low_part, high)):
            span = slice(third * width, (third + 1) * width)
            factor_left[power, :, span] = piece
            factor_right[power, span, :] = piece

    def spread_out(strip, value):
        high, low_part = split(value)
        for third, piece in enumerate((high, high, low_part)):
            vector_parts[
                slice(third * width + strip.start, third * width + strip.stop), :
            ] = piece
        return fold(value * value)

    a_side.wait_recv()
    b_side.wait_recv()
    a_last.wait_recv()
    b_last.wait_recv()
    squares = []
    for strip in strips:
        later = strip.start >= half
        inside = slice(strip.start - half, strip.stop - half) if later else strip
        side, last = (first_b, second_b) if later else (first_a, second_a)
        value = ((own_sum[3, strip, :] + side[1, inside, :]) + last[1, inside, :]) * scale_target
        basis[0, strip, :] = value
        squares.append(spread_out(strip, value))

    lane = lax.broadcasted_iota(jnp.int32, (1, 128), 1)
    record = jnp.zeros((1, 128), f32)

    def noted(record, place, value):
        return jnp.where(lane == place, value, record)

    def sized(square):
        inverse = jnp.where(square > 0.0, lax.rsqrt(square), 0.0)
        return inverse, square * inverse

    inverses, lengths, diagonals = [], [], []
    for index in range(0, ITERS, 2):
        for power in (0, 1):
            for first in panels:
                inner = jnp.dot(
                    factor_left[power, first : first + PANEL, :],
                    vector_parts[...],
                    preferred_element_type=f32,
                )
                for step in range(0, PANEL, STRIP):
                    high, low_part = split(inner[step : step + STRIP])
                    rows = slice(first + step, first + step + STRIP)
                    for third, piece in enumerate((high, high, low_part)):
                        inner_parts[power, rows, third * width : (third + 1) * width] = piece
        if index + 2 == ITERS:
            b_last.wait_send()
        crosses = []
        for power, dest in ((0, image), (1, image_twice)):
            for first in panels:
                outer = jnp.dot(
                    inner_parts[power, first : first + PANEL, :],
                    factor_right[power],
                    preferred_element_type=f32,
                )
                dest[first : first + PANEL, :] = outer
                for step in range(0, PANEL, STRIP):
                    if power == 0:
                        rows = slice(first + step, first + step + STRIP)
                        crosses.append(fold(outer[step : step + STRIP] * basis[index, rows, :]))
        inverse, length = sized(total(squares))
        diagonal = (total(crosses) * inverse) * inverse
        ready_now = diagonal == diagonal
        step_inverse = inverse
        scaled = diagonal * inverse
        ratio = length * inverses[-1] if index > 0 else None
        squares, crosses = [], []
        now, before = (index // 2) % 2, (index // 2 + 1) % 2
        for strip in strips:
            value = image[strip, :] * step_inverse - scaled * basis[index, strip, :]
            if index > 0:
                value = value - ratio * basis[index - 1, strip, :]
            basis[index + 1, strip, :] = value
            squares.append(fold(value * value))
            beyond = image_twice[strip, :] * step_inverse - scaled * image[strip, :]
            if index > 0:
                beyond = beyond - ratio * mapped[before, strip, :]
            mapped[now, strip, :] = beyond
            crosses.append(fold(value * beyond))
        next_inverse, next_length = sized(total(squares))
        next_diagonal = (total(crosses) * next_inverse) * next_inverse
        inverses += [inverse, next_inverse]
        lengths += [length, next_length]
        diagonals += [diagonal + ridge_weight, next_diagonal + ridge_weight]
        for place in (index, index + 1):
            record = noted(record, place, diagonals[place])
            record = noted(record, ITERS + place, lengths[place])
        if index + 4 == ITERS:
            early[0] = record
            early_copy = spread(early)
        if index + 2 == ITERS:
            late[0] = record
            late_copy = spread(late)
            a_last.wait_send()
        next_scaled, next_ratio = next_diagonal * next_inverse, next_length * inverse
        squares = []
        for strip in strips:
            value = (
                mapped[now, strip, :] * next_inverse - next_ratio * basis[index, strip, :]
            ) - next_scaled * basis[index + 1, strip, :]
            basis[index + 2, strip, :] = value
            if index + 2 < ITERS:
                squares.append(spread_out(strip, value))
    inverses.append(jnp.ones((1, 1), f32))
    for copy in sent:
        if copy is not a_last and copy is not b_last:
            copy.wait_send()

    def lanes_of(table):
        lines = table[...].reshape(8 * z_count, 128)
        blank_lines = jnp.zeros((128 - 8 * z_count, 128), f32)
        return jnp.concatenate([lines, blank_lines], axis=0).T

    def reduced(rows):
        added = rows[0]
        for row in rows[1:]:
            added = added + row
        return jnp.sum(added, axis=1, keepdims=True)

    def small_map(rows, alpha, beta):
        count = len(rows)
        made = []
        for j in range(min(count + 1, len(beta))):
            entry = None
            if j < count:
                entry = alpha[j] * rows[j]
            if j > 0:
                term = beta[j] * rows[j - 1]
                entry = term if entry is None else entry + term
            if j + 1 < count:
                entry = entry + beta[j + 1] * rows[j + 1]
            made.append(entry)
        return made

    def mixed_sum(first, ratio, second):
        return [
            one + ratio * second[j] if j < len(second) else one for j, one in enumerate(first)
        ]

    def products(residual, image):
        return (
            reduced([row * row for row in residual]),
            reduced([row * image[j] for j, row in enumerate(residual)]),
        )

    for place in range(2 * ITERS + 1):
        inverse = inverses[place if place < ITERS else place - ITERS]
        scale_ref[place : place + 1, :] = jnp.broadcast_to(inverse, (1, 128))
    early_copy.wait()
    filled = lanes_of(early)
    known = ITERS - 2
    alpha = [filled[j : j + 1, :] for j in range(known)]
    beta = [filled[ITERS + j : ITERS + j + 1, :] for j in range(known)]
    residual = [beta[0]]
    image = small_map(residual, alpha, beta)
    norm_now, product = products(residual, image)
    step_size = norm_now / product
    direction, along = residual, image
    fitted = []
    for index in range(known):
        if index == 0:
            fitted = [step_size * row for row in direction]
        else:
            fitted = [
                fitted[j] + step_size * row if j < len(fitted) else step_size * row
                for j, row in enumerate(direction)
            ]
        residual = [
            residual[j] - step_size * row if j < len(residual) else -(step_size * row)
            for j, row in enumerate(along)
        ]
        if index + 1 < known:
            image = small_map(residual, alpha, beta)
            norm_next, product = products(residual, image)
            ratio = norm_next / norm_now
            step_size = norm_next / (product - ratio * norm_next / step_size)
            direction = mixed_sum(residual, ratio, direction)
            along = mixed_sum(image, ratio, along)
            norm_now = norm_next

    late_copy.wait()
    filled = lanes_of(late)
    alpha += [filled[j : j + 1, :] for j in range(known, ITERS)]
    beta += [filled[ITERS + j : ITERS + j + 1, :] for j in range(known, ITERS)]
    beta.append(jnp.ones((1, 128), f32))
    along = along + [beta[known] * direction[-1]]
    residual = residual + [-(step_size * along[-1])]
    image = small_map(residual, alpha, beta)
    norm_next, product = products(residual, image)
    ratio = norm_next / norm_now
    step_next = norm_next / (product - ratio * norm_next / step_size)
    residual_before, image_before = residual, image
    residual = [
        residual[j] - step_next * row if j < len(residual) else -(step_next * row)
        for j, row in enumerate(mixed_sum(image, ratio, along))
    ]
    fitted = [
        fitted[j] + step_next * row if j < len(fitted) else step_next * row
        for j, row in enumerate(mixed_sum(residual_before, ratio, direction))
    ]
    image = small_map(residual, alpha, beta)
    norm_last, product = products(residual, image)
    ratio_last = norm_last / norm_next
    step_last = norm_last / (product - ratio_last * norm_last / step_next)
    direction = mixed_sum(residual, ratio_last, mixed_sum(residual_before, ratio, direction))
    along = mixed_sum(image, ratio_last, mixed_sum(image_before, ratio, along))
    fitted = [
        fitted[j] + step_last * row if j < len(fitted) else step_last * row
        for j, row in enumerate(direction)
    ]
    residual = [
        residual[j] - step_last * row if j < len(residual) else -(step_last * row)
        for j, row in enumerate(along)
    ]
    for place, row in enumerate(fitted + residual):
        mix_ref[place : place + 1, :] = row


def finish_kernel(
    basis, mix_ref, scale_ref, fit_hbm, res_hbm, fit_rows, res_rows, fit_sem, res_sem
):
    count = basis.shape[0] - 1
    width = basis.shape[2]
    own_weights = mix_ref[0 : 2 * count + 1, 0:1] * scale_ref[0 : 2 * count + 1, 0:1]
    spread_weights = jnp.broadcast_to(own_weights, (2 * count + 1, width))
    weights = [spread_weights[place : place + 1, :] for place in range(2 * count + 1)]
    height = fit_rows.shape[0] // CHUNKS
    copies = []
    for slot in range(CHUNKS):
        for first in range(slot * height, (slot + 1) * height, STRIP):
            strip = slice(first, first + STRIP)
            vector = basis[0, strip, :]
            fit, res = weights[0] * vector, weights[count] * vector
            for j in range(1, count + 1):
                vector = basis[j, strip, :]
                res = res + weights[count + j] * vector
                if j < count:
                    fit = fit + weights[j] * vector
            fit_rows[strip, :] = fit
            res_rows[strip, :] = res
        rows = pl.ds(slot * height, height)
        for source, dest, sem in ((fit_rows, fit_hbm, fit_sem), (res_rows, res_hbm, res_sem)):
            copies.append(
                pltpu.make_async_copy(source.at[rows], dest.at[0, rows], sem.at[slot])
            )
            copies[-1].start()
    for copy in copies:
        copy.wait()


def fused_body(factors, heads, tails, values):
    shards = lax.axis_size(("ent", "blk"))
    z_count = lax.axis_size("rel")
    ent_dev, width = factors.shape
    triples = heads.shape[3]
    half = width // 2
    f32, bf16 = jnp.float32, jnp.bfloat16
    vmem = pl.BlockSpec(memory_space=pltpu.VMEM)
    share = half // z_count
    basis, mix, scale = pl.pallas_call(
        functools.partial(
            fused_kernel, z_count, 1.0 / (ent_dev * shards), 1.0 / math.sqrt(shards * triples)
        ),
        out_shape=(
            pltpu.VMEM((ITERS + 1, width, width), f32),
            pltpu.VMEM((4 * ITERS, 128), f32),
            pltpu.VMEM((4 * ITERS, 128), f32),
        ),
        in_specs=[pl.BlockSpec(memory_space=pl.ANY)] * 4,
        out_specs=(vmem, vmem, vmem),
        scratch_shapes=[
            pltpu.VMEM((ent_dev // tile_width, tile_width, width), bf16),
            pltpu.VMEM(heads.shape, jnp.int32),
            pltpu.VMEM(tails.shape, jnp.int32),
            pltpu.VMEM(values.shape, f32),
            pltpu.SMEM(heads.shape, jnp.int32),
            pltpu.SMEM(tails.shape, jnp.int32),
            pltpu.SMEM((1,) + heads.shape[1:], jnp.int32),
            pltpu.SMEM((1,) + heads.shape[1:], jnp.int32),
            pltpu.SemaphoreType.DMA((ent_dev // tile_width,)),
            pltpu.SemaphoreType.DMA((7,)),
            pltpu.SemaphoreType.REGULAR((max(z_count - 2, 1),)),
            pltpu.VMEM((ent_dev // tile_width, width, tile_width), bf16),
            pltpu.VMEM((width, triples), bf16),
            pltpu.VMEM((triples, width), bf16),
            pltpu.VMEM((width, width), f32),
            pltpu.VMEM((share, width), f32),
            pltpu.VMEM((2, share, width), f32),
            pltpu.VMEM((2, share, width), f32),
            pltpu.VMEM((z_count, share, width), f32),
            pltpu.VMEM((width, width), f32),
            pltpu.VMEM((2, half, width), f32),
            pltpu.VMEM((4, width, width), f32),
            pltpu.VMEM((4, width, width), f32),
            pltpu.VMEM((4, width, width), f32),
            pltpu.VMEM((2, half, width), f32),
            pltpu.VMEM((2, half, width), f32),
            pltpu.VMEM((2, half, width), f32),
            pltpu.VMEM((2, half, width), f32),
            pltpu.VMEM((2, width, 3 * width), bf16),
            pltpu.VMEM((2, 3 * width, width), bf16),
            pltpu.VMEM((3 * width, width), bf16),
            pltpu.VMEM((2, width, 3 * width), bf16),
            pltpu.VMEM((width, width), f32),
            pltpu.VMEM((width, width), f32),
            pltpu.VMEM((2, width, width), f32),
            pltpu.VMEM((8 * z_count, 1, 128), f32),
            pltpu.VMEM((8 * z_count, 1, 128), f32),
            pltpu.SemaphoreType.DMA((COPIES,)),
            pltpu.SemaphoreType.DMA((COPIES,)),
        ],
        compiler_params=pltpu.CompilerParams(collective_id=0, has_side_effects=True),
    )(factors, heads, tails, values)
    out = jax.ShapeDtypeStruct((1, width, width), f32)
    anywhere = pl.BlockSpec(memory_space=pl.ANY)
    return pl.pallas_call(
        finish_kernel,
        out_shape=(out, out),
        in_specs=[vmem, vmem, vmem],
        out_specs=(anywhere, anywhere),
        scratch_shapes=[
            pltpu.VMEM((width, width), f32),
            pltpu.VMEM((width, width), f32),
            pltpu.SemaphoreType.DMA((CHUNKS,)),
            pltpu.SemaphoreType.DMA((CHUNKS,)),
        ],
        compiler_params=pltpu.CompilerParams(vmem_limit_bytes=16 * width * width * 4),
    )(basis, mix, scale)


def solution(mesh):
    placed = (
        P(("ent", "blk"), None),
        P(None, "rel", None, ("ent", "blk")),
        P(None, "rel", None, ("ent", "blk")),
        P(None, "rel", None, ("ent", "blk")),
    )
    sizes = dict(mesh.shape)
    fused = sizes["ent"] == 2 and sizes["blk"] == 4 and sizes["rel"] in (2, 4, 8)
    return jax.shard_map(
        fused_body if fused else body,
        mesh=mesh,
        in_specs=placed,
        out_specs=(P(("ent", "blk", "rel"), None, None), P(("ent", "blk", "rel"), None, None)),
        check_vma=False,
    )
```

```python
import functools
import math

import jax
import jax.numpy as jnp
from jax import lax
from jax.experimental import pallas as pl
from jax.experimental.pallas import tpu as pltpu
from jax.sharding import PartitionSpec as P

ITERS = 8


ridge_weight = 0.01
tile_width = 128


def apply_normal(gram_matrix, stacked):
    left_side = jnp.einsum("ab,kbc->kac", gram_matrix, stacked, precision=lax.Precision.HIGHEST)
    return (
        jnp.einsum("kac,cd->kad", left_side, gram_matrix, precision=lax.Precision.HIGHEST)
        + ridge_weight * stacked
    )


def two_products(residual, image_map):
    return lax.psum(
        (jnp.sum(residual * residual), jnp.sum(residual * image_map)), ("ent", "blk", "rel")
    )


def select_rows(entity_ids, block_table):
    group_size, width = entity_ids.shape
    tile_count = width // tile_width
    block_count = block_table.shape[0]
    tiled_ids = entity_ids.reshape(group_size, tile_count, tile_width)
    block_of = tiled_ids[:, :, 0] // tile_width
    block_pick = (
        block_of[:, :, None] == jnp.arange(block_count, dtype=jnp.int32)[None, None, :]
    ).astype(jnp.bfloat16)
    chosen = jnp.einsum(
        "gtb,bcr->gtcr", block_pick, block_table, preferred_element_type=jnp.float32
    ).astype(jnp.bfloat16)
    inside = tiled_ids % tile_width
    slot_pick = (
        inside[:, :, :, None] == jnp.arange(tile_width, dtype=jnp.int32)[None, None, None, :]
    ).astype(jnp.bfloat16)
    return jnp.einsum("gtoc,gtcr->gtor", slot_pick, chosen, preferred_element_type=jnp.float32)


def body(factors, heads, tails, values):
    shards = lax.axis_size(("ent", "blk"))
    ent_dev = factors.shape[0]
    rank_width = factors.shape[1]
    triple_count = heads.shape[3]
    relation_rows = heads.shape[0] * heads.shape[2]
    norm_scale = 1.0 / math.sqrt(shards * triple_count)
    gram_total = lax.psum(
        jnp.dot(factors.T, factors, preferred_element_type=jnp.float32), ("ent", "blk")
    )
    gram_matrix = gram_total / (ent_dev * shards)
    block_table = factors.reshape(ent_dev // tile_width, tile_width, rank_width)
    head_ids = heads.reshape(relation_rows, triple_count)
    tail_ids = tails.reshape(relation_rows, triple_count)
    weights = values.reshape(relation_rows, triple_count)

    def grouped(operands):
        head_group, tail_group, weight_group = operands
        group_size = head_group.shape[0]
        tile_count = triple_count // tile_width
        head_rows = select_rows(head_group, block_table)
        weighted = (
            weight_group.reshape(group_size, tile_count, tile_width)[:, :, :, None] * head_rows
        ).astype(jnp.bfloat16)
        tail_rows = select_rows(tail_group, block_table).astype(jnp.bfloat16)
        product = jnp.einsum(
            "gtci,gtcj->gij", weighted, tail_rows, preferred_element_type=jnp.float32
        )
        return product * norm_scale

    own_rows = relation_rows // shards
    group_size = math.gcd(own_rows * lax.axis_size(("ent", "blk")), 4)
    group_total = own_rows * lax.axis_size(("ent", "blk")) // group_size
    shaped = (
        head_ids.reshape(group_total, group_size, triple_count),
        tail_ids.reshape(group_total, group_size, triple_count),
        weights.reshape(group_total, group_size, triple_count),
    )
    results = lax.map(grouped, shaped)
    target = lax.psum_scatter(
        results.reshape(own_rows * lax.axis_size(("ent", "blk")), rank_width, rank_width),
        ("ent", "blk"),
        scatter_dimension=0,
        tiled=True,
    )
    fitted = jnp.zeros_like(target)
    residual = target
    image_map = apply_normal(gram_matrix, residual)
    norm_now, product = two_products(residual, image_map)
    step_size = norm_now / product
    direction = residual
    along = image_map
    for step_index in range(ITERS):
        fitted = fitted + step_size * direction
        residual = residual - step_size * along
        if step_index + 1 < ITERS:
            image_map = apply_normal(gram_matrix, residual)
            norm_next, product = two_products(residual, image_map)
            ratio_next = norm_next / norm_now
            step_size = norm_next / (product - ratio_next * norm_next / step_size)
            direction = residual + ratio_next * direction
            along = image_map + ratio_next * along
            norm_now = norm_next
    return (fitted, residual)


MESH = pl.DeviceIdType.MESH
COPIES = 22
CHUNKS = 4
STRIP = 32
PANEL = 128


def fused_kernel(
    z_count, scale_gram, scale_target,
    factors_hbm, heads_hbm, tails_hbm, values_hbm,
    basis, mix_ref, scale_ref,
    factors_ref, heads_ref, tails_ref, values_ref, head_ids, tail_ids,
    first_heads, first_tails, factor_sem, load_sem, ready,
    turned, left_rows, right_rows,
    gram_part, gram_in, gram_half, gram_xy, gram_line, gram_full, gram_pair,
    pair_out, pair_in, own_sum, first_a, first_b, second_a, second_b,
    factor_left, factor_right, vector_parts, inner_parts, image, image_twice, raw, mapped,
    early, late, send_sem, recv_sem,
):
    f32, bf16 = jnp.float32, jnp.bfloat16
    width = factors_ref.shape[2]
    half = width // 2
    share = half // z_count
    part = share // 2
    triples = heads_ref.shape[3]
    e = lax.axis_index("ent")
    b = lax.axis_index("blk")
    z = lax.axis_index("rel")
    y = b // 2
    c = b % 2
    pair_peer = (e, y * 2 + 1 - c, z)
    x_peer = (1 - e, b, z)
    y_peer = (e, (1 - y) * 2 + c, z)

    def group_peer(mask):
        me, my, mc = mask // 4, (mask // 2) % 2, mask % 2
        return (
            (1 - e) if me else e,
            ((1 - y) if my else y) * 2 + ((1 - c) if mc else c),
            z,
        )

    def z_peer(hop):
        return (e, b, lax.rem(z + hop, z_count))

    near = [group_peer(m) for m in (1, 2, 4)]
    inner = ((z > 0, -1), (z < z_count - 1, 1))

    def tell(semaphore):
        for present, hop in inner:
            @pl.when(present)
            def _():
                pl.semaphore_signal(
                    semaphore, inc=1, device_id=(e, b, z + hop), device_id_type=MESH
                )

    line_count = jnp.where(z > 0, 1, 0) + jnp.where(z < z_count - 1, 1, 0)
    barrier = pltpu.get_barrier_semaphore()
    for peer in near:
        pl.semaphore_signal(barrier, inc=1, device_id=peer, device_id_type=MESH)
    tell(barrier)
    first_q = (1 - e) * 4 + (1 - y) * 2 + 1 - c
    block_count = factors_ref.shape[0]
    factor_loads = []
    for block in range(block_count):
        rows = pl.ds(block * tile_width, tile_width)
        factor_loads.append(
            pltpu.make_async_copy(
                factors_hbm.at[rows], factors_ref.at[block], factor_sem.at[block]
            )
        )
        factor_loads[-1].start()
    loads = []
    for slot, (source, dest) in enumerate(
        (
            (heads_hbm.at[pl.ds(first_q, 1)], first_heads),
            (tails_hbm.at[pl.ds(first_q, 1)], first_tails),
            (heads_hbm, heads_ref),
            (values_hbm, values_ref),
            (tails_hbm, tails_ref),
            (heads_hbm, head_ids),
            (tails_hbm, tail_ids),
        )
    ):
        loads.append(pltpu.make_async_copy(source, dest, load_sem.at[slot]))
        loads[-1].start()

    counter = [0]
    sent = []

    def spare():
        slot = counter[0]
        counter[0] += 1
        return send_sem.at[slot], recv_sem.at[slot]

    def copy_to(source, dest, peer, pair):
        return pltpu.make_async_remote_copy(
            src_ref=source, dst_ref=dest, send_sem=pair[0], recv_sem=pair[1],
            device_id=peer, device_id_type=MESH,
        )

    def send(source, dest, peer):
        copy = copy_to(source, dest, peer, spare())
        copy.start()
        sent.append(copy)
        return copy

    far_peers = [
        (m, hop) for hop in (*range(1, z_count), 0) for m in (7, 6, 5, 3, 4, 2, 1, 0) if m or hop
    ]

    def spread(table):
        pair = spare()
        for m, hop in far_peers:
            peer = group_peer(m)[:2] + (lax.rem(z + hop, z_count),)
            place = m * z_count + (z_count - hop) % z_count
            copy_to(table.at[0], table.at[place], peer, pair).start()
        others = table.at[pl.ds(1, 8 * z_count - 1)]
        return copy_to(others, others, pair_peer, pair)

    flipped = []
    for block in range(block_count):
        factor_loads[block].wait()
        flipped.append(factors_ref[block].T)
        turned[block] = flipped[-1]
    own_rows = pl.ds(pl.multiple_of(c * half, half), half)
    other_rows = pl.ds(pl.multiple_of((1 - c) * half, half), half)
    own_share = pl.ds(pl.multiple_of(c * half + z * share, share), share)
    other_share = pl.ds(pl.multiple_of((1 - c) * half + z * share, share), share)

    row_number = lax.broadcasted_iota(jnp.int32, (tile_width, tile_width), 0)
    blank = jnp.zeros((tile_width, tile_width), bf16)

    top, low = slice(0, half), slice(half, width)

    def by_halves(left, right):
        return jnp.concatenate(
            [
                jnp.dot(left[rows], right, preferred_element_type=f32)
                for rows in (slice(0, half), slice(half, width))
            ],
            axis=0,
        )

    def picked(ids_ref, q, first):
        picks = []
        for tile in (first, first + 1):
            start = tile * tile_width
            inside = lax.rem(ids_ref[q, 0, :, start : start + tile_width], tile_width)
            picks.append(jnp.where(row_number == inside, 1.0, 0.0).astype(bf16))
        return picks

    def paired(picks):
        return jnp.concatenate(
            [
                jnp.concatenate([picks[0], blank], axis=1),
                jnp.concatenate([blank, picks[1]], axis=1),
            ],
            axis=0,
        )

    def block_of(scalar_ref, place, tile):
        return lax.div(scalar_ref[place, 0, 0, tile * tile_width], tile_width)

    def partial(pe, py, pc, head_blocks=head_ids, tail_blocks=tail_ids, place=None):
        q = pe * 4 + py * 2 + pc
        place = q if place is None else place
        for first in range(0, triples // tile_width, 2):
            cols = slice(first * tile_width, (first + 2) * tile_width)
            picks = picked(heads_ref, q, first)
            blocks = [turned[block_of(head_blocks, place, tile)] for tile in (first, first + 1)]
            rows = jnp.dot(
                jnp.concatenate(blocks, axis=1), paired(picks), preferred_element_type=f32
            )
            left_rows[:, cols] = (values_ref[q, 0, :, cols] * rows).astype(bf16)
            picks = [pick.T for pick in picked(tails_ref, q, first)]
            blocks = [
                factors_ref[block_of(tail_blocks, place, tile)] for tile in (first, first + 1)
            ]
            right_rows[cols, :] = jnp.dot(
                paired(picks), jnp.concatenate(blocks, axis=0), preferred_element_type=f32
            ).astype(bf16)
        return [
            jnp.dot(left_rows[rows, :], right_rows[...], preferred_element_type=f32)
            for rows in (top, low)
        ]

    targets = ((1 - e, 1 - y), (1 - e, y), (e, 1 - y), (e, y))
    pair_copies = []

    def give(index):
        pe, py = targets[index]
        pair_out[index, top], pair_out[index, low] = partial(pe, py, 1 - c)
        pair_copies.append(send(pair_out.at[index], pair_in.at[index], pair_peer))

    def keep(index):
        pe, py = targets[index]
        own_sum[index, top], own_sum[index, low] = partial(pe, py, c)

    def join(index):
        pair_copies[index].wait_recv()
        own_sum[index] = own_sum[index] + pair_in[index]

    for load in loads[:5]:
        load.wait()
    pair_out[0, top], pair_out[0, low] = partial(
        1 - e, 1 - y, 1 - c, first_heads, first_tails, 0
    )
    pl.semaphore_wait(barrier, len(near) + line_count)
    pair_top = send(pair_out.at[0, pl.ds(0, half)], pair_in.at[0, pl.ds(0, half)], pair_peer)
    pair_low = send(pair_out.at[0, pl.ds(half, half)], pair_in.at[0, pl.ds(half, half)], pair_peer)
    pair_copies.append(None)
    if z_count > 2:
        tell(ready.at[0])
    gram_part[...] = by_halves(
        jnp.concatenate(flipped, axis=1),
        jnp.concatenate([factors_ref[block] for block in range(block_count)], axis=0),
    )
    g_pair = send(gram_part.at[other_share], gram_in, pair_peer)
    for load in loads[5:]:
        load.wait()
    keep(0)
    g_pair.wait_recv()
    gram_half[0] = gram_part[own_share, :] + gram_in[...]
    upper, lower = pl.ds(0, part), pl.ds(part, part)
    g_a1 = send(gram_half.at[0, upper], gram_xy.at[0, upper], x_peer)
    g_b1 = send(gram_half.at[0, lower], gram_xy.at[0, lower], y_peer)
    pair_top.wait_recv()
    own_sum[0, top] = own_sum[0, top] + pair_in[0, top]
    a_diag = send(own_sum.at[0, pl.ds(0, half)], first_a.at[0], x_peer)
    pair_low.wait_recv()
    own_sum[0, low] = own_sum[0, low] + pair_in[0, low]
    b_diag = send(own_sum.at[0, pl.ds(half, half)], first_b.at[0], y_peer)
    give(1)
    give(2)
    for step in range(1, z_count - 2):
        pl.semaphore_wait(ready.at[step - 1], line_count)
        tell(ready.at[step])
    keep(1)
    g_a1.wait_recv()
    g_b1.wait_recv()
    gram_half[1] = gram_half[0] + gram_xy[0]
    g_a2 = send(gram_half.at[1, upper], gram_xy.at[1, upper], y_peer)
    g_b2 = send(gram_half.at[1, lower], gram_xy.at[1, lower], x_peer)
    join(1)
    a_side = send(own_sum.at[1, pl.ds(0, half)], first_a.at[1], x_peer)
    keep(2)
    join(2)
    b_side = send(own_sum.at[2, pl.ds(half, half)], first_b.at[1], y_peer)
    give(3)
    keep(3)
    a_diag.wait_recv()
    second_a[0] = own_sum[2, :half, :] + first_a[0]
    a_last = send(second_a.at[0], second_a.at[1], y_peer)
    b_diag.wait_recv()
    second_b[0] = own_sum[1, half:, :] + first_b[0]
    b_last = send(second_b.at[0], second_b.at[1], x_peer)
    g_a2.wait_recv()
    g_b2.wait_recv()
    gram_line[0] = gram_half[1] + gram_xy[1]
    if z_count > 2:
        pl.semaphore_wait(ready.at[z_count - 3], line_count)
    line_copies = [
        send(gram_line.at[0], gram_line.at[z_count - hop], z_peer(hop))
        for hop in range(1, z_count)
    ]
    join(3)
    for copy in line_copies:
        copy.wait_recv()
    for hop in range(z_count):
        place = lax.rem(z + hop, z_count)
        gram_pair[0, pl.ds(pl.multiple_of(place * share, share), share), :] = gram_line[hop]
    g_full = send(gram_pair.at[0], gram_pair.at[1], pair_peer)
    g_full.wait_recv()
    gram_full[own_rows, :] = gram_pair[0] * scale_gram
    gram_full[other_rows, :] = gram_pair[1] * scale_gram

    def split(value):
        high = value.astype(bf16)
        return high, (value - high.astype(f32)).astype(bf16)

    def fold(value):
        return jnp.sum(value.reshape(-1, 8, value.shape[1]), axis=0)

    def total(parts):
        added = parts[0]
        for piece in parts[1:]:
            added = added + piece
        return jnp.sum(jnp.sum(added, axis=0, keepdims=True), axis=1, keepdims=True)

    strips = [slice(first, first + STRIP) for first in range(0, width, STRIP)]
    panels = range(0, width, PANEL)
    gram = gram_full[...]
    gram_high, gram_low = split(gram)
    gram_twice = jnp.dot(gram_high, gram_high, preferred_element_type=f32) + (
        jnp.dot(gram_high, gram_low, preferred_element_type=f32)
        + jnp.dot(gram_low, gram_high, preferred_element_type=f32)
    )
    for power, (high, low_part) in enumerate(((gram_high, gram_low), split(gram_twice))):
        for third, piece in enumerate((high, low_part, high)):
            span = slice(third * width, (third + 1) * width)
            factor_left[power, :, span] = piece
            factor_right[power, span, :] = piece

    def spread_out(strip, value):
        high, low_part = split(value)
        for third, piece in enumerate((high, high, low_part)):
            vector_parts[
                slice(third * width + strip.start, third * width + strip.stop), :
            ] = piece
        return fold(value * value)

    a_side.wait_recv()
    b_side.wait_recv()
    a_last.wait_recv()
    b_last.wait_recv()
    squares = []
    for strip in strips:
        later = strip.start >= half
        inside = slice(strip.start - half, strip.stop - half) if later else strip
        side, last = (first_b, second_b) if later else (first_a, second_a)
        value = ((own_sum[3, strip, :] + side[1, inside, :]) + last[1, inside, :]) * scale_target
        basis[0, strip, :] = value
        squares.append(spread_out(strip, value))

    lane = lax.broadcasted_iota(jnp.int32, (1, 128), 1)
    record = jnp.zeros((1, 128), f32)

    def noted(record, place, value):
        return jnp.where(lane == place, value, record)

    def sized(square):
        inverse = jnp.where(square > 0.0, lax.rsqrt(square), 0.0)
        return inverse, square * inverse

    def left_stage():
        for power in (0, 1):
            for first in panels:
                inner = jnp.dot(
                    factor_left[power, first : first + PANEL, :],
                    vector_parts[...],
                    preferred_element_type=f32,
                )
                for step in range(0, PANEL, STRIP):
                    high, low_part = split(inner[step : step + STRIP])
                    rows = slice(first + step, first + step + STRIP)
                    for third, piece in enumerate((high, high, low_part)):
                        inner_parts[power, rows, third * width : (third + 1) * width] = piece

    def right_stage(power, put):
        for first in panels:
            outer = jnp.dot(
                inner_parts[power, first : first + PANEL, :],
                factor_right[power],
                preferred_element_type=f32,
            )
            for step in range(0, PANEL, STRIP):
                put(slice(first + step, first + step + STRIP), outer[step : step + STRIP])

    inverses, lengths, diagonals = [], [], []
    crosses = []

    def put_image(strip, value):
        image[strip, :] = value
        crosses.append(fold(value * basis[0, strip, :]))

    def put_twice(strip, value):
        image_twice[strip, :] = value

    left_stage()
    right_stage(0, put_image)
    right_stage(1, put_twice)
    for index in range(0, ITERS, 2):
        inverse, length = sized(total(squares))
        diagonal = (total(crosses) * inverse) * inverse
        scaled = diagonal * inverse
        ratio = length * inverses[-1] if index > 0 else None
        squares, crosses = [], []
        now, before = (index // 2) % 2, (index // 2 + 1) % 2
        for strip in strips:
            value = image[strip, :] * inverse - scaled * basis[index, strip, :]
            if index > 0:
                value = value - ratio * basis[index - 1, strip, :]
            basis[index + 1, strip, :] = value
            squares.append(fold(value * value))
            beyond = image_twice[strip, :] * inverse - scaled * image[strip, :]
            if index > 0:
                beyond = beyond - ratio * mapped[before, strip, :]
            mapped[now, strip, :] = beyond
            crosses.append(fold(value * beyond))
            if index + 2 < ITERS:
                spread_out(strip, beyond)
        if index + 2 < ITERS:
            left_stage()
        next_inverse, next_length = sized(total(squares))
        next_diagonal = (total(crosses) * next_inverse) * next_inverse
        inverses += [inverse, next_inverse]
        lengths += [length, next_length]
        diagonals += [diagonal + ridge_weight, next_diagonal + ridge_weight]
        for place in (index, index + 1):
            record = noted(record, place, diagonals[place])
            record = noted(record, ITERS + place, lengths[place])
        if index + 4 == ITERS:
            early[0] = record
            early_copy = spread(early)
            b_last.wait_send()
        if index + 2 == ITERS:
            late[0] = record
            late_copy = spread(late)
            a_last.wait_send()
        next_scaled, next_ratio = next_diagonal * next_inverse, next_length * inverse
        squares, crosses = [], []
        for strip in strips:
            value = (
                mapped[now, strip, :] * next_inverse - next_ratio * basis[index, strip, :]
            ) - next_scaled * basis[index + 1, strip, :]
            basis[index + 2, strip, :] = value
            if index + 2 < ITERS:
                squares.append(fold(value * value))

        def next_image(strip, outer):
            raw[strip, :] = outer
            value = (
                outer * next_inverse - next_scaled * mapped[now, strip, :]
            ) - next_ratio * image[strip, :]
            image[strip, :] = value
            crosses.append(fold(value * basis[index + 2, strip, :]))

        def next_twice(strip, outer):
            image_twice[strip, :] = (
                outer * next_inverse - next_scaled * raw[strip, :]
            ) - next_ratio * image_twice[strip, :]

        if index + 2 < ITERS:
            right_stage(0, next_image)
            right_stage(1, next_twice)
    inverses.append(jnp.ones((1, 1), f32))
    for copy in sent:
        if copy is not a_last and copy is not b_last:
            copy.wait_send()

    def lanes_of(table):
        lines = table[...].reshape(8 * z_count, 128)
        blank_lines = jnp.zeros((128 - 8 * z_count, 128), f32)
        return jnp.concatenate([lines, blank_lines], axis=0).T

    def reduced(rows):
        added = rows[0]
        for row in rows[1:]:
            added = added + row
        return jnp.sum(added, axis=1, keepdims=True)

    def small_map(rows, alpha, beta):
        count = len(rows)
        made = []
        for j in range(min(count + 1, len(beta))):
            entry = None
            if j < count:
                entry = alpha[j] * rows[j]
            if j > 0:
                term = beta[j] * rows[j - 1]
                entry = term if entry is None else entry + term
            if j + 1 < count:
                entry = entry + beta[j + 1] * rows[j + 1]
            made.append(entry)
        return made

    def mixed_sum(first, ratio, second):
        return [
            one + ratio * second[j] if j < len(second) else one for j, one in enumerate(first)
        ]

    def products(residual, image):
        return (
            reduced([row * row for row in residual]),
            reduced([row * image[j] for j, row in enumerate(residual)]),
        )

    for place in range(2 * ITERS + 1):
        inverse = inverses[place if place < ITERS else place - ITERS]
        scale_ref[place : place + 1, :] = jnp.broadcast_to(inverse, (1, 128))
    early_copy.wait()
    filled = lanes_of(early)
    known = ITERS - 2
    alpha = [filled[j : j + 1, :] for j in range(known)]
    beta = [filled[ITERS + j : ITERS + j + 1, :] for j in range(known)]
    residual = [beta[0]]
    image = small_map(residual, alpha, beta)
    norm_now, product = products(residual, image)
    step_size = norm_now / product
    direction, along = residual, image
    fitted = []
    for index in range(known):
        if index == 0:
            fitted = [step_size * row for row in direction]
        else:
            fitted = [
                fitted[j] + step_size * row if j < len(fitted) else step_size * row
                for j, row in enumerate(direction)
            ]
        residual = [
            residual[j] - step_size * row if j < len(residual) else -(step_size * row)
            for j, row in enumerate(along)
        ]
        if index + 1 < known:
            image = small_map(residual, alpha, beta)
            norm_next, product = products(residual, image)
            ratio = norm_next / norm_now
            step_size = norm_next / (product - ratio * norm_next / step_size)
            direction = mixed_sum(residual, ratio, direction)
            along = mixed_sum(image, ratio, along)
            norm_now = norm_next

    late_copy.wait()
    filled = lanes_of(late)
    alpha += [filled[j : j + 1, :] for j in range(known, ITERS)]
    beta += [filled[ITERS + j : ITERS + j + 1, :] for j in range(known, ITERS)]
    beta.append(jnp.ones((1, 128), f32))
    along = along + [beta[known] * direction[-1]]
    residual = residual + [-(step_size * along[-1])]
    image = small_map(residual, alpha, beta)
    norm_next, product = products(residual, image)
    ratio = norm_next / norm_now
    step_next = norm_next / (product - ratio * norm_next / step_size)
    residual_before, image_before = residual, image
    residual = [
        residual[j] - step_next * row if j < len(residual) else -(step_next * row)
        for j, row in enumerate(mixed_sum(image, ratio, along))
    ]
    fitted = [
        fitted[j] + step_next * row if j < len(fitted) else step_next * row
        for j, row in enumerate(mixed_sum(residual_before, ratio, direction))
    ]
    image = small_map(residual, alpha, beta)
    norm_last, product = products(residual, image)
    ratio_last = norm_last / norm_next
    step_last = norm_last / (product - ratio_last * norm_last / step_next)
    direction = mixed_sum(residual, ratio_last, mixed_sum(residual_before, ratio, direction))
    along = mixed_sum(image, ratio_last, mixed_sum(image_before, ratio, along))
    fitted = [
        fitted[j] + step_last * row if j < len(fitted) else step_last * row
        for j, row in enumerate(direction)
    ]
    residual = [
        residual[j] - step_last * row if j < len(residual) else -(step_last * row)
        for j, row in enumerate(along)
    ]
    for place, row in enumerate(fitted + residual):
        mix_ref[place : place + 1, :] = row


def finish_kernel(
    basis, mix_ref, scale_ref, fit_hbm, res_hbm, fit_rows, res_rows, fit_sem, res_sem
):
    count = basis.shape[0] - 1
    width = basis.shape[2]
    own_weights = mix_ref[0 : 2 * count + 1, 0:1] * scale_ref[0 : 2 * count + 1, 0:1]
    spread_weights = jnp.broadcast_to(own_weights, (2 * count + 1, width))
    weights = [spread_weights[place : place + 1, :] for place in range(2 * count + 1)]
    height = fit_rows.shape[0] // CHUNKS
    copies = []
    for slot in range(CHUNKS):
        for first in range(slot * height, (slot + 1) * height, STRIP):
            strip = slice(first, first + STRIP)
            vector = basis[0, strip, :]
            fit, res = weights[0] * vector, weights[count] * vector
            for j in range(1, count + 1):
                vector = basis[j, strip, :]
                res = res + weights[count + j] * vector
                if j < count:
                    fit = fit + weights[j] * vector
            fit_rows[strip, :] = fit
            res_rows[strip, :] = res
        rows = pl.ds(slot * height, height)
        for source, dest, sem in ((fit_rows, fit_hbm, fit_sem), (res_rows, res_hbm, res_sem)):
            copies.append(
                pltpu.make_async_copy(source.at[rows], dest.at[0, rows], sem.at[slot])
            )
            copies[-1].start()
    for copy in copies:
        copy.wait()


def fused_body(factors, heads, tails, values):
    shards = lax.axis_size(("ent", "blk"))
    z_count = lax.axis_size("rel")
    ent_dev, width = factors.shape
    triples = heads.shape[3]
    half = width // 2
    f32, bf16 = jnp.float32, jnp.bfloat16
    vmem = pl.BlockSpec(memory_space=pltpu.VMEM)
    share = half // z_count
    basis, mix, scale = pl.pallas_call(
        functools.partial(
            fused_kernel, z_count, 1.0 / (ent_dev * shards), 1.0 / math.sqrt(shards * triples)
        ),
        out_shape=(
            pltpu.VMEM((ITERS + 1, width, width), f32),
            pltpu.VMEM((4 * ITERS, 128), f32),
            pltpu.VMEM((4 * ITERS, 128), f32),
        ),
        in_specs=[pl.BlockSpec(memory_space=pl.ANY)] * 4,
        out_specs=(vmem, vmem, vmem),
        scratch_shapes=[
            pltpu.VMEM((ent_dev // tile_width, tile_width, width), bf16),
            pltpu.VMEM(heads.shape, jnp.int32),
            pltpu.VMEM(tails.shape, jnp.int32),
            pltpu.VMEM(values.shape, f32),
            pltpu.SMEM(heads.shape, jnp.int32),
            pltpu.SMEM(tails.shape, jnp.int32),
            pltpu.SMEM((1,) + heads.shape[1:], jnp.int32),
            pltpu.SMEM((1,) + heads.shape[1:], jnp.int32),
            pltpu.SemaphoreType.DMA((ent_dev // tile_width,)),
            pltpu.SemaphoreType.DMA((7,)),
            pltpu.SemaphoreType.REGULAR((max(z_count - 2, 1),)),
            pltpu.VMEM((ent_dev // tile_width, width, tile_width), bf16),
            pltpu.VMEM((width, triples), bf16),
            pltpu.VMEM((triples, width), bf16),
            pltpu.VMEM((width, width), f32),
            pltpu.VMEM((share, width), f32),
            pltpu.VMEM((2, share, width), f32),
            pltpu.VMEM((2, share, width), f32),
            pltpu.VMEM((z_count, share, width), f32),
            pltpu.VMEM((width, width), f32),
            pltpu.VMEM((2, half, width), f32),
            pltpu.VMEM((4, width, width), f32),
            pltpu.VMEM((4, width, width), f32),
            pltpu.VMEM((4, width, width), f32),
            pltpu.VMEM((2, half, width), f32),
            pltpu.VMEM((2, half, width), f32),
            pltpu.VMEM((2, half, width), f32),
            pltpu.VMEM((2, half, width), f32),
            pltpu.VMEM((2, width, 3 * width), bf16),
            pltpu.VMEM((2, 3 * width, width), bf16),
            pltpu.VMEM((3 * width, width), bf16),
            pltpu.VMEM((2, width, 3 * width), bf16),
            pltpu.VMEM((width, width), f32),
            pltpu.VMEM((width, width), f32),
            pltpu.VMEM((width, width), f32),
            pltpu.VMEM((2, width, width), f32),
            pltpu.VMEM((8 * z_count, 1, 128), f32),
            pltpu.VMEM((8 * z_count, 1, 128), f32),
            pltpu.SemaphoreType.DMA((COPIES,)),
            pltpu.SemaphoreType.DMA((COPIES,)),
        ],
        compiler_params=pltpu.CompilerParams(collective_id=0, has_side_effects=True),
    )(factors, heads, tails, values)
    out = jax.ShapeDtypeStruct((1, width, width), f32)
    anywhere = pl.BlockSpec(memory_space=pl.ANY)
    return pl.pallas_call(
        finish_kernel,
        out_shape=(out, out),
        in_specs=[vmem, vmem, vmem],
        out_specs=(anywhere, anywhere),
        scratch_shapes=[
            pltpu.VMEM((width, width), f32),
            pltpu.VMEM((width, width), f32),
            pltpu.SemaphoreType.DMA((CHUNKS,)),
            pltpu.SemaphoreType.DMA((CHUNKS,)),
        ],
        compiler_params=pltpu.CompilerParams(vmem_limit_bytes=16 * width * width * 4),
    )(basis, mix, scale)


def solution(mesh):
    placed = (
        P(("ent", "blk"), None),
        P(None, "rel", None, ("ent", "blk")),
        P(None, "rel", None, ("ent", "blk")),
        P(None, "rel", None, ("ent", "blk")),
    )
    sizes = dict(mesh.shape)
    fused = sizes["ent"] == 2 and sizes["blk"] == 4 and sizes["rel"] in (2, 4, 8)
    return jax.shard_map(
        fused_body if fused else body,
        mesh=mesh,
        in_specs=placed,
        out_specs=(P(("ent", "blk", "rel"), None, None), P(("ent", "blk", "rel"), None, None)),
        check_vma=False,
    )
```

```python
import functools
import math

import jax
import jax.numpy as jnp
from jax import lax
from jax.experimental import pallas as pl
from jax.experimental.pallas import tpu as pltpu
from jax.sharding import PartitionSpec as P

ITERS = 8


ridge_weight = 0.01
tile_width = 128


def apply_normal(gram_matrix, stacked):
    left_side = jnp.einsum("ab,kbc->kac", gram_matrix, stacked, precision=lax.Precision.HIGHEST)
    return (
        jnp.einsum("kac,cd->kad", left_side, gram_matrix, precision=lax.Precision.HIGHEST)
        + ridge_weight * stacked
    )


def two_products(residual, image_map):
    return lax.psum(
        (jnp.sum(residual * residual), jnp.sum(residual * image_map)), ("ent", "blk", "rel")
    )


def select_rows(entity_ids, block_table):
    group_size, width = entity_ids.shape
    tile_count = width // tile_width
    block_count = block_table.shape[0]
    tiled_ids = entity_ids.reshape(group_size, tile_count, tile_width)
    block_of = tiled_ids[:, :, 0] // tile_width
    block_pick = (
        block_of[:, :, None] == jnp.arange(block_count, dtype=jnp.int32)[None, None, :]
    ).astype(jnp.bfloat16)
    chosen = jnp.einsum(
        "gtb,bcr->gtcr", block_pick, block_table, preferred_element_type=jnp.float32
    ).astype(jnp.bfloat16)
    inside = tiled_ids % tile_width
    slot_pick = (
        inside[:, :, :, None] == jnp.arange(tile_width, dtype=jnp.int32)[None, None, None, :]
    ).astype(jnp.bfloat16)
    return jnp.einsum("gtoc,gtcr->gtor", slot_pick, chosen, preferred_element_type=jnp.float32)


def body(factors, heads, tails, values):
    shards = lax.axis_size(("ent", "blk"))
    ent_dev = factors.shape[0]
    rank_width = factors.shape[1]
    triple_count = heads.shape[3]
    relation_rows = heads.shape[0] * heads.shape[2]
    norm_scale = 1.0 / math.sqrt(shards * triple_count)
    gram_total = lax.psum(
        jnp.dot(factors.T, factors, preferred_element_type=jnp.float32), ("ent", "blk")
    )
    gram_matrix = gram_total / (ent_dev * shards)
    block_table = factors.reshape(ent_dev // tile_width, tile_width, rank_width)
    head_ids = heads.reshape(relation_rows, triple_count)
    tail_ids = tails.reshape(relation_rows, triple_count)
    weights = values.reshape(relation_rows, triple_count)

    def grouped(operands):
        head_group, tail_group, weight_group = operands
        group_size = head_group.shape[0]
        tile_count = triple_count // tile_width
        head_rows = select_rows(head_group, block_table)
        weighted = (
            weight_group.reshape(group_size, tile_count, tile_width)[:, :, :, None] * head_rows
        ).astype(jnp.bfloat16)
        tail_rows = select_rows(tail_group, block_table).astype(jnp.bfloat16)
        product = jnp.einsum(
            "gtci,gtcj->gij", weighted, tail_rows, preferred_element_type=jnp.float32
        )
        return product * norm_scale

    own_rows = relation_rows // shards
    group_size = math.gcd(own_rows * lax.axis_size(("ent", "blk")), 4)
    group_total = own_rows * lax.axis_size(("ent", "blk")) // group_size
    shaped = (
        head_ids.reshape(group_total, group_size, triple_count),
        tail_ids.reshape(group_total, group_size, triple_count),
        weights.reshape(group_total, group_size, triple_count),
    )
    results = lax.map(grouped, shaped)
    target = lax.psum_scatter(
        results.reshape(own_rows * lax.axis_size(("ent", "blk")), rank_width, rank_width),
        ("ent", "blk"),
        scatter_dimension=0,
        tiled=True,
    )
    fitted = jnp.zeros_like(target)
    residual = target
    image_map = apply_normal(gram_matrix, residual)
    norm_now, product = two_products(residual, image_map)
    step_size = norm_now / product
    direction = residual
    along = image_map
    for step_index in range(ITERS):
        fitted = fitted + step_size * direction
        residual = residual - step_size * along
        if step_index + 1 < ITERS:
            image_map = apply_normal(gram_matrix, residual)
            norm_next, product = two_products(residual, image_map)
            ratio_next = norm_next / norm_now
            step_size = norm_next / (product - ratio_next * norm_next / step_size)
            direction = residual + ratio_next * direction
            along = image_map + ratio_next * along
            norm_now = norm_next
    return (fitted, residual)


MESH = pl.DeviceIdType.MESH
COPIES = 20
CHUNKS = 4
STRIP = 32
PANEL = 128


def fused_kernel(
    z_count, scale_gram, scale_target,
    factors_hbm, heads_hbm, tails_hbm, values_hbm,
    basis, mix_ref, scale_ref,
    factors_ref, heads_ref, tails_ref, values_ref, head_ids, tail_ids,
    first_heads, first_tails, factor_sem, load_sem, ready,
    turned, left_rows, right_rows,
    gram_part, gram_in, gram_half, gram_xy, gram_line, gram_full, gram_pair,
    pair_out, pair_in, own_sum, first_a, first_b, second_a, second_b,
    factor_left, factor_right, vector_parts, inner_parts, image, image_twice, raw, mapped,
    early, late, send_sem, recv_sem,
):
    f32, bf16 = jnp.float32, jnp.bfloat16
    width = factors_ref.shape[2]
    half = width // 2
    share = half // z_count
    part = share // 2
    triples = heads_ref.shape[3]
    e = lax.axis_index("ent")
    b = lax.axis_index("blk")
    z = lax.axis_index("rel")
    y = b // 2
    c = b % 2
    pair_peer = (e, y * 2 + 1 - c, z)
    x_peer = (1 - e, b, z)
    y_peer = (e, (1 - y) * 2 + c, z)

    def group_peer(mask):
        me, my, mc = mask // 4, (mask // 2) % 2, mask % 2
        return (
            (1 - e) if me else e,
            ((1 - y) if my else y) * 2 + ((1 - c) if mc else c),
            z,
        )

    def z_peer(hop):
        return (e, b, lax.rem(z + hop, z_count))

    near = [group_peer(m) for m in (1, 2, 4)]
    inner = ((z > 0, -1), (z < z_count - 1, 1))

    def tell(semaphore):
        for present, hop in inner:
            @pl.when(present)
            def _():
                pl.semaphore_signal(
                    semaphore, inc=1, device_id=(e, b, z + hop), device_id_type=MESH
                )

    line_count = jnp.where(z > 0, 1, 0) + jnp.where(z < z_count - 1, 1, 0)
    barrier = pltpu.get_barrier_semaphore()
    for peer in near:
        pl.semaphore_signal(barrier, inc=1, device_id=peer, device_id_type=MESH)
    tell(barrier)
    first_q = (1 - e) * 4 + (1 - y) * 2 + 1 - c
    block_count = factors_ref.shape[0]
    factor_load = pltpu.make_async_copy(factors_hbm, factors_ref, factor_sem)
    factor_load.start()
    loads = []
    for slot, (source, dest) in enumerate(
        (
            (heads_hbm.at[pl.ds(first_q, 1)], first_heads),
            (tails_hbm.at[pl.ds(first_q, 1)], first_tails),
            (heads_hbm, heads_ref),
            (values_hbm, values_ref),
            (tails_hbm, tails_ref),
            (heads_hbm, head_ids),
            (tails_hbm, tail_ids),
        )
    ):
        loads.append(pltpu.make_async_copy(source, dest, load_sem.at[slot]))
        loads[-1].start()

    counter = [0]
    sent = []

    def spare():
        slot = counter[0]
        counter[0] += 1
        return send_sem.at[slot], recv_sem.at[slot]

    def copy_to(source, dest, peer, pair):
        return pltpu.make_async_remote_copy(
            src_ref=source, dst_ref=dest, send_sem=pair[0], recv_sem=pair[1],
            device_id=peer, device_id_type=MESH,
        )

    def send(source, dest, peer):
        copy = copy_to(source, dest, peer, spare())
        copy.start()
        sent.append(copy)
        return copy

    far_peers = [
        (m, hop) for hop in (*range(1, z_count), 0) for m in (7, 6, 5, 3, 4, 2, 1, 0) if m or hop
    ]

    def spread(table):
        pair = spare()
        for m, hop in far_peers:
            peer = group_peer(m)[:2] + (lax.rem(z + hop, z_count),)
            place = m * z_count + (z_count - hop) % z_count
            copy_to(table.at[0], table.at[place], peer, pair).start()
        others = table.at[pl.ds(1, 8 * z_count - 1)]
        return copy_to(others, others, pair_peer, pair)

    flipped = []
    factor_load.wait()
    for block in range(block_count):
        flipped.append(factors_ref[block].T)
        turned[block] = flipped[-1]
    own_rows = pl.ds(pl.multiple_of(c * half, half), half)
    other_rows = pl.ds(pl.multiple_of((1 - c) * half, half), half)
    own_share = pl.ds(pl.multiple_of(c * half + z * share, share), share)
    other_share = pl.ds(pl.multiple_of((1 - c) * half + z * share, share), share)

    row_number = lax.broadcasted_iota(jnp.int32, (tile_width, tile_width), 0)
    blank = jnp.zeros((tile_width, tile_width), bf16)

    top, low = slice(0, half), slice(half, width)

    def by_halves(left, right):
        return jnp.concatenate(
            [
                jnp.dot(left[rows], right, preferred_element_type=f32)
                for rows in (slice(0, half), slice(half, width))
            ],
            axis=0,
        )

    def picked(ids_ref, q, first):
        picks = []
        for tile in (first, first + 1):
            start = tile * tile_width
            inside = lax.rem(ids_ref[q, 0, :, start : start + tile_width], tile_width)
            picks.append(jnp.where(row_number == inside, 1.0, 0.0).astype(bf16))
        return picks

    def paired(picks):
        return jnp.concatenate(
            [
                jnp.concatenate([picks[0], blank], axis=1),
                jnp.concatenate([blank, picks[1]], axis=1),
            ],
            axis=0,
        )

    def block_of(scalar_ref, place, tile):
        return lax.div(scalar_ref[place, 0, 0, tile * tile_width], tile_width)

    def partial(pe, py, pc, head_blocks=head_ids, tail_blocks=tail_ids, place=None):
        q = pe * 4 + py * 2 + pc
        place = q if place is None else place
        for first in range(0, triples // tile_width, 2):
            cols = slice(first * tile_width, (first + 2) * tile_width)
            picks = picked(heads_ref, q, first)
            blocks = [turned[block_of(head_blocks, place, tile)] for tile in (first, first + 1)]
            rows = jnp.dot(
                jnp.concatenate(blocks, axis=1), paired(picks), preferred_element_type=f32
            )
            left_rows[:, cols] = (values_ref[q, 0, :, cols] * rows).astype(bf16)
            picks = [pick.T for pick in picked(tails_ref, q, first)]
            blocks = [
                factors_ref[block_of(tail_blocks, place, tile)] for tile in (first, first + 1)
            ]
            right_rows[cols, :] = jnp.dot(
                paired(picks), jnp.concatenate(blocks, axis=0), preferred_element_type=f32
            ).astype(bf16)
        return [
            jnp.dot(left_rows[rows, :], right_rows[...], preferred_element_type=f32)
            for rows in (top, low)
        ]

    targets = ((1 - e, 1 - y), (1 - e, y), (e, 1 - y), (e, y))
    pair_copies = []

    def give(index):
        pe, py = targets[index]
        pair_out[index, top], pair_out[index, low] = partial(pe, py, 1 - c)
        pair_copies.append(send(pair_out.at[index], pair_in.at[index], pair_peer))

    def keep(index):
        pe, py = targets[index]
        own_sum[index, top], own_sum[index, low] = partial(pe, py, c)

    def join(index):
        pair_copies[index].wait_recv()
        own_sum[index] = own_sum[index] + pair_in[index]

    for load in loads[:5]:
        load.wait()
    pair_out[0, top], pair_out[0, low] = partial(
        1 - e, 1 - y, 1 - c, first_heads, first_tails, 0
    )
    pl.semaphore_wait(barrier, len(near) + line_count)
    pair_top = send(pair_out.at[0, pl.ds(0, half)], pair_in.at[0, pl.ds(0, half)], pair_peer)
    pair_low = send(pair_out.at[0, pl.ds(half, half)], pair_in.at[0, pl.ds(half, half)], pair_peer)
    pair_copies.append(None)
    if z_count > 2:
        tell(ready.at[0])
    gram_part[...] = by_halves(
        jnp.concatenate(flipped, axis=1),
        jnp.concatenate([factors_ref[block] for block in range(block_count)], axis=0),
    )
    g_pair = send(gram_part.at[other_share], gram_in, pair_peer)
    for load in loads[5:]:
        load.wait()
    keep(0)
    g_pair.wait_recv()
    gram_half[0] = gram_part[own_share, :] + gram_in[...]
    upper, lower = pl.ds(0, part), pl.ds(part, part)
    g_a1 = send(gram_half.at[0, upper], gram_xy.at[0, upper], x_peer)
    g_b1 = send(gram_half.at[0, lower], gram_xy.at[0, lower], y_peer)
    pair_top.wait_recv()
    own_sum[0, top] = own_sum[0, top] + pair_in[0, top]
    a_diag = send(own_sum.at[0, pl.ds(0, half)], first_a.at[0], x_peer)
    pair_low.wait_recv()
    own_sum[0, low] = own_sum[0, low] + pair_in[0, low]
    b_diag = send(own_sum.at[0, pl.ds(half, half)], first_b.at[0], y_peer)
    give(1)
    give(2)
    for step in range(1, z_count - 2):
        pl.semaphore_wait(ready.at[step - 1], line_count)
        tell(ready.at[step])
    keep(1)
    g_a1.wait_recv()
    g_b1.wait_recv()
    gram_half[1] = gram_half[0] + gram_xy[0]
    g_a2 = send(gram_half.at[1, upper], gram_xy.at[1, upper], y_peer)
    g_b2 = send(gram_half.at[1, lower], gram_xy.at[1, lower], x_peer)
    join(1)
    a_side = send(own_sum.at[1, pl.ds(0, half)], first_a.at[1], x_peer)
    keep(2)
    join(2)
    b_side = send(own_sum.at[2, pl.ds(half, half)], first_b.at[1], y_peer)
    give(3)
    keep(3)
    a_diag.wait_recv()
    second_a[0] = own_sum[2, :half, :] + first_a[0]
    a_last = send(second_a.at[0], second_a.at[1], y_peer)
    b_diag.wait_recv()
    second_b[0] = own_sum[1, half:, :] + first_b[0]
    b_last = send(second_b.at[0], second_b.at[1], x_peer)
    g_a2.wait_recv()
    g_b2.wait_recv()
    gram_line[0] = gram_half[1] + gram_xy[1]
    if z_count > 2:
        pl.semaphore_wait(ready.at[z_count - 3], line_count)
    line_pair = spare()
    for hop in range(1, z_count):
        copy_to(gram_line.at[0], gram_line.at[z_count - hop], z_peer(hop), line_pair).start()
    line_rest = gram_line.at[pl.ds(1, z_count - 1)]
    line_copy = copy_to(line_rest, line_rest, pair_peer, line_pair)
    sent.append(line_copy)
    join(3)
    line_copy.wait_recv()
    for hop in range(z_count):
        place = lax.rem(z + hop, z_count)
        gram_pair[0, pl.ds(pl.multiple_of(place * share, share), share), :] = gram_line[hop]
    g_full = send(gram_pair.at[0], gram_pair.at[1], pair_peer)
    g_full.wait_recv()
    gram_full[own_rows, :] = gram_pair[0] * scale_gram
    gram_full[other_rows, :] = gram_pair[1] * scale_gram

    def split(value):
        high = value.astype(bf16)
        return high, (value - high.astype(f32)).astype(bf16)

    def fold(value):
        return jnp.sum(value.reshape(-1, 8, value.shape[1]), axis=0)

    def total(parts):
        added = parts[0]
        for piece in parts[1:]:
            added = added + piece
        return jnp.sum(jnp.sum(added, axis=0, keepdims=True), axis=1, keepdims=True)

    strips = [slice(first, first + STRIP) for first in range(0, width, STRIP)]
    panels = range(0, width, PANEL)
    gram = gram_full[...]
    gram_high, gram_low = split(gram)
    gram_twice = jnp.dot(gram_high, gram_high, preferred_element_type=f32) + (
        jnp.dot(gram_high, gram_low, preferred_element_type=f32)
        + jnp.dot(gram_low, gram_high, preferred_element_type=f32)
    )
    for power, (high, low_part) in enumerate(((gram_high, gram_low), split(gram_twice))):
        for third, piece in enumerate((high, low_part, high)):
            span = slice(third * width, (third + 1) * width)
            factor_left[power, :, span] = piece
            factor_right[power, span, :] = piece

    def spread_out(strip, value):
        high, low_part = split(value)
        for third, piece in enumerate((high, high, low_part)):
            vector_parts[
                slice(third * width + strip.start, third * width + strip.stop), :
            ] = piece
        return fold(value * value)

    a_side.wait_recv()
    b_side.wait_recv()
    a_last.wait_recv()
    b_last.wait_recv()
    squares = []
    for strip in strips:
        later = strip.start >= half
        inside = slice(strip.start - half, strip.stop - half) if later else strip
        side, last = (first_b, second_b) if later else (first_a, second_a)
        value = ((own_sum[3, strip, :] + side[1, inside, :]) + last[1, inside, :]) * scale_target
        basis[0, strip, :] = value
        squares.append(spread_out(strip, value))

    lane = lax.broadcasted_iota(jnp.int32, (1, 128), 1)
    record = jnp.zeros((1, 128), f32)

    def noted(record, place, value):
        return jnp.where(lane == place, value, record)

    def sized(square):
        inverse = jnp.where(square > 0.0, lax.rsqrt(square), 0.0)
        return inverse, square * inverse

    def left_stage():
        for power in (0, 1):
            for first in panels:
                inner = jnp.dot(
                    factor_left[power, first : first + PANEL, :],
                    vector_parts[...],
                    preferred_element_type=f32,
                )
                for step in range(0, PANEL, STRIP):
                    high, low_part = split(inner[step : step + STRIP])
                    rows = slice(first + step, first + step + STRIP)
                    for third, piece in enumerate((high, high, low_part)):
                        inner_parts[power, rows, third * width : (third + 1) * width] = piece

    def right_stage(power, put):
        for first in panels:
            outer = jnp.dot(
                inner_parts[power, first : first + PANEL, :],
                factor_right[power],
                preferred_element_type=f32,
            )
            for step in range(0, PANEL, STRIP):
                put(slice(first + step, first + step + STRIP), outer[step : step + STRIP])

    inverses, lengths, diagonals = [], [], []
    crosses = []

    def put_image(strip, value):
        image[strip, :] = value
        crosses.append(fold(value * basis[0, strip, :]))

    def put_twice(strip, value):
        image_twice[strip, :] = value

    left_stage()
    right_stage(0, put_image)
    right_stage(1, put_twice)
    for index in range(0, ITERS, 2):
        inverse, length = sized(total(squares))
        diagonal = (total(crosses) * inverse) * inverse
        scaled = diagonal * inverse
        ratio = length * inverses[-1] if index > 0 else None
        squares, crosses = [], []
        now, before = (index // 2) % 2, (index // 2 + 1) % 2
        for strip in strips:
            value = image[strip, :] * inverse - scaled * basis[index, strip, :]
            if index > 0:
                value = value - ratio * basis[index - 1, strip, :]
            basis[index + 1, strip, :] = value
            squares.append(fold(value * value))
            beyond = image_twice[strip, :] * inverse - scaled * image[strip, :]
            if index > 0:
                beyond = beyond - ratio * mapped[before, strip, :]
            mapped[now, strip, :] = beyond
            crosses.append(fold(value * beyond))
            if index + 2 < ITERS:
                spread_out(strip, beyond)
        if index + 2 < ITERS:
            left_stage()
        next_inverse, next_length = sized(total(squares))
        next_diagonal = (total(crosses) * next_inverse) * next_inverse
        inverses += [inverse, next_inverse]
        lengths += [length, next_length]
        diagonals += [diagonal + ridge_weight, next_diagonal + ridge_weight]
        for place in (index, index + 1):
            record = noted(record, place, diagonals[place])
            record = noted(record, ITERS + place, lengths[place])
        if index + 4 == ITERS:
            early[0] = record
            early_copy = spread(early)
            b_last.wait_send()
        if index + 2 == ITERS:
            late[0] = record
            late_copy = spread(late)
            a_last.wait_send()
        next_scaled, next_ratio = next_diagonal * next_inverse, next_length * inverse
        squares, crosses = [], []
        for strip in strips:
            value = (
                mapped[now, strip, :] * next_inverse - next_ratio * basis[index, strip, :]
            ) - next_scaled * basis[index + 1, strip, :]
            basis[index + 2, strip, :] = value
            if index + 2 < ITERS:
                squares.append(fold(value * value))

        def next_image(strip, outer):
            raw[strip, :] = outer
            value = (
                outer * next_inverse - next_scaled * mapped[now, strip, :]
            ) - next_ratio * image[strip, :]
            image[strip, :] = value
            crosses.append(fold(value * basis[index + 2, strip, :]))

        def next_twice(strip, outer):
            image_twice[strip, :] = (
                outer * next_inverse - next_scaled * raw[strip, :]
            ) - next_ratio * image_twice[strip, :]

        if index + 2 < ITERS:
            right_stage(0, next_image)
            right_stage(1, next_twice)
    inverses.append(jnp.ones((1, 1), f32))
    for copy in sent:
        if copy is not a_last and copy is not b_last:
            copy.wait_send()

    def lanes_of(table):
        lines = table[...].reshape(8 * z_count, 128)
        blank_lines = jnp.zeros((128 - 8 * z_count, 128), f32)
        return jnp.concatenate([lines, blank_lines], axis=0).T

    def reduced(rows):
        added = rows[0]
        for row in rows[1:]:
            added = added + row
        return jnp.sum(added, axis=1, keepdims=True)

    def small_map(rows, alpha, beta):
        count = len(rows)
        made = []
        for j in range(min(count + 1, len(beta))):
            entry = None
            if j < count:
                entry = alpha[j] * rows[j]
            if j > 0:
                term = beta[j] * rows[j - 1]
                entry = term if entry is None else entry + term
            if j + 1 < count:
                entry = entry + beta[j + 1] * rows[j + 1]
            made.append(entry)
        return made

    def mixed_sum(first, ratio, second):
        return [
            one + ratio * second[j] if j < len(second) else one for j, one in enumerate(first)
        ]

    def products(residual, image):
        return (
            reduced([row * row for row in residual]),
            reduced([row * image[j] for j, row in enumerate(residual)]),
        )

    for place in range(2 * ITERS + 1):
        inverse = inverses[place if place < ITERS else place - ITERS]
        scale_ref[place : place + 1, :] = jnp.broadcast_to(inverse, (1, 128))
    early_copy.wait()
    filled = lanes_of(early)
    known = ITERS - 2
    alpha = [filled[j : j + 1, :] for j in range(known)]
    beta = [filled[ITERS + j : ITERS + j + 1, :] for j in range(known)]
    residual = [beta[0]]
    image = small_map(residual, alpha, beta)
    norm_now, product = products(residual, image)
    step_size = norm_now / product
    direction, along = residual, image
    fitted = []
    for index in range(known):
        if index == 0:
            fitted = [step_size * row for row in direction]
        else:
            fitted = [
                fitted[j] + step_size * row if j < len(fitted) else step_size * row
                for j, row in enumerate(direction)
            ]
        residual = [
            residual[j] - step_size * row if j < len(residual) else -(step_size * row)
            for j, row in enumerate(along)
        ]
        if index + 1 < known:
            image = small_map(residual, alpha, beta)
            norm_next, product = products(residual, image)
            ratio = norm_next / norm_now
            step_size = norm_next / (product - ratio * norm_next / step_size)
            direction = mixed_sum(residual, ratio, direction)
            along = mixed_sum(image, ratio, along)
            norm_now = norm_next

    late_copy.wait()
    filled = lanes_of(late)
    alpha += [filled[j : j + 1, :] for j in range(known, ITERS)]
    beta += [filled[ITERS + j : ITERS + j + 1, :] for j in range(known, ITERS)]
    beta.append(jnp.ones((1, 128), f32))
    along = along + [beta[known] * direction[-1]]
    residual = residual + [-(step_size * along[-1])]
    image = small_map(residual, alpha, beta)
    norm_next, product = products(residual, image)
    ratio = norm_next / norm_now
    step_next = norm_next / (product - ratio * norm_next / step_size)
    residual_before, image_before = residual, image
    residual = [
        residual[j] - step_next * row if j < len(residual) else -(step_next * row)
        for j, row in enumerate(mixed_sum(image, ratio, along))
    ]
    fitted = [
        fitted[j] + step_next * row if j < len(fitted) else step_next * row
        for j, row in enumerate(mixed_sum(residual_before, ratio, direction))
    ]
    image = small_map(residual, alpha, beta)
    norm_last, product = products(residual, image)
    ratio_last = norm_last / norm_next
    step_last = norm_last / (product - ratio_last * norm_last / step_next)
    direction = mixed_sum(residual, ratio_last, mixed_sum(residual_before, ratio, direction))
    along = mixed_sum(image, ratio_last, mixed_sum(image_before, ratio, along))
    fitted = [
        fitted[j] + step_last * row if j < len(fitted) else step_last * row
        for j, row in enumerate(direction)
    ]
    residual = [
        residual[j] - step_last * row if j < len(residual) else -(step_last * row)
        for j, row in enumerate(along)
    ]
    for place, row in enumerate(fitted + residual):
        mix_ref[place : place + 1, :] = row


def finish_kernel(
    basis, mix_ref, scale_ref, fit_hbm, res_hbm, fit_rows, res_rows, fit_sem, res_sem
):
    count = basis.shape[0] - 1
    width = basis.shape[2]
    own_weights = mix_ref[0 : 2 * count + 1, 0:1] * scale_ref[0 : 2 * count + 1, 0:1]
    spread_weights = jnp.broadcast_to(own_weights, (2 * count + 1, width))
    weights = [spread_weights[place : place + 1, :] for place in range(2 * count + 1)]
    height = fit_rows.shape[0] // CHUNKS
    copies = []
    for slot in range(CHUNKS):
        for first in range(slot * height, (slot + 1) * height, STRIP):
            strip = slice(first, first + STRIP)
            vector = basis[0, strip, :]
            fit, res = weights[0] * vector, weights[count] * vector
            for j in range(1, count + 1):
                vector = basis[j, strip, :]
                res = res + weights[count + j] * vector
                if j < count:
                    fit = fit + weights[j] * vector
            fit_rows[strip, :] = fit
            res_rows[strip, :] = res
        rows = pl.ds(slot * height, height)
        for source, dest, sem in ((fit_rows, fit_hbm, fit_sem), (res_rows, res_hbm, res_sem)):
            copies.append(
                pltpu.make_async_copy(source.at[rows], dest.at[0, rows], sem.at[slot])
            )
            copies[-1].start()
    for copy in copies:
        copy.wait()


def fused_body(factors, heads, tails, values):
    shards = lax.axis_size(("ent", "blk"))
    z_count = lax.axis_size("rel")
    ent_dev, width = factors.shape
    triples = heads.shape[3]
    half = width // 2
    f32, bf16 = jnp.float32, jnp.bfloat16
    vmem = pl.BlockSpec(memory_space=pltpu.VMEM)
    share = half // z_count
    basis, mix, scale = pl.pallas_call(
        functools.partial(
            fused_kernel, z_count, 1.0 / (ent_dev * shards), 1.0 / math.sqrt(shards * triples)
        ),
        out_shape=(
            pltpu.VMEM((ITERS + 1, width, width), f32),
            pltpu.VMEM((4 * ITERS, 128), f32),
            pltpu.VMEM((4 * ITERS, 128), f32),
        ),
        in_specs=[pl.BlockSpec(memory_space=pl.ANY)] * 4,
        out_specs=(vmem, vmem, vmem),
        scratch_shapes=[
            pltpu.VMEM((ent_dev // tile_width, tile_width, width), bf16),
            pltpu.VMEM(heads.shape, jnp.int32),
            pltpu.VMEM(tails.shape, jnp.int32),
            pltpu.VMEM(values.shape, f32),
            pltpu.SMEM(heads.shape, jnp.int32),
            pltpu.SMEM(tails.shape, jnp.int32),
            pltpu.SMEM((1,) + heads.shape[1:], jnp.int32),
            pltpu.SMEM((1,) + heads.shape[1:], jnp.int32),
            pltpu.SemaphoreType.DMA,
            pltpu.SemaphoreType.DMA((7,)),
            pltpu.SemaphoreType.REGULAR((max(z_count - 2, 1),)),
            pltpu.VMEM((ent_dev // tile_width, width, tile_width), bf16),
            pltpu.VMEM((width, triples), bf16),
            pltpu.VMEM((triples, width), bf16),
            pltpu.VMEM((width, width), f32),
            pltpu.VMEM((share, width), f32),
            pltpu.VMEM((2, share, width), f32),
            pltpu.VMEM((2, share, width), f32),
            pltpu.VMEM((z_count, share, width), f32),
            pltpu.VMEM((width, width), f32),
            pltpu.VMEM((2, half, width), f32),
            pltpu.VMEM((4, width, width), f32),
            pltpu.VMEM((4, width, width), f32),
            pltpu.VMEM((4, width, width), f32),
            pltpu.VMEM((2, half, width), f32),
            pltpu.VMEM((2, half, width), f32),
            pltpu.VMEM((2, half, width), f32),
            pltpu.VMEM((2, half, width), f32),
            pltpu.VMEM((2, width, 3 * width), bf16),
            pltpu.VMEM((2, 3 * width, width), bf16),
            pltpu.VMEM((3 * width, width), bf16),
            pltpu.VMEM((2, width, 3 * width), bf16),
            pltpu.VMEM((width, width), f32),
            pltpu.VMEM((width, width), f32),
            pltpu.VMEM((width, width), f32),
            pltpu.VMEM((2, width, width), f32),
            pltpu.VMEM((8 * z_count, 1, 128), f32),
            pltpu.VMEM((8 * z_count, 1, 128), f32),
            pltpu.SemaphoreType.DMA((COPIES,)),
            pltpu.SemaphoreType.DMA((COPIES,)),
        ],
        compiler_params=pltpu.CompilerParams(collective_id=0, has_side_effects=True),
    )(factors.reshape(ent_dev // tile_width, tile_width, width), heads, tails, values)
    out = jax.ShapeDtypeStruct((1, width, width), f32)
    anywhere = pl.BlockSpec(memory_space=pl.ANY)
    return pl.pallas_call(
        finish_kernel,
        out_shape=(out, out),
        in_specs=[vmem, vmem, vmem],
        out_specs=(anywhere, anywhere),
        scratch_shapes=[
            pltpu.VMEM((width, width), f32),
            pltpu.VMEM((width, width), f32),
            pltpu.SemaphoreType.DMA((CHUNKS,)),
            pltpu.SemaphoreType.DMA((CHUNKS,)),
        ],
        compiler_params=pltpu.CompilerParams(vmem_limit_bytes=16 * width * width * 4),
    )(basis, mix, scale)


def solution(mesh):
    placed = (
        P(("ent", "blk"), None),
        P(None, "rel", None, ("ent", "blk")),
        P(None, "rel", None, ("ent", "blk")),
        P(None, "rel", None, ("ent", "blk")),
    )
    sizes = dict(mesh.shape)
    fused = sizes["ent"] == 2 and sizes["blk"] == 4 and sizes["rel"] in (2, 4, 8)
    return jax.shard_map(
        fused_body if fused else body,
        mesh=mesh,
        in_specs=placed,
        out_specs=(P(("ent", "blk", "rel"), None, None), P(("ent", "blk", "rel"), None, None)),
        check_vma=False,
    )
```

```python
import functools
import math

import jax
import jax.numpy as jnp
from jax import lax
from jax.experimental import pallas as pl
from jax.experimental.pallas import tpu as pltpu
from jax.sharding import PartitionSpec as P

ITERS = 8


ridge_weight = 0.01
tile_width = 128


def apply_normal(gram_matrix, stacked):
    left_side = jnp.einsum("ab,kbc->kac", gram_matrix, stacked, precision=lax.Precision.HIGHEST)
    return (
        jnp.einsum("kac,cd->kad", left_side, gram_matrix, precision=lax.Precision.HIGHEST)
        + ridge_weight * stacked
    )


def two_products(residual, image_map):
    return lax.psum(
        (jnp.sum(residual * residual), jnp.sum(residual * image_map)), ("ent", "blk", "rel")
    )


def select_rows(entity_ids, block_table):
    group_size, width = entity_ids.shape
    tile_count = width // tile_width
    block_count = block_table.shape[0]
    tiled_ids = entity_ids.reshape(group_size, tile_count, tile_width)
    block_of = tiled_ids[:, :, 0] // tile_width
    block_pick = (
        block_of[:, :, None] == jnp.arange(block_count, dtype=jnp.int32)[None, None, :]
    ).astype(jnp.bfloat16)
    chosen = jnp.einsum(
        "gtb,bcr->gtcr", block_pick, block_table, preferred_element_type=jnp.float32
    ).astype(jnp.bfloat16)
    inside = tiled_ids % tile_width
    slot_pick = (
        inside[:, :, :, None] == jnp.arange(tile_width, dtype=jnp.int32)[None, None, None, :]
    ).astype(jnp.bfloat16)
    return jnp.einsum("gtoc,gtcr->gtor", slot_pick, chosen, preferred_element_type=jnp.float32)


def body(factors, heads, tails, values):
    shards = lax.axis_size(("ent", "blk"))
    ent_dev = factors.shape[0]
    rank_width = factors.shape[1]
    triple_count = heads.shape[3]
    relation_rows = heads.shape[0] * heads.shape[2]
    norm_scale = 1.0 / math.sqrt(shards * triple_count)
    gram_total = lax.psum(
        jnp.dot(factors.T, factors, preferred_element_type=jnp.float32), ("ent", "blk")
    )
    gram_matrix = gram_total / (ent_dev * shards)
    block_table = factors.reshape(ent_dev // tile_width, tile_width, rank_width)
    head_ids = heads.reshape(relation_rows, triple_count)
    tail_ids = tails.reshape(relation_rows, triple_count)
    weights = values.reshape(relation_rows, triple_count)

    def grouped(operands):
        head_group, tail_group, weight_group = operands
        group_size = head_group.shape[0]
        tile_count = triple_count // tile_width
        head_rows = select_rows(head_group, block_table)
        weighted = (
            weight_group.reshape(group_size, tile_count, tile_width)[:, :, :, None] * head_rows
        ).astype(jnp.bfloat16)
        tail_rows = select_rows(tail_group, block_table).astype(jnp.bfloat16)
        product = jnp.einsum(
            "gtci,gtcj->gij", weighted, tail_rows, preferred_element_type=jnp.float32
        )
        return product * norm_scale

    own_rows = relation_rows // shards
    group_size = math.gcd(own_rows * lax.axis_size(("ent", "blk")), 4)
    group_total = own_rows * lax.axis_size(("ent", "blk")) // group_size
    shaped = (
        head_ids.reshape(group_total, group_size, triple_count),
        tail_ids.reshape(group_total, group_size, triple_count),
        weights.reshape(group_total, group_size, triple_count),
    )
    results = lax.map(grouped, shaped)
    target = lax.psum_scatter(
        results.reshape(own_rows * lax.axis_size(("ent", "blk")), rank_width, rank_width),
        ("ent", "blk"),
        scatter_dimension=0,
        tiled=True,
    )
    fitted = jnp.zeros_like(target)
    residual = target
    image_map = apply_normal(gram_matrix, residual)
    norm_now, product = two_products(residual, image_map)
    step_size = norm_now / product
    direction = residual
    along = image_map
    for step_index in range(ITERS):
        fitted = fitted + step_size * direction
        residual = residual - step_size * along
        if step_index + 1 < ITERS:
            image_map = apply_normal(gram_matrix, residual)
            norm_next, product = two_products(residual, image_map)
            ratio_next = norm_next / norm_now
            step_size = norm_next / (product - ratio_next * norm_next / step_size)
            direction = residual + ratio_next * direction
            along = image_map + ratio_next * along
            norm_now = norm_next
    return (fitted, residual)


MESH = pl.DeviceIdType.MESH
COPIES = 20
CHUNKS = 4
STRIP = 32
PANEL = 128


def fused_kernel(
    z_count, scale_gram, scale_target,
    factors_hbm, heads_hbm, tails_hbm, values_hbm,
    basis, mix_ref, scale_ref,
    factors_ref, heads_ref, tails_ref, values_ref, head_ids, tail_ids,
    first_heads, first_tails, factor_sem, load_sem, ready,
    turned, left_rows, right_rows,
    gram_part, gram_in, gram_half, gram_xy, gram_line, gram_full, gram_pair,
    pair_out, pair_in, own_sum, first_a, first_b, second_a, second_b,
    factor_left, factor_right, vector_parts, inner_parts, image, image_twice, raw, mapped,
    early, late, send_sem, recv_sem,
):
    f32, bf16 = jnp.float32, jnp.bfloat16
    width = factors_ref.shape[2]
    half = width // 2
    share = half // z_count
    part = share // 2
    triples = heads_ref.shape[3]
    e = lax.axis_index("ent")
    b = lax.axis_index("blk")
    z = lax.axis_index("rel")
    y = b // 2
    c = b % 2
    pair_peer = (e, y * 2 + 1 - c, z)
    x_peer = (1 - e, b, z)
    y_peer = (e, (1 - y) * 2 + c, z)

    def group_peer(mask):
        me, my, mc = mask // 4, (mask // 2) % 2, mask % 2
        return (
            (1 - e) if me else e,
            ((1 - y) if my else y) * 2 + ((1 - c) if mc else c),
            z,
        )

    def z_peer(hop):
        return (e, b, lax.rem(z + hop, z_count))

    near = [group_peer(m) for m in (1, 2, 4)]
    inner = ((z > 0, -1), (z < z_count - 1, 1))

    def tell(semaphore):
        for present, hop in inner:
            @pl.when(present)
            def _():
                pl.semaphore_signal(
                    semaphore, inc=1, device_id=(e, b, z + hop), device_id_type=MESH
                )

    line_count = jnp.where(z > 0, 1, 0) + jnp.where(z < z_count - 1, 1, 0)
    barrier = pltpu.get_barrier_semaphore()
    for peer in near:
        pl.semaphore_signal(barrier, inc=1, device_id=peer, device_id_type=MESH)
    tell(barrier)
    first_q = (1 - e) * 4 + (1 - y) * 2 + 1 - c
    block_count = factors_ref.shape[0]
    factor_load = pltpu.make_async_copy(factors_hbm, factors_ref, factor_sem)
    factor_load.start()
    loads = []
    for slot, (source, dest) in enumerate(
        (
            (heads_hbm.at[pl.ds(first_q, 1)], first_heads),
            (tails_hbm.at[pl.ds(first_q, 1)], first_tails),
            (heads_hbm, heads_ref),
            (values_hbm, values_ref),
            (tails_hbm, tails_ref),
            (heads_hbm, head_ids),
            (tails_hbm, tail_ids),
        )
    ):
        loads.append(pltpu.make_async_copy(source, dest, load_sem.at[slot]))
        loads[-1].start()

    counter = [0]
    sent = []

    def spare():
        slot = counter[0]
        counter[0] += 1
        return send_sem.at[slot], recv_sem.at[slot]

    def copy_to(source, dest, peer, pair):
        return pltpu.make_async_remote_copy(
            src_ref=source, dst_ref=dest, send_sem=pair[0], recv_sem=pair[1],
            device_id=peer, device_id_type=MESH,
        )

    def send(source, dest, peer):
        copy = copy_to(source, dest, peer, spare())
        copy.start()
        sent.append(copy)
        return copy

    far_peers = [
        (m, hop) for hop in (*range(1, z_count), 0) for m in (7, 6, 5, 3, 4, 2, 1, 0) if m or hop
    ]

    def spread(table):
        pair = spare()
        for m, hop in far_peers:
            peer = group_peer(m)[:2] + (lax.rem(z + hop, z_count),)
            place = m * z_count + (z_count - hop) % z_count
            copy_to(table.at[0], table.at[place], peer, pair).start()
        others = table.at[pl.ds(1, 8 * z_count - 1)]
        return copy_to(others, others, pair_peer, pair)

    flipped = []
    factor_load.wait()
    for block in range(block_count):
        flipped.append(factors_ref[block].T)
        turned[block] = flipped[-1]
    own_rows = pl.ds(pl.multiple_of(c * half, half), half)
    other_rows = pl.ds(pl.multiple_of((1 - c) * half, half), half)
    own_share = pl.ds(pl.multiple_of(c * half + z * share, share), share)
    other_share = pl.ds(pl.multiple_of((1 - c) * half + z * share, share), share)

    row_number = lax.broadcasted_iota(jnp.int32, (tile_width, tile_width), 0)
    blank = jnp.zeros((tile_width, tile_width), bf16)

    top, low = slice(0, half), slice(half, width)

    def by_halves(left, right):
        return jnp.concatenate(
            [
                jnp.dot(left[rows], right, preferred_element_type=f32)
                for rows in (slice(0, half), slice(half, width))
            ],
            axis=0,
        )

    def picked(ids_ref, q, first):
        picks = []
        for tile in (first, first + 1):
            start = tile * tile_width
            inside = lax.rem(ids_ref[q, 0, :, start : start + tile_width], tile_width)
            picks.append(jnp.where(row_number == inside, 1.0, 0.0).astype(bf16))
        return picks

    def paired(picks):
        return jnp.concatenate(
            [
                jnp.concatenate([picks[0], blank], axis=1),
                jnp.concatenate([blank, picks[1]], axis=1),
            ],
            axis=0,
        )

    def block_of(scalar_ref, place, tile):
        return lax.div(scalar_ref[place, 0, 0, tile * tile_width], tile_width)

    def partial(pe, py, pc, head_blocks=head_ids, tail_blocks=tail_ids, place=None):
        q = pe * 4 + py * 2 + pc
        place = q if place is None else place
        for first in range(0, triples // tile_width, 2):
            cols = slice(first * tile_width, (first + 2) * tile_width)
            picks = picked(heads_ref, q, first)
            blocks = [turned[block_of(head_blocks, place, tile)] for tile in (first, first + 1)]
            rows = jnp.dot(
                jnp.concatenate(blocks, axis=1), paired(picks), preferred_element_type=f32
            )
            left_rows[:, cols] = (values_ref[q, 0, :, cols] * rows).astype(bf16)
            picks = [pick.T for pick in picked(tails_ref, q, first)]
            blocks = [
                factors_ref[block_of(tail_blocks, place, tile)] for tile in (first, first + 1)
            ]
            right_rows[cols, :] = jnp.dot(
                paired(picks), jnp.concatenate(blocks, axis=0), preferred_element_type=f32
            ).astype(bf16)
        return [
            jnp.dot(left_rows[rows, :], right_rows[...], preferred_element_type=f32)
            for rows in (top, low)
        ]

    targets = ((1 - e, 1 - y), (1 - e, y), (e, 1 - y), (e, y))
    pair_copies = []

    def give(index):
        pe, py = targets[index]
        pair_out[index, top], pair_out[index, low] = partial(pe, py, 1 - c)
        pair_copies.append(send(pair_out.at[index], pair_in.at[index], pair_peer))

    def keep(index):
        pe, py = targets[index]
        own_sum[index, top], own_sum[index, low] = partial(pe, py, c)

    def join(index):
        pair_copies[index].wait_recv()
        own_sum[index] = own_sum[index] + pair_in[index]

    for load in loads[:5]:
        load.wait()
    pair_out[0, top], pair_out[0, low] = partial(
        1 - e, 1 - y, 1 - c, first_heads, first_tails, 0
    )
    pl.semaphore_wait(barrier, len(near) + line_count)
    pair_top = send(pair_out.at[0, pl.ds(0, half)], pair_in.at[0, pl.ds(0, half)], pair_peer)
    pair_low = send(pair_out.at[0, pl.ds(half, half)], pair_in.at[0, pl.ds(half, half)], pair_peer)
    pair_copies.append(None)
    if z_count > 2:
        tell(ready.at[0])
    gram_part[...] = by_halves(
        jnp.concatenate(flipped, axis=1),
        jnp.concatenate([factors_ref[block] for block in range(block_count)], axis=0),
    )
    g_pair = send(gram_part.at[other_share], gram_in, pair_peer)
    for load in loads[5:]:
        load.wait()
    keep(0)
    g_pair.wait_recv()
    gram_half[0] = gram_part[own_share, :] + gram_in[...]
    upper, lower = pl.ds(0, part), pl.ds(part, part)
    g_a1 = send(gram_half.at[0, upper], gram_xy.at[0, upper], x_peer)
    g_b1 = send(gram_half.at[0, lower], gram_xy.at[0, lower], y_peer)
    pair_top.wait_recv()
    own_sum[0, top] = own_sum[0, top] + pair_in[0, top]
    a_diag = send(own_sum.at[0, pl.ds(0, half)], first_a.at[0], x_peer)
    pair_low.wait_recv()
    own_sum[0, low] = own_sum[0, low] + pair_in[0, low]
    b_diag = send(own_sum.at[0, pl.ds(half, half)], first_b.at[0], y_peer)
    give(1)
    give(2)
    for step in range(1, z_count - 2):
        pl.semaphore_wait(ready.at[step - 1], line_count)
        tell(ready.at[step])
    keep(1)
    g_a1.wait_recv()
    g_b1.wait_recv()
    gram_half[1] = gram_half[0] + gram_xy[0]
    g_a2 = send(gram_half.at[1, upper], gram_xy.at[1, upper], y_peer)
    g_b2 = send(gram_half.at[1, lower], gram_xy.at[1, lower], x_peer)
    join(1)
    a_side = send(own_sum.at[1, pl.ds(0, half)], first_a.at[1], x_peer)
    keep(2)
    join(2)
    b_side = send(own_sum.at[2, pl.ds(half, half)], first_b.at[1], y_peer)
    give(3)
    keep(3)
    a_diag.wait_recv()
    second_a[0] = own_sum[2, :half, :] + first_a[0]
    a_last = send(second_a.at[0], second_a.at[1], y_peer)
    b_diag.wait_recv()
    second_b[0] = own_sum[1, half:, :] + first_b[0]
    b_last = send(second_b.at[0], second_b.at[1], x_peer)
    g_a2.wait_recv()
    g_b2.wait_recv()
    gram_line[0] = gram_half[1] + gram_xy[1]
    if z_count > 2:
        pl.semaphore_wait(ready.at[z_count - 3], line_count)
    line_pair = spare()
    for hop in range(1, z_count):
        copy_to(gram_line.at[0], gram_line.at[z_count - hop], z_peer(hop), line_pair).start()
    line_rest = gram_line.at[pl.ds(1, z_count - 1)]
    line_copy = copy_to(line_rest, line_rest, pair_peer, line_pair)
    sent.append(line_copy)
    join(3)
    line_copy.wait_recv()
    for hop in range(z_count):
        place = lax.rem(z + hop, z_count)
        gram_pair[0, pl.ds(pl.multiple_of(place * share, share), share), :] = gram_line[hop]
    g_full = send(gram_pair.at[0], gram_pair.at[1], pair_peer)
    g_full.wait_recv()
    gram_full[own_rows, :] = gram_pair[0] * scale_gram
    gram_full[other_rows, :] = gram_pair[1] * scale_gram

    def split(value):
        high = value.astype(bf16)
        return high, (value - high.astype(f32)).astype(bf16)

    def fold(value):
        return jnp.sum(value.reshape(-1, 8, value.shape[1]), axis=0)

    def total(parts):
        added = parts[0]
        for piece in parts[1:]:
            added = added + piece
        return jnp.sum(jnp.sum(added, axis=0, keepdims=True), axis=1, keepdims=True)

    strips = [slice(first, first + STRIP) for first in range(0, width, STRIP)]
    panels = range(0, width, PANEL)
    gram = gram_full[...]
    gram_high, gram_low = split(gram)
    for third in range(3):
        span = slice(third * width, (third + 1) * width)
        factor_left[0, :, span] = (gram_high, gram_low, gram_high)[third]
        factor_right[0, span, :] = (gram_high, gram_low, gram_high)[third]
        vector_parts[span, :] = (gram_high, gram_high, gram_low)[third]
    for first in panels:
        rows = slice(first, first + PANEL)
        high, low_part = split(
            jnp.dot(factor_left[0, rows, :], vector_parts[...], preferred_element_type=f32)
        )
        for third, piece in enumerate((high, low_part, high)):
            factor_left[1, rows, third * width : (third + 1) * width] = piece
            factor_right[1, third * width + first : third * width + first + PANEL, :] = piece

    def spread_out(strip, value):
        high, low_part = split(value)
        for third, piece in enumerate((high, high, low_part)):
            vector_parts[
                slice(third * width + strip.start, third * width + strip.stop), :
            ] = piece
        return fold(value * value)

    a_side.wait_recv()
    b_side.wait_recv()
    a_last.wait_recv()
    b_last.wait_recv()
    squares = []
    for strip in strips:
        later = strip.start >= half
        inside = slice(strip.start - half, strip.stop - half) if later else strip
        side, last = (first_b, second_b) if later else (first_a, second_a)
        value = ((own_sum[3, strip, :] + side[1, inside, :]) + last[1, inside, :]) * scale_target
        basis[0, strip, :] = value
        squares.append(spread_out(strip, value))

    lane = lax.broadcasted_iota(jnp.int32, (1, 128), 1)
    record = jnp.zeros((1, 128), f32)

    def noted(record, place, value):
        return jnp.where(lane == place, value, record)

    def sized(square):
        inverse = jnp.where(square > 0.0, lax.rsqrt(square), 0.0)
        return inverse, square * inverse

    def left_stage():
        for power in (0, 1):
            for first in panels:
                inner = jnp.dot(
                    factor_left[power, first : first + PANEL, :],
                    vector_parts[...],
                    preferred_element_type=f32,
                )
                for step in range(0, PANEL, STRIP):
                    high, low_part = split(inner[step : step + STRIP])
                    rows = slice(first + step, first + step + STRIP)
                    for third, piece in enumerate((high, high, low_part)):
                        inner_parts[power, rows, third * width : (third + 1) * width] = piece

    def right_stage(power, put):
        for first in panels:
            outer = jnp.dot(
                inner_parts[power, first : first + PANEL, :],
                factor_right[power],
                preferred_element_type=f32,
            )
            for step in range(0, PANEL, STRIP):
                put(slice(first + step, first + step + STRIP), outer[step : step + STRIP])

    inverses, lengths, diagonals = [], [], []
    crosses = []

    def put_image(strip, value):
        image[strip, :] = value
        crosses.append(fold(value * basis[0, strip, :]))

    def put_twice(strip, value):
        image_twice[strip, :] = value

    left_stage()
    right_stage(0, put_image)
    right_stage(1, put_twice)
    for index in range(0, ITERS, 2):
        inverse, length = sized(total(squares))
        diagonal = (total(crosses) * inverse) * inverse
        scaled = diagonal * inverse
        ratio = length * inverses[-1] if index > 0 else None
        squares, crosses = [], []
        now, before = (index // 2) % 2, (index // 2 + 1) % 2
        for strip in strips:
            value = image[strip, :] * inverse - scaled * basis[index, strip, :]
            if index > 0:
                value = value - ratio * basis[index - 1, strip, :]
            basis[index + 1, strip, :] = value
            squares.append(fold(value * value))
            beyond = image_twice[strip, :] * inverse - scaled * image[strip, :]
            if index > 0:
                beyond = beyond - ratio * mapped[before, strip, :]
            mapped[now, strip, :] = beyond
            crosses.append(fold(value * beyond))
            if index + 2 < ITERS:
                spread_out(strip, beyond)
        if index + 2 < ITERS:
            left_stage()
        next_inverse, next_length = sized(total(squares))
        next_diagonal = (total(crosses) * next_inverse) * next_inverse
        inverses += [inverse, next_inverse]
        lengths += [length, next_length]
        diagonals += [diagonal + ridge_weight, next_diagonal + ridge_weight]
        for place in (index, index + 1):
            record = noted(record, place, diagonals[place])
            record = noted(record, ITERS + place, lengths[place])
        if index + 4 == ITERS:
            early[0] = record
            early_copy = spread(early)
            b_last.wait_send()
        if index + 2 == ITERS:
            late[0] = record
            late_copy = spread(late)
            a_last.wait_send()
        next_scaled, next_ratio = next_diagonal * next_inverse, next_length * inverse
        squares, crosses = [], []
        for strip in strips:
            value = (
                mapped[now, strip, :] * next_inverse - next_ratio * basis[index, strip, :]
            ) - next_scaled * basis[index + 1, strip, :]
            basis[index + 2, strip, :] = value
            if index + 2 < ITERS:
                squares.append(fold(value * value))

        def next_image(strip, outer):
            raw[strip, :] = outer
            value = (
                outer * next_inverse - next_scaled * mapped[now, strip, :]
            ) - next_ratio * image[strip, :]
            image[strip, :] = value
            crosses.append(fold(value * basis[index + 2, strip, :]))

        def next_twice(strip, outer):
            image_twice[strip, :] = (
                outer * next_inverse - next_scaled * raw[strip, :]
            ) - next_ratio * image_twice[strip, :]

        if index + 2 < ITERS:
            right_stage(0, next_image)
            right_stage(1, next_twice)
    inverses.append(jnp.ones((1, 1), f32))
    for copy in sent:
        if copy is not a_last and copy is not b_last:
            copy.wait_send()

    def lanes_of(table):
        lines = table[...].reshape(8 * z_count, 128)
        blank_lines = jnp.zeros((128 - 8 * z_count, 128), f32)
        return jnp.concatenate([lines, blank_lines], axis=0).T

    def reduced(rows):
        added = rows[0]
        for row in rows[1:]:
            added = added + row
        return jnp.sum(added, axis=1, keepdims=True)

    def small_map(rows, alpha, beta):
        count = len(rows)
        made = []
        for j in range(min(count + 1, len(beta))):
            entry = None
            if j < count:
                entry = alpha[j] * rows[j]
            if j > 0:
                term = beta[j] * rows[j - 1]
                entry = term if entry is None else entry + term
            if j + 1 < count:
                entry = entry + beta[j + 1] * rows[j + 1]
            made.append(entry)
        return made

    def mixed_sum(first, ratio, second):
        return [
            one + ratio * second[j] if j < len(second) else one for j, one in enumerate(first)
        ]

    def products(residual, image):
        return (
            reduced([row * row for row in residual]),
            reduced([row * image[j] for j, row in enumerate(residual)]),
        )

    for place in range(2 * ITERS + 1):
        inverse = inverses[place if place < ITERS else place - ITERS]
        scale_ref[place : place + 1, :] = jnp.broadcast_to(inverse, (1, 128))
    early_copy.wait()
    filled = lanes_of(early)
    known = ITERS - 2
    alpha = [filled[j : j + 1, :] for j in range(known)]
    beta = [filled[ITERS + j : ITERS + j + 1, :] for j in range(known)]
    residual = [beta[0]]
    image = small_map(residual, alpha, beta)
    norm_now, product = products(residual, image)
    step_size = norm_now / product
    direction, along = residual, image
    fitted = []
    for index in range(known):
        if index == 0:
            fitted = [step_size * row for row in direction]
        else:
            fitted = [
                fitted[j] + step_size * row if j < len(fitted) else step_size * row
                for j, row in enumerate(direction)
            ]
        residual = [
            residual[j] - step_size * row if j < len(residual) else -(step_size * row)
            for j, row in enumerate(along)
        ]
        if index + 1 < known:
            image = small_map(residual, alpha, beta)
            norm_next, product = products(residual, image)
            ratio = norm_next / norm_now
            step_size = norm_next / (product - ratio * norm_next / step_size)
            direction = mixed_sum(residual, ratio, direction)
            along = mixed_sum(image, ratio, along)
            norm_now = norm_next

    late_copy.wait()
    filled = lanes_of(late)
    alpha += [filled[j : j + 1, :] for j in range(known, ITERS)]
    beta += [filled[ITERS + j : ITERS + j + 1, :] for j in range(known, ITERS)]
    beta.append(jnp.ones((1, 128), f32))
    along = along + [beta[known] * direction[-1]]
    residual = residual + [-(step_size * along[-1])]
    image = small_map(residual, alpha, beta)
    norm_next, product = products(residual, image)
    ratio = norm_next / norm_now
    step_next = norm_next / (product - ratio * norm_next / step_size)
    residual_before, image_before = residual, image
    residual = [
        residual[j] - step_next * row if j < len(residual) else -(step_next * row)
        for j, row in enumerate(mixed_sum(image, ratio, along))
    ]
    fitted = [
        fitted[j] + step_next * row if j < len(fitted) else step_next * row
        for j, row in enumerate(mixed_sum(residual_before, ratio, direction))
    ]
    image = small_map(residual, alpha, beta)
    norm_last, product = products(residual, image)
    ratio_last = norm_last / norm_next
    step_last = norm_last / (product - ratio_last * norm_last / step_next)
    direction = mixed_sum(residual, ratio_last, mixed_sum(residual_before, ratio, direction))
    along = mixed_sum(image, ratio_last, mixed_sum(image_before, ratio, along))
    fitted = [
        fitted[j] + step_last * row if j < len(fitted) else step_last * row
        for j, row in enumerate(direction)
    ]
    residual = [
        residual[j] - step_last * row if j < len(residual) else -(step_last * row)
        for j, row in enumerate(along)
    ]
    for place, row in enumerate(fitted + residual):
        mix_ref[place : place + 1, :] = row


def finish_kernel(
    basis, mix_ref, scale_ref, fit_hbm, res_hbm, fit_rows, res_rows, fit_sem, res_sem
):
    count = basis.shape[0] - 1
    width = basis.shape[2]
    own_weights = mix_ref[0 : 2 * count + 1, 0:1] * scale_ref[0 : 2 * count + 1, 0:1]
    spread_weights = jnp.broadcast_to(own_weights, (2 * count + 1, width))
    weights = [spread_weights[place : place + 1, :] for place in range(2 * count + 1)]
    height = fit_rows.shape[0] // CHUNKS
    copies = []
    for slot in range(CHUNKS):
        for first in range(slot * height, (slot + 1) * height, STRIP):
            strip = slice(first, first + STRIP)
            vector = basis[0, strip, :]
            fit, res = weights[0] * vector, weights[count] * vector
            for j in range(1, count + 1):
                vector = basis[j, strip, :]
                res = res + weights[count + j] * vector
                if j < count:
                    fit = fit + weights[j] * vector
            fit_rows[strip, :] = fit
            res_rows[strip, :] = res
        rows = pl.ds(slot * height, height)
        for source, dest, sem in ((fit_rows, fit_hbm, fit_sem), (res_rows, res_hbm, res_sem)):
            copies.append(
                pltpu.make_async_copy(source.at[rows], dest.at[0, rows], sem.at[slot])
            )
            copies[-1].start()
    for copy in copies:
        copy.wait()


def fused_body(factors, heads, tails, values):
    shards = lax.axis_size(("ent", "blk"))
    z_count = lax.axis_size("rel")
    ent_dev, width = factors.shape
    triples = heads.shape[3]
    half = width // 2
    f32, bf16 = jnp.float32, jnp.bfloat16
    vmem = pl.BlockSpec(memory_space=pltpu.VMEM)
    share = half // z_count
    basis, mix, scale = pl.pallas_call(
        functools.partial(
            fused_kernel, z_count, 1.0 / (ent_dev * shards), 1.0 / math.sqrt(shards * triples)
        ),
        out_shape=(
            pltpu.VMEM((ITERS + 1, width, width), f32),
            pltpu.VMEM((4 * ITERS, 128), f32),
            pltpu.VMEM((4 * ITERS, 128), f32),
        ),
        in_specs=[pl.BlockSpec(memory_space=pl.ANY)] * 4,
        out_specs=(vmem, vmem, vmem),
        scratch_shapes=[
            pltpu.VMEM((ent_dev // tile_width, tile_width, width), bf16),
            pltpu.VMEM(heads.shape, jnp.int32),
            pltpu.VMEM(tails.shape, jnp.int32),
            pltpu.VMEM(values.shape, f32),
            pltpu.SMEM(heads.shape, jnp.int32),
            pltpu.SMEM(tails.shape, jnp.int32),
            pltpu.SMEM((1,) + heads.shape[1:], jnp.int32),
            pltpu.SMEM((1,) + heads.shape[1:], jnp.int32),
            pltpu.SemaphoreType.DMA,
            pltpu.SemaphoreType.DMA((7,)),
            pltpu.SemaphoreType.REGULAR((max(z_count - 2, 1),)),
            pltpu.VMEM((ent_dev // tile_width, width, tile_width), bf16),
            pltpu.VMEM((width, triples), bf16),
            pltpu.VMEM((triples, width), bf16),
            pltpu.VMEM((width, width), f32),
            pltpu.VMEM((share, width), f32),
            pltpu.VMEM((2, share, width), f32),
            pltpu.VMEM((2, share, width), f32),
            pltpu.VMEM((z_count, share, width), f32),
            pltpu.VMEM((width, width), f32),
            pltpu.VMEM((2, half, width), f32),
            pltpu.VMEM((4, width, width), f32),
            pltpu.VMEM((4, width, width), f32),
            pltpu.VMEM((4, width, width), f32),
            pltpu.VMEM((2, half, width), f32),
            pltpu.VMEM((2, half, width), f32),
            pltpu.VMEM((2, half, width), f32),
            pltpu.VMEM((2, half, width), f32),
            pltpu.VMEM((2, width, 3 * width), bf16),
            pltpu.VMEM((2, 3 * width, width), bf16),
            pltpu.VMEM((3 * width, width), bf16),
            pltpu.VMEM((2, width, 3 * width), bf16),
            pltpu.VMEM((width, width), f32),
            pltpu.VMEM((width, width), f32),
            pltpu.VMEM((width, width), f32),
            pltpu.VMEM((2, width, width), f32),
            pltpu.VMEM((8 * z_count, 1, 128), f32),
            pltpu.VMEM((8 * z_count, 1, 128), f32),
            pltpu.SemaphoreType.DMA((COPIES,)),
            pltpu.SemaphoreType.DMA((COPIES,)),
        ],
        compiler_params=pltpu.CompilerParams(collective_id=0, has_side_effects=True),
    )(factors.reshape(ent_dev // tile_width, tile_width, width), heads, tails, values)
    out = jax.ShapeDtypeStruct((1, width, width), f32)
    anywhere = pl.BlockSpec(memory_space=pl.ANY)
    return pl.pallas_call(
        finish_kernel,
        out_shape=(out, out),
        in_specs=[vmem, vmem, vmem],
        out_specs=(anywhere, anywhere),
        scratch_shapes=[
            pltpu.VMEM((width, width), f32),
            pltpu.VMEM((width, width), f32),
            pltpu.SemaphoreType.DMA((CHUNKS,)),
            pltpu.SemaphoreType.DMA((CHUNKS,)),
        ],
        compiler_params=pltpu.CompilerParams(vmem_limit_bytes=16 * width * width * 4),
    )(basis, mix, scale)


def solution(mesh):
    placed = (
        P(("ent", "blk"), None),
        P(None, "rel", None, ("ent", "blk")),
        P(None, "rel", None, ("ent", "blk")),
        P(None, "rel", None, ("ent", "blk")),
    )
    sizes = dict(mesh.shape)
    fused = sizes["ent"] == 2 and sizes["blk"] == 4 and sizes["rel"] in (2, 4, 8)
    return jax.shard_map(
        fused_body if fused else body,
        mesh=mesh,
        in_specs=placed,
        out_specs=(P(("ent", "blk", "rel"), None, None), P(("ent", "blk", "rel"), None, None)),
        check_vma=False,
    )
```
